32 devices in a mesh: dp: 4 (over x, core), seq: 8 (over z, y).
Axes of the slice: x: 2, y: 2, z: 4, core: 2. Of those that a mesh axis runs over, the one named last changes fastest.
Arguments:
- tokens: bfloat16 [8, 1024, 1024], P('dp', 'seq'), may hold values from -6 to 6
- segment_ids: int32 [8, 1024], P('dp', 'seq'), may hold values from 0 to 3, never falling along the last dimension, each value on 1 to 512 neighbouring positions
- variate_ids: int32 [8, 1024], P('dp', 'seq'), may hold values from 0 to 3
- time_ids: int32 [8, 1024], P('dp', 'seq'), may hold values from 0 to 2047
- pad_mask: int32 [8, 1024], P('dp', 'seq'), may hold values 0 or 1
- cotangent: bfloat16 [8, 1024, 1024], P('dp', 'seq'), may hold values from -6 to 6
- w_qkv: bfloat16 [1024, 3072], P('dp', 'seq'), may hold values from -0.1875 to 0.1875
- w_out: bfloat16 [1024, 1024], P('dp', 'seq'), may hold values from -4 to 4
- w_gate: bfloat16 [1024, 4096], P('dp', 'seq'), may hold values from -0.1875 to 0.1875
- w_up: bfloat16 [1024, 4096], P('dp', 'seq'), may hold values from -0.1875 to 0.1875
- w_down: bfloat16 [4096, 1024], P('dp', 'seq'), may hold values from -0.09375 to 0.09375
- gain_attn: bfloat16 [1024], replicated, may hold values from 0.5 to 1.5
- gain_ffn: bfloat16 [1024], replicated, may hold values from 0.5 to 1.5
- variate_bias: bfloat16 [16], replicated, may hold values from -3 to 3
Outputs:
- output: bfloat16 [8, 1024, 1024], P('dp', 'seq')
- input_grad: bfloat16 [8, 1024, 1024], P('dp', 'seq')
- grad_w_qkv: float32 [1024, 3072], P('dp', 'seq')
- grad_w_out: float32 [1024, 1024], P('dp', 'seq')
- grad_w_gate: float32 [1024, 4096], P('dp', 'seq')
- grad_w_up: float32 [1024, 4096], P('dp', 'seq')
- grad_w_down: float32 [4096, 1024], P('dp', 'seq')
- grad_gain_attn: float32 [1024], replicated
- grad_gain_ffn: float32 [1024], replicated
- grad_variate_bias: float32 [16], replicated
The draws below stay inside these ranges and needn't reach their ends.
Inputs may be any that keep to these rules, and one draw needn't show every extreme that they name: `segment_ids`: along each sequence the ids never fall; a document spans 1 to 512 positions, and one spans exactly that many.
All inputs are finite; a program needn't handle non-finite values. No bound on the sum of `pad_mask` on one device may be relied on, other than what follows from the above.
Results may differ from the reference program's by a relative error of at most 0.015.
Values may be sent and summed in bfloat16 or wider, within the bound.
A program may use at most 256 MiB of HBM per device.

```python
import math
import jax
import jax.numpy as jnp
import numpy as np
from jax import lax

D = 1024
HEADS = 16
HEAD_DIM = 64
FF = 4096
WINDOW = 512
LENGTH = 1024
SEQS = 8


def plant(values, stream_key, least, largest):
    longest = values.shape.index(max(values.shape))
    spots = []
    for shift in (0, 1):
        where = [jax.random.randint(jax.random.fold_in(stream_key, axis), (), 0, length) for axis, length in enumerate(values.shape)]
        where[longest] = (where[longest] + shift) % values.shape[longest]
        spots.append(tuple(where))
    return values.at[spots[0]].set(least).at[spots[1]].set(largest)


def level_of(rng, dims, pieces, low, largest):
    gain = 1.0
    for axis_at, shards_of in pieces:
        steps = jax.random.uniform(jax.random.fold_in(jax.random.fold_in(rng, 6), axis_at), (shards_of,), jnp.float32, low / len(pieces), largest / len(pieces))
        gain = gain * jnp.repeat(jnp.exp(steps), dims[axis_at] // shards_of).reshape((-1,) + (1,) * (len(dims) - 1 - axis_at))
    return gain


def profile(amount, total, bound, lean):
    loads = [(1 << 20) // math.isqrt(rank ** lean) + 1 for rank in range(2, amount + 1)]
    spare, given = total - bound - (amount - 1), [1] * (amount - 1)
    while spare > 0:
        movable = [i for i in range(amount - 1) if given[i] < bound]
        mass, left = sum([loads[i] for i in movable]), spare
        for i in movable:
            addition = min(bound - given[i], max(1, left * loads[i] // mass), spare)
            given[i] = given[i] + addition
            spare = spare - addition
    return np.array([bound] + given)


def ragged(stream_key, count, total, bound, lean):
    if count == 2:
        one = jax.random.randint(stream_key, (), max(1, total - bound), min(bound, total - 1) + 1)
        return jnp.stack([one, total - one])
    tallies = jnp.asarray(profile(count, total, bound, lean), jnp.int32)
    twos = (count - 1) // 2
    giver, sink = tallies[1:1 + 2 * twos:2], tallies[2:2 + 2 * twos:2]
    room = jnp.minimum(giver - 1, bound - sink)
    passed = jax.random.randint(jax.random.fold_in(stream_key, 1), (twos,), 0, 1 << 20) % (room + 1)
    tallies = tallies.at[1:1 + 2 * twos:2].set(giver - passed).at[2:2 + 2 * twos:2].set(sink + passed)
    return tallies[jax.random.permutation(jax.random.fold_in(stream_key, 2), count)]


def centred(own_key, shape, scale, bound, pieces=(), kind=jnp.bfloat16):
    array = jax.random.normal(own_key, shape, jnp.float32) * scale
    if len(pieces) > 0:
        array = level_of(own_key, shape, pieces, -0.22, 0.18) * array
    return jnp.clip(array, min=-bound, max=bound).astype(kind)


def setup_inputs(seed: int = 0) -> dict:
    keys = jax.random.split(jax.random.key(seed), 15)
    return {
        "tokens": centred(keys[0], (SEQS, LENGTH, D), 1.0, 6.0, ((0, 4), (1, 8))),
        "segment_ids": jax.vmap(lambda own: jnp.searchsorted(jnp.cumsum(ragged(own, 4, LENGTH, LENGTH // 2, 1)), jnp.arange(LENGTH), side="right"))(jax.random.split(keys[1], SEQS)).reshape((SEQS, LENGTH)).astype(jnp.int32),
        "variate_ids": plant(jax.random.randint(keys[2], (SEQS, LENGTH), 0, 4), jax.random.fold_in(keys[2], 1), 0, 3).astype(jnp.int32),
        "time_ids": plant(jax.random.randint(keys[3], (SEQS, LENGTH), 0, 2048), jax.random.fold_in(keys[3], 1), 0, 2047).astype(jnp.int32),
        "pad_mask": plant((jax.random.randint(keys[4], (SEQS, LENGTH), 0, 8) < 7).astype(jnp.int32), jax.random.fold_in(keys[4], 1), 0, 1),
        "cotangent": centred(keys[5], (SEQS, LENGTH, D), 1.0, 6.0, ((0, 4), (1, 8))),
        "w_qkv": centred(keys[6], (D, 3 * D), D ** -0.5, 0.1875, ((0, 4), (1, 8))),
        "w_out": centred(keys[7], (D, D), (D // WINDOW) ** -0.5, 4.0, ((0, 4), (1, 8))),
        "w_gate": centred(keys[8], (D, FF), D ** -0.5, 0.1875, ((0, 4), (1, 8))),
        "w_up": centred(keys[9], (D, FF), D ** -0.5, 0.1875, ((0, 4), (1, 8))),
        "w_down": centred(keys[10], (FF, D), FF ** -0.5, 0.09375, ((0, 4), (1, 8))),
        "gain_attn": jnp.clip(1.0 + 0.1 * jax.random.normal(keys[11], (D,), jnp.float32), 0.5, 1.5).astype(jnp.bfloat16),
        "gain_ffn": jnp.clip(1.0 + 0.1 * jax.random.normal(keys[12], (D,), jnp.float32), 0.5, 1.5).astype(jnp.bfloat16),
        "variate_bias": centred(keys[13], (HEADS,), 1.0, 3.0),
    }


EPSILON = 1e-06
NEGATIVE = -1e+30
HIGHEST = lax.Precision.HIGHEST

@jax.custom_vjp
def low(v):
    return lax.optimization_barrier(v.astype(jnp.bfloat16)).astype(jnp.float32)

@jax.custom_vjp
def low_back(v):
    return v

def low_keep(v):
    return (low(v), None)

def low_pass(kept, grad):
    return (grad,)

def back_keep(v):
    return (v, None)

def back_low(kept, grad):
    return (low(grad),)
low.defvjp(low_keep, low_pass)
low_back.defvjp(back_keep, back_low)

def matmul(first_op, second_op):
    return jnp.dot(first_op, second_op, precision=HIGHEST, preferred_element_type=jnp.float32)

def rms_norm(hidden, gain_vector):
    return hidden * lax.rsqrt(lax.optimization_barrier(jnp.mean(hidden * hidden, axis=-1, keepdims=True)) + EPSILON) * gain_vector

def rope_tables(time_row):
    half_dim = HEAD_DIM // 2
    frequency = jnp.exp(-jnp.log(10000.0) * jnp.arange(half_dim, dtype=jnp.float32) / half_dim)
    angles = time_row.astype(jnp.float32)[:, None] * frequency[None, :]
    return (jnp.cos(angles)[:, None, :], jnp.sin(angles)[:, None, :])

def rotate(values_in, cos_table, sine_table):
    half_dim = cos_table.shape[-1]
    first_half = values_in[..., :half_dim]
    second_half = values_in[..., half_dim:]
    return jnp.concatenate([first_half * cos_table - second_half * sine_table, second_half * cos_table + first_half * sine_table], axis=-1)

def attention(query_rot, key_rot, value_low, var_bias, segment_row, variate_row, pad_row):
    length_all = query_rot.shape[0]
    query_block = min(512, length_all)
    key_span = query_block + 2 * WINDOW
    widths = ((WINDOW, WINDOW), (0, 0), (0, 0))
    keys_padded = jnp.pad(key_rot, widths)
    values_padded = jnp.pad(value_low, widths)
    segment_padded = jnp.pad(segment_row, (WINDOW, WINDOW), constant_values=-1)
    variate_padded = jnp.pad(variate_row, (WINDOW, WINDOW), constant_values=-1)
    pad_padded = jnp.pad(pad_row, (WINDOW, WINDOW))
    offsets = jnp.arange(key_span)[None, :] - WINDOW - jnp.arange(query_block)[:, None]

    def one_block(block_start):
        q_block = lax.dynamic_slice_in_dim(query_rot, block_start, query_block, 0)
        k_block = lax.dynamic_slice_in_dim(keys_padded, block_start, key_span, 0)
        v_block = lax.dynamic_slice_in_dim(values_padded, block_start, key_span, 0)
        seg_query = lax.dynamic_slice_in_dim(segment_row, block_start, query_block, 0)
        seg_keys = lax.dynamic_slice_in_dim(segment_padded, block_start, key_span, 0)
        var_query = lax.dynamic_slice_in_dim(variate_row, block_start, query_block, 0)
        var_keys = lax.dynamic_slice_in_dim(variate_padded, block_start, key_span, 0)
        pad_keys = lax.dynamic_slice_in_dim(pad_padded, block_start, key_span, 0)
        same_var = (var_query[:, None] == var_keys[None, :]).astype(jnp.float32)
        allowed = (jnp.abs(offsets) <= WINDOW) & (seg_query[:, None] == seg_keys[None, :]) & ((pad_keys[None, :] == 1) | (offsets == 0))
        scores = jnp.einsum('qhd,khd->hqk', q_block, k_block, precision=HIGHEST) * HEAD_DIM ** (-0.5) + var_bias[:, None, None] * same_var[None]
        scores = low_back(scores)
        scores = jnp.where(allowed[None], scores, NEGATIVE)
        exp_shift = jnp.exp(scores - lax.optimization_barrier(jnp.max(scores, axis=-1, keepdims=True)))
        probs_full = exp_shift / lax.optimization_barrier(jnp.sum(exp_shift, axis=-1, keepdims=True))
        return jnp.einsum('hqk,khd->qhd', low(probs_full), v_block, precision=HIGHEST)
    starts = jnp.arange(length_all // query_block, dtype=jnp.int32) * query_block
    blocks_out = lax.map(jax.checkpoint(one_block), starts)
    return blocks_out.reshape(length_all, HEADS * HEAD_DIM)

def encoder_layer(token_f32, weights, segment_row, variate_row, time_row, pad_row):
    w_qkv, w_out, w_gate, w_up, w_down, gain_attn, gain_ffn, var_bias = weights
    length_all = token_f32.shape[0]
    normed_one = low(rms_norm(token_f32, gain_attn))
    qkv_proj = low_back(matmul(normed_one, w_qkv))
    cos_table, sine_table = rope_tables(time_row)
    query_rot = low(rotate(qkv_proj[:, :D].reshape(length_all, HEADS, HEAD_DIM), cos_table, sine_table))
    key_rot = low(rotate(qkv_proj[:, D:2 * D].reshape(length_all, HEADS, HEAD_DIM), cos_table, sine_table))
    value_low = low(qkv_proj[:, 2 * D:].reshape(length_all, HEADS, HEAD_DIM))
    attended = attention(query_rot, key_rot, value_low, var_bias, segment_row, variate_row, pad_row)
    attended = low_back(low(attended))
    resid_mid = token_f32 + low_back(matmul(attended, w_out))
    normed_two = low(rms_norm(resid_mid, gain_ffn))
    gate_proj = low_back(matmul(normed_two, w_gate))
    up_proj = low_back(matmul(normed_two, w_up))
    hidden = low(gate_proj * jax.nn.sigmoid(gate_proj) * up_proj)
    return resid_mid + low_back(matmul(hidden, w_down))

def reference(tokens, segment_ids, variate_ids, time_ids, pad_mask, cotangent, w_qkv, w_out, w_gate, w_up, w_down, gain_attn, gain_ffn, variate_bias):
    params = tuple((weight.astype(jnp.float32) for weight in (w_qkv, w_out, w_gate, w_up, w_down, gain_attn, gain_ffn, variate_bias)))

    def per_sequence(grad_carry, inputs):
        token_rows, cot_rows, segment_row, variate_row, time_row, pad_row = inputs

        def forward(token_f32, *weights):
            return encoder_layer(token_f32, weights, segment_row, variate_row, time_row, pad_row)
        output_rows, pullback = jax.vjp(forward, token_rows.astype(jnp.float32), *params)
        gradients = pullback(cot_rows.astype(jnp.float32))
        grad_carry = tuple((carried + fresh_grad for carried, fresh_grad in zip(grad_carry, gradients[1:])))
        return (grad_carry, (output_rows.astype(jnp.bfloat16), gradients[0].astype(jnp.bfloat16)))
    zeros_init = tuple((jnp.zeros(parameter.shape, jnp.float32) for parameter in params))
    sums_out, (outputs, input_grads) = lax.scan(per_sequence, zeros_init, (tokens, cotangent, segment_ids, variate_ids, time_ids, pad_mask))
    return (outputs, input_grads, sums_out[0], sums_out[1], sums_out[2], sums_out[3], sums_out[4], sums_out[5], sums_out[6], sums_out[7])
```

```python
import functools

import jax
import jax.numpy as jnp
from jax import lax
from jax.experimental import pallas as pl
from jax.experimental.pallas import tpu as pltpu
from jax.sharding import PartitionSpec as P


HEADS = 16
HEAD_DIM = 64
WINDOW = 512


EPSILON = 1e-06
NEGATIVE = -1e30


def passed_along(block, axis, distance):
    devices = range(lax.axis_size(axis))
    route = [(i - distance, i) for i in devices if i - distance in devices]
    return lax.ppermute(block, axis, route)


def norm_scale(hidden):
    return lax.rsqrt(jnp.mean(hidden * hidden, axis=-1, keepdims=True) + EPSILON)


def norm_back(grad_in, hidden, inv_rms):
    return inv_rms * grad_in - hidden * inv_rms * inv_rms * inv_rms * jnp.mean(
        grad_in * hidden, axis=-1, keepdims=True
    )


def rope_tables(time_row, half_dim):
    frequency = jnp.exp(-jnp.log(10000.0) * jnp.arange(half_dim, dtype=jnp.float32) / half_dim)
    angles = time_row.astype(jnp.float32)[:, None] * frequency[None, :]
    return (jnp.cos(angles)[:, None, :], jnp.sin(angles)[:, None, :])


def rotate(values_in, cos_table, sine_table):
    half_dim = cos_table.shape[-1]
    first_half = values_in[..., :half_dim]
    second_half = values_in[..., half_dim:]
    return jnp.concatenate(
        [
            first_half * cos_table - second_half * sine_table,
            second_half * cos_table + first_half * sine_table,
        ],
        axis=-1,
    )


def rotate_back(grad_in, cos_table, sine_table):
    half_dim = cos_table.shape[-1]
    first_half = grad_in[..., :half_dim]
    second_half = grad_in[..., half_dim:]
    return jnp.concatenate(
        [
            first_half * cos_table + second_half * sine_table,
            second_half * cos_table - first_half * sine_table,
        ],
        axis=-1,
    )


def masked_scores(query_rot, keys_all, labels_own, labels_keys, var_bias, hop_count):
    row_count = query_rot.shape[0]
    key_count = keys_all.shape[0]
    offsets = (
        jnp.arange(key_count)[None, :] - hop_count * row_count - jnp.arange(row_count)[:, None]
    )
    allowed = (
        (jnp.abs(offsets) <= WINDOW)
        & (labels_own[0][:, None] == labels_keys[0][None, :])
        & ((labels_keys[2][None, :] == 1) | (offsets == 0))
    )
    same_var = (labels_own[1][:, None] == labels_keys[1][None, :]).astype(jnp.float32)
    scores = jnp.einsum(
        "qhd,khd->hqk", query_rot, keys_all, preferred_element_type=jnp.float32
    ) * HEAD_DIM ** (-0.5)
    scores = scores + var_bias[:, None, None] * same_var[None]
    return (jnp.where(allowed[None], scores, NEGATIVE), same_var)


def fetch_weights(shards):
    row_blocks = (
        lax.all_gather(shards[0], "dp", axis=0, tiled=True),
        lax.all_gather(shards[1], "dp", axis=0, tiled=True),
        lax.all_gather(shards[2], "dp", axis=0, tiled=True),
        lax.all_gather(shards[3], "dp", axis=0, tiled=True),
        lax.all_gather(shards[4], "dp", axis=0, tiled=True),
    )
    return (
        lax.all_gather(row_blocks[0], "seq", axis=1, tiled=True),
        lax.all_gather(row_blocks[1], "seq", axis=1, tiled=True),
        lax.all_gather(row_blocks[2], "seq", axis=1, tiled=True),
        lax.all_gather(row_blocks[3], "seq", axis=1, tiled=True),
        lax.all_gather(row_blocks[4], "seq", axis=1, tiled=True),
    )


def fetch_keep(shards):
    row_blocks = (
        lax.all_gather(shards[0], "dp", axis=0, tiled=True),
        lax.all_gather(shards[1], "dp", axis=0, tiled=True),
        lax.all_gather(shards[2], "dp", axis=0, tiled=True),
        lax.all_gather(shards[3], "dp", axis=0, tiled=True),
        lax.all_gather(shards[4], "dp", axis=0, tiled=True),
    )
    return (
        lax.all_gather(row_blocks[0], "seq", axis=1, tiled=True),
        lax.all_gather(row_blocks[1], "seq", axis=1, tiled=True),
        lax.all_gather(row_blocks[2], "seq", axis=1, tiled=True),
        lax.all_gather(row_blocks[3], "seq", axis=1, tiled=True),
        lax.all_gather(row_blocks[4], "seq", axis=1, tiled=True),
    )


def reduce_last(grads_full):
    col_sums = (
        lax.psum_scatter(grads_full[0], "seq", scatter_dimension=1, tiled=True),
        lax.psum_scatter(grads_full[1], "seq", scatter_dimension=1, tiled=True),
        lax.psum_scatter(grads_full[2], "seq", scatter_dimension=1, tiled=True),
        lax.psum_scatter(grads_full[3], "seq", scatter_dimension=1, tiled=True),
        lax.psum_scatter(grads_full[4], "seq", scatter_dimension=1, tiled=True),
    )
    return (
        lax.psum_scatter(
            col_sums[0].astype(jnp.bfloat16), "dp", scatter_dimension=0, tiled=True
        ).astype(jnp.float32),
        lax.psum_scatter(
            col_sums[1].astype(jnp.bfloat16), "dp", scatter_dimension=0, tiled=True
        ).astype(jnp.float32),
        lax.psum_scatter(
            col_sums[2].astype(jnp.bfloat16), "dp", scatter_dimension=0, tiled=True
        ).astype(jnp.float32),
        lax.psum_scatter(
            col_sums[3].astype(jnp.bfloat16), "dp", scatter_dimension=0, tiled=True
        ).astype(jnp.float32),
        lax.psum_scatter(
            col_sums[4].astype(jnp.bfloat16), "dp", scatter_dimension=0, tiled=True
        ).astype(jnp.float32),
    )


def weight_grads(pieces):
    (
        normed_one,
        grad_qkv,
        attended,
        grad_branch,
        normed_two,
        grad_gate,
        grad_up,
        hidden,
        grad_ffn,
    ) = pieces
    grad_w_qkv = jnp.einsum("td,tf->df", normed_one, grad_qkv, preferred_element_type=jnp.float32)
    grad_w_out = jnp.einsum("ti,to->io", attended, grad_branch, preferred_element_type=jnp.float32)
    grad_w_gate = jnp.einsum("td,tf->df", normed_two, grad_gate, preferred_element_type=jnp.float32)
    grad_w_up = jnp.einsum("td,tf->df", normed_two, grad_up, preferred_element_type=jnp.float32)
    grad_w_down = jnp.einsum("tf,td->fd", hidden, grad_ffn, preferred_element_type=jnp.float32)
    return (grad_w_qkv, grad_w_out, grad_w_gate, grad_w_up, grad_w_down)


def on_device(
    tokens,
    segment_ids,
    variate_ids,
    time_ids,
    pad_mask,
    cotangent,
    w_qkv,
    w_out,
    w_gate,
    w_up,
    w_down,
    gain_attn,
    gain_ffn,
    variate_bias,
):
    micro_count, row_count, model_width = tokens.shape
    hop_count = -(-WINDOW // row_count)
    key_count = (2 * hop_count + 1) * row_count
    shards = (w_qkv, w_out, w_gate, w_up, w_down)
    var_bias = variate_bias.astype(jnp.float32)
    gain_one = gain_attn.astype(jnp.float32)
    gain_two = gain_ffn.astype(jnp.float32)
    bias_total = jnp.zeros(var_bias.shape, jnp.float32)
    gain_one_total = jnp.zeros(gain_one.shape, jnp.float32)
    gain_two_total = jnp.zeros(gain_two.shape, jnp.float32)
    grad_totals = None
    saved = []
    outputs = []
    input_grads = []
    held_weights = fetch_weights(shards)
    for micro_step in range(micro_count):
        if micro_step == 0:
            weights = held_weights
        else:
            weights = fetch_keep(shards)
        resid_in = tokens[micro_step].astype(jnp.float32)
        inv_one = norm_scale(resid_in)
        normed_one = (resid_in * inv_one * gain_one).astype(jnp.bfloat16)
        qkv_proj = jnp.dot(normed_one, weights[0], preferred_element_type=jnp.float32)
        cos_table, sine_table = rope_tables(time_ids[micro_step], HEAD_DIM // 2)
        query_rot = rotate(
            qkv_proj[:, :model_width].reshape(row_count, HEADS, HEAD_DIM), cos_table, sine_table
        ).astype(jnp.bfloat16)
        key_rot = rotate(
            qkv_proj[:, model_width : 2 * model_width].reshape(row_count, HEADS, HEAD_DIM),
            cos_table,
            sine_table,
        ).astype(jnp.bfloat16)
        value_own = qkv_proj[:, 2 * model_width :].astype(jnp.bfloat16)
        kv_own = jnp.stack([key_rot.reshape(row_count, model_width), value_own])
        labels_own = jnp.stack(
            [segment_ids[micro_step], variate_ids[micro_step], pad_mask[micro_step]]
        )
        kv_slots = []
        label_slots = []
        for slot_index in range(2 * hop_count + 1):
            offset = slot_index - hop_count
            if offset == 0:
                kv_slots.append(kv_own)
                label_slots.append(labels_own)
            else:
                kv_slots.append(passed_along(kv_own, "seq", -offset))
                label_slots.append(passed_along(labels_own, "seq", -offset))
        kv_all = jnp.concatenate(kv_slots, axis=1)
        labels_keys = jnp.concatenate(label_slots, axis=1)
        keys_all = kv_all[0].reshape(key_count, HEADS, HEAD_DIM)
        values_all = kv_all[1].reshape(key_count, HEADS, HEAD_DIM)
        scores, same_var = masked_scores(
            query_rot, keys_all, labels_own, labels_keys, var_bias, hop_count
        )
        maxima = jnp.max(scores, axis=-1, keepdims=True)
        exp_shift = jnp.exp(scores - maxima)
        denom_sum = jnp.sum(exp_shift, axis=-1, keepdims=True)
        log_norm = maxima + jnp.log(denom_sum)
        prob_low = (exp_shift / denom_sum).astype(jnp.bfloat16)
        attended = jnp.einsum(
            "hqk,khd->qhd", prob_low, values_all, preferred_element_type=jnp.float32
        )
        attended = attended.reshape(row_count, model_width).astype(jnp.bfloat16)
        resid_mid = resid_in + jnp.dot(attended, weights[1], preferred_element_type=jnp.float32)
        inv_two = norm_scale(resid_mid)
        normed_two = (resid_mid * inv_two * gain_two).astype(jnp.bfloat16)
        gate_proj = jnp.dot(normed_two, weights[2], preferred_element_type=jnp.float32)
        up_proj = jnp.dot(normed_two, weights[3], preferred_element_type=jnp.float32)
        gate_sig = jax.nn.sigmoid(gate_proj)
        hidden = (gate_proj * gate_sig * up_proj).astype(jnp.bfloat16)
        ffn_out = jnp.dot(hidden, weights[4], preferred_element_type=jnp.float32)
        outputs.append((resid_mid + ffn_out).astype(jnp.bfloat16))
        grad_out = cotangent[micro_step].astype(jnp.float32)
        grad_ffn = grad_out.astype(jnp.bfloat16)
        grad_hidden = jnp.einsum(
            "td,fd->tf", grad_ffn, weights[4], preferred_element_type=jnp.float32
        )
        grad_gate = (
            grad_hidden * up_proj * gate_sig * (1.0 + gate_proj * (1.0 - gate_sig))
        ).astype(jnp.bfloat16)
        grad_up = (grad_hidden * gate_proj * gate_sig).astype(jnp.bfloat16)
        grad_normed_two = jnp.einsum(
            "tf,df->td", grad_gate, weights[2], preferred_element_type=jnp.float32
        )
        grad_normed_two = grad_normed_two + jnp.einsum(
            "tf,df->td", grad_up, weights[3], preferred_element_type=jnp.float32
        )
        gain_two_total = gain_two_total + jnp.sum(grad_normed_two * resid_mid * inv_two, axis=0)
        grad_mid = grad_out + norm_back(grad_normed_two * gain_two, resid_mid, inv_two)
        grad_branch = grad_mid.astype(jnp.bfloat16)
        grad_attended = jnp.einsum(
            "to,io->ti", grad_branch, weights[1], preferred_element_type=jnp.float32
        )
        grad_attended = grad_attended.astype(jnp.bfloat16).reshape(row_count, HEADS, HEAD_DIM)
        scores, same_var = masked_scores(
            query_rot, keys_all, labels_own, labels_keys, var_bias, hop_count
        )
        prob_full = jnp.exp(scores - log_norm)
        prob_low = prob_full.astype(jnp.bfloat16)
        grad_values = jnp.einsum(
            "hqk,qhd->khd", prob_low, grad_attended, preferred_element_type=jnp.float32
        )
        grad_prob = jnp.einsum(
            "qhd,khd->hqk", grad_attended, values_all, preferred_element_type=jnp.float32
        )
        grad_scores = prob_full * (
            grad_prob - jnp.sum(prob_full * grad_prob, axis=-1, keepdims=True)
        )
        grad_scores = grad_scores.astype(jnp.bfloat16)
        bias_total = bias_total + jnp.sum(
            grad_scores.astype(jnp.float32) * same_var[None], axis=(1, 2)
        )
        grad_query = jnp.einsum(
            "hqk,khd->qhd", grad_scores, keys_all, preferred_element_type=jnp.float32
        ) * HEAD_DIM ** (-0.5)
        grad_keys = jnp.einsum(
            "hqk,qhd->khd", grad_scores, query_rot, preferred_element_type=jnp.float32
        ) * HEAD_DIM ** (-0.5)
        grad_kv = jnp.stack(
            [grad_keys.reshape(key_count, model_width), grad_values.reshape(key_count, model_width)]
        )
        grad_kv_own = grad_kv[:, hop_count * row_count : (hop_count + 1) * row_count]
        for slot_index in range(2 * hop_count + 1):
            offset = slot_index - hop_count
            if offset != 0:
                slot_grad = grad_kv[:, slot_index * row_count : (slot_index + 1) * row_count]
                grad_kv_own = grad_kv_own + passed_along(
                    slot_grad.astype(jnp.bfloat16), "seq", offset
                ).astype(slot_grad.dtype)
        grad_q_plain = rotate_back(grad_query, cos_table, sine_table).reshape(
            row_count, model_width
        )
        grad_k_plain = rotate_back(
            grad_kv_own[0].reshape(row_count, HEADS, HEAD_DIM), cos_table, sine_table
        ).reshape(row_count, model_width)
        grad_qkv = jnp.concatenate([grad_q_plain, grad_k_plain, grad_kv_own[1]], axis=1).astype(
            jnp.bfloat16
        )
        grad_normed_one = jnp.einsum(
            "tf,df->td", grad_qkv, weights[0], preferred_element_type=jnp.float32
        )
        gain_one_total = gain_one_total + jnp.sum(grad_normed_one * resid_in * inv_one, axis=0)
        grad_input = grad_mid + norm_back(grad_normed_one * gain_one, resid_in, inv_one)
        input_grads.append(grad_input.astype(jnp.bfloat16))
        pieces = (
            normed_one,
            grad_qkv,
            attended,
            grad_branch,
            normed_two,
            grad_gate,
            grad_up,
            hidden,
            grad_ffn,
        )
        saved.append(pieces)
    joined = tuple(
        (
            jnp.concatenate([entry[index] for entry in saved], axis=0)
            for index in range(len(saved[0]))
        )
    )
    grad_totals = reduce_last(weight_grads(joined))
    bias_sum, gain_one_sum, gain_two_sum = lax.psum(
        (bias_total, gain_one_total, gain_two_total), ("dp", "seq")
    )
    return (
        jnp.stack(outputs),
        jnp.stack(input_grads),
        grad_totals[0],
        grad_totals[1],
        grad_totals[2],
        grad_totals[3],
        grad_totals[4],
        gain_one_sum,
        gain_two_sum,
        bias_sum,
    )


MESH = pl.DeviceIdType.MESH
VM = pl.BlockSpec(memory_space=pltpu.VMEM)
DMA = pltpu.SemaphoreType.DMA


def at(dp, seq):
    return {"dp": dp, "seq": seq}


def ring(i):
    return i + 1 - 2 * lax.rem(i, 2), lax.rem(i + 2, 4)


def meet(peers):
    barrier = pltpu.get_barrier_semaphore()
    for peer in peers:
        pl.semaphore_signal(barrier, inc=1, device_id=peer, device_id_type=MESH)
    pl.semaphore_wait(barrier, len(peers))


def send(src, dst, send_sem, recv_sem, peer):
    return pltpu.make_async_remote_copy(
        src_ref=src,
        dst_ref=dst,
        send_sem=send_sem,
        recv_sem=recv_sem,
        device_id=peer,
        device_id_type=MESH,
    )


def comm_call(kernel, outs, scratch, collective_id, in_count, vmem=None):
    return pl.pallas_call(
        kernel,
        out_shape=outs,
        in_specs=[VM] * in_count,
        out_specs=[VM] * len(outs),
        scratch_shapes=scratch,
        compiler_params=pltpu.CompilerParams(
            collective_id=collective_id, has_side_effects=True, vmem_limit_bytes=vmem
        ),
    )


def bf16(*shape):
    return jax.ShapeDtypeStruct(shape, jnp.bfloat16)


def f32(*shape):
    return jax.ShapeDtypeStruct(shape, jnp.float32)


def weight_pieces(kind, refs, dst, me, other, seq):
    if kind == "attention":
        w_qkv, w_out = refs
        place = lax.rem(other + 2 * lax.rem(seq, 2), 4)
        return [
            (w_qkv.at[place], dst.at[pl.ds(256 * me, 256)]),
            (w_out.at[pl.ds(64 * other, 64)], dst.at[pl.ds(1024 + 64 * me, 64)]),
        ]
    w_gate, w_up, w_down = refs
    columns = pl.ds(pl.multiple_of(128 * other, 128), 128)
    pairs = [
        (w_gate.at[:, columns], dst.at[pl.ds(256 * me, 256)]),
        (w_up.at[:, columns], dst.at[pl.ds(1024 + 256 * me, 256)]),
    ]
    for half in (0, 1):
        pairs.append(
            (
                w_down.at[pl.ds(512 * half + 128 * other, 128)],
                dst.at[pl.ds(2048 + 256 * me + 128 * half, 128)],
            )
        )
    return pairs


def grad_pieces(kind, src, dst, me, other, seq):
    if kind == "attention":
        g_qkv, g_out = dst
        place = lax.rem(me + 2 * lax.rem(seq, 2), 4)
        return [
            (src.at[pl.ds(256 * other, 256)], g_qkv.at[place]),
            (src.at[pl.ds(1024 + 64 * other, 64)], g_out.at[pl.ds(64 * me, 64)]),
        ]
    g_gate, g_up, g_down = dst
    columns = pl.ds(pl.multiple_of(128 * me, 128), 128)
    pairs = [
        (src.at[pl.ds(256 * other, 256)], g_gate.at[:, columns]),
        (src.at[pl.ds(1024 + 256 * other, 256)], g_up.at[:, columns]),
    ]
    for half in (0, 1):
        pairs.append(
            (
                src.at[pl.ds(2048 + 256 * other + 128 * half, 128)],
                g_down.at[pl.ds(512 * half + 128 * me, 128)],
            )
        )
    return pairs


def exchange_kernel(pieces, n_in, n_out, *refs):
    ins, outs = refs[:n_in], refs[n_in : n_in + n_out]
    send_sem, recv_sem, own_sem = refs[n_in + n_out :]
    me, seq = lax.axis_index("dp"), lax.axis_index("seq")
    others = [lax.rem(me + step, 4) for step in (1, 2, 3)]
    meet([at(other, seq) for other in others])
    copies = []
    for step, other in enumerate(others):
        for index, (src, dst) in enumerate(pieces(ins, outs, me, other, seq)):
            copy = send(
                src, dst, send_sem.at[step, index], recv_sem.at[step, index], at(other, seq)
            )
            copy.start()
            copies.append(copy)
    own = [
        pltpu.make_async_copy(src, dst, own_sem.at[index])
        for index, (src, dst) in enumerate(pieces(ins, outs, me, me, seq))
    ]
    for copy in own:
        copy.start()
    for copy in own:
        copy.wait()
    for copy in copies:
        copy.wait()


def exchange(pieces, ins, outs, count, collective_id):
    kernel = functools.partial(exchange_kernel, pieces, len(ins), len(outs))
    return comm_call(
        kernel, outs, [DMA((3, count)), DMA((3, count)), DMA((count,))], collective_id, len(ins)
    )(*ins)


def home_meet(peers):
    i, j = lax.axis_index("dp"), lax.axis_index("seq")
    target, stays = j // 2, j // 2 == i
    barrier = pltpu.get_barrier_semaphore()
    for peer in peers:
        pl.semaphore_signal(barrier, inc=1, device_id=peer, device_id_type=MESH)
    for s in (0, 1):

        @pl.when(jnp.logical_not(stays & (2 * i + s == j)))
        def _():
            pl.semaphore_signal(
                barrier, inc=1, device_id=at(target, 2 * i + s), device_id_type=MESH
            )

    pl.semaphore_wait(barrier, len(peers) + jnp.where(stays, 1, 2))


def home_start(ins, outs, send_sem, recv_sem):
    i, j = lax.axis_index("dp"), lax.axis_index("seq")
    target, stays = j // 2, j // 2 == i
    slot = lax.rem(j, 2)
    for a in range(len(ins)):
        for s in (0, 1):
            here = stays & (2 * i + s == j)

            @pl.when(jnp.logical_not(here))
            def _():
                send(
                    ins[a].at[s],
                    outs[a].at[slot],
                    send_sem.at[a, s],
                    recv_sem.at[a, slot],
                    at(target, 2 * i + s),
                ).start()

            @pl.when(here)
            def _():
                pltpu.make_async_copy(ins[a].at[s], outs[a].at[slot], recv_sem.at[a, slot]).start()


def home_finish(ins, outs, send_sem, recv_sem):
    i, j = lax.axis_index("dp"), lax.axis_index("seq")
    stays = j // 2 == i
    for a in range(len(ins)):
        for s in (0, 1):
            pltpu.make_async_copy(ins[a].at[s], outs[a].at[s], recv_sem.at[a, s]).wait()

            @pl.when(jnp.logical_not(stays & (2 * i + s == j)))
            def _():
                pltpu.make_async_copy(ins[a].at[s], outs[a].at[s], send_sem.at[a, s]).wait()


def home_kernel(count, *refs):
    ins, outs = refs[:count], refs[count : 2 * count]
    send_sem, recv_sem = refs[2 * count :]
    home_meet([])
    home_start(ins, outs, send_sem, recv_sem)
    home_finish(ins, outs, send_sem, recv_sem)


def front_kernel(*refs):
    (tok, cot, ids, packed, w_out, w_gate, w_up, w_down), refs = refs[:8], refs[8:]
    (tok_o, cot_o, ids_o, attn_o, ffn_o), refs = refs[:5], refs[5:]
    h_send, h_recv, a_send, a_recv, a_own, f_send, f_recv, f_own = refs
    i, j = lax.axis_index("dp"), lax.axis_index("seq")
    others = [lax.rem(i + step, 4) for step in (1, 2, 3)]
    home_meet([at(other, j) for other in others])
    home_start((tok, cot, ids), (tok_o, cot_o, ids_o), h_send, h_recv)
    copies = []
    for kind, ins, out, sems in (
        ("attention", (packed, w_out), attn_o, (a_send, a_recv, a_own)),
        ("ffn", (w_gate, w_up, w_down), ffn_o, (f_send, f_recv, f_own)),
    ):
        for step, other in enumerate(others):
            for index, (src, dst) in enumerate(weight_pieces(kind, ins, out, i, other, j)):
                copy = send(
                    src, dst, sems[0].at[step, index], sems[1].at[step, index], at(other, j)
                )
                copy.start()
                copies.append(copy)
        for index, (src, dst) in enumerate(weight_pieces(kind, ins, out, i, i, j)):
            copy = pltpu.make_async_copy(src, dst, sems[2].at[index])
            copy.start()
            copies.append(copy)
    for copy in copies:
        copy.wait()
    home_finish((tok, cot, ids), (tok_o, cot_o, ids_o), h_send, h_recv)


def front(arrays, collective_id):
    return comm_call(
        front_kernel,
        [jax.ShapeDtypeStruct(v.shape, v.dtype) for v in arrays[:3]]
        + [bf16(1280, 128), bf16(3072, 128)],
        [DMA((3, 2)), DMA((3, 2)), DMA((3, 2)), DMA((3, 2)), DMA((2,)), DMA((3, 4)), DMA((3, 4)), DMA((4,))],
        collective_id,
        8,
    )(*arrays)


def send_home(arrays, collective_id):
    count = len(arrays)
    return comm_call(
        functools.partial(home_kernel, count),
        [jax.ShapeDtypeStruct(v.shape, v.dtype) for v in arrays],
        [DMA((count, 2)), DMA((count, 2))],
        collective_id,
        count,
    )(*arrays)


def gather_kernel(count, *refs):
    ins, outs = refs[:count], refs[count : 2 * count]
    own_sem, s_core, r_core, s_x, r_x, s_on, r_on = refs[2 * count :]
    i, j = lax.axis_index("dp"), lax.axis_index("seq")
    core, across = ring(i)
    diagonal = lax.rem(core + 2, 4)
    meet([at(core, j), at(across, j)])
    pending = []
    for a in range(count):
        for s in (0, 1):
            for sems, peer in (((s_x, r_x), across), ((s_core, r_core), core)):
                copy = send(
                    ins[a].at[s],
                    outs[a].at[2 * i + s],
                    sems[0].at[a, s],
                    sems[1].at[a, s],
                    at(peer, j),
                )
                copy.start()
                pending.append(copy)
            copy = pltpu.make_async_copy(ins[a].at[s], outs[a].at[2 * i + s], own_sem.at[a, s])
            copy.start()
            pending.append(copy)
    onward = []
    for a in range(count):
        for s in (0, 1):
            block = outs[a].at[2 * across + s]
            pltpu.make_async_copy(ins[a].at[s], block, r_x.at[a, s]).wait()
            copy = send(block, block, s_on.at[a, s], r_on.at[a, s], at(core, j))
            copy.start()
            onward.append(copy)
    for a in range(count):
        for s in (0, 1):
            pltpu.make_async_copy(ins[a].at[s], outs[a].at[2 * core + s], r_core.at[a, s]).wait()
            pltpu.make_async_copy(ins[a].at[s], outs[a].at[2 * diagonal + s], r_on.at[a, s]).wait()
    for index, copy in enumerate(pending):
        if index % 3 == 2:
            copy.wait()
        else:
            copy.wait_send()
    for copy in onward:
        copy.wait_send()


def gather_group(arrays, collective_id):
    count = len(arrays)
    return comm_call(
        functools.partial(gather_kernel, count),
        [jax.ShapeDtypeStruct((8,) + v.shape[1:], v.dtype) for v in arrays],
        [DMA((count, 2))] * 7,
        collective_id,
        count,
    )(*arrays)


def reduce_kernel(count, *refs):
    ins, outs = refs[:count], refs[count : 2 * count]
    from_core, to_x, from_x, s_core, r_core, s_x, r_x = refs[2 * count :]
    i, j = lax.axis_index("dp"), lax.axis_index("seq")
    core, across = ring(i)
    diagonal = lax.rem(core + 2, 4)
    meet([at(core, j), at(across, j)])
    pending = []
    for a in range(count):
        for side, owner in ((0, diagonal), (1, core)):
            for s in (0, 1):
                copy = send(
                    ins[a].at[2 * owner + s],
                    from_core.at[a, side, s],
                    s_core.at[a, side, s],
                    r_core.at[a, side, s],
                    at(core, j),
                )
                copy.start()
                pending.append(copy)
    across_copies = []
    for a in range(count):
        for s in (0, 1):
            pltpu.make_async_copy(
                ins[a].at[s], from_core.at[a, 0, s], r_core.at[a, 0, s]
            ).wait()
            both = ins[a][2 * across + s].astype(jnp.float32) + from_core[a, 0, s].astype(
                jnp.float32
            )
            to_x[a, s] = both.astype(jnp.bfloat16)
            copy = send(
                to_x.at[a, s], from_x.at[a, s], s_x.at[a, s], r_x.at[a, s], at(across, j)
            )
            copy.start()
            across_copies.append(copy)
    for a in range(count):
        for s in (0, 1):
            pltpu.make_async_copy(
                ins[a].at[s], from_core.at[a, 1, s], r_core.at[a, 1, s]
            ).wait()
            outs[a][s] = ins[a][2 * i + s].astype(jnp.float32) + from_core[a, 1, s].astype(
                jnp.float32
            )
    for a in range(count):
        for s in (0, 1):
            pltpu.make_async_copy(ins[a].at[s], from_x.at[a, s], r_x.at[a, s]).wait()
            outs[a][s] = outs[a][s] + from_x[a, s].astype(jnp.float32)
    for copy in pending + across_copies:
        copy.wait_send()


def reduce_group(arrays, collective_id):
    count = len(arrays)
    _, rows, width = arrays[0].shape
    block = (rows, width)
    return comm_call(
        functools.partial(reduce_kernel, count),
        [f32(2, rows, width) for _ in arrays],
        [
            pltpu.VMEM((count, 2, 2) + block, jnp.bfloat16),
            pltpu.VMEM((count, 2) + block, jnp.bfloat16),
            pltpu.VMEM((count, 2) + block, jnp.bfloat16),
            DMA((count, 2, 2)),
            DMA((count, 2, 2)),
            DMA((count, 2)),
            DMA((count, 2)),
        ],
        collective_id,
        count,
    )(*arrays)


def small_sum_kernel(x_ref, o_ref, first, second, s_sem, r_sem, s_sem2, r_sem2):
    i, j = lax.axis_index("dp"), lax.axis_index("seq")
    groups = [at(lax.rem(i + step, 4), j) for step in (1, 2, 3)]
    chains = [at(i, lax.rem(j + step, 8)) for step in range(1, 8)]
    meet(groups + chains)
    copies = []
    for step, peer in enumerate(groups):
        copy = send(x_ref, first.at[i], s_sem.at[step], r_sem.at[step], peer)
        copy.start()
        copies.append(copy)
    first[i] = x_ref[...]
    for copy in copies:
        copy.wait()
    second[j] = (first[0] + first[1]) + (first[2] + first[3])
    copies = []
    for step, peer in enumerate(chains):
        copy = send(second.at[j], second.at[j], s_sem2.at[step], r_sem2.at[step], peer)
        copy.start()
        copies.append(copy)
    for copy in copies:
        copy.wait()
    total = second[0]
    for step in range(1, 8):
        total = total + second[step]
    o_ref[...] = total


def small_sum(x, collective_id):
    return comm_call(
        small_sum_kernel,
        [jax.ShapeDtypeStruct(x.shape, x.dtype)],
        [
            pltpu.VMEM((4,) + x.shape, x.dtype),
            pltpu.VMEM((8,) + x.shape, x.dtype),
            DMA((3,)),
            DMA((3,)),
            DMA((7,)),
            DMA((7,)),
        ],
        collective_id,
        1,
    )(x)[0]


NT = (((1,), (1,)), ((), ()))
TN = (((0,), (0,)), ((), ()))


def swap_halves(x):
    lane = lax.broadcasted_iota(jnp.int32, x.shape, 1)
    width = x.shape[1]
    return jnp.where(lane % 64 < 32, pltpu.roll(x, width - 32, 1), pltpu.roll(x, 32, 1))


def attention_kernel(p_ref, cos_ref, sin_ref, idc_ref, idr_ref, bias_ref, q_ref, k_ref, v_ref, o_ref, lse_ref):
    @pl.loop(0, 4)
    def _(block):
        rows = pl.ds(block * 256, 256)
        cos_t, sin_t = cos_ref[rows, :], sin_ref[rows, :]
        for pair in (0, 1):
            cols = slice(128 * pair, 128 * pair + 128)
            for base, out in ((0, q_ref), (256, k_ref)):
                x = p_ref[rows, base + 128 * pair : base + 128 * pair + 128]
                out[rows, cols] = (x * cos_t + swap_halves(x) * sin_t).astype(jnp.bfloat16)
        v_ref[rows, :] = p_ref[rows, 512:768].astype(jnp.bfloat16)

    @pl.loop(0, 4)
    def _(block):
        start = block * 256
        rows = pl.ds(start, 256)
        seg_q, var_q = idc_ref[rows, 0:1], idc_ref[rows, 1:2]
        code_k, var_k = idr_ref[0:1, :], idr_ref[1:2, :]
        row = start + lax.broadcasted_iota(jnp.int32, (256, 1024), 0)
        col = lax.broadcasted_iota(jnp.int32, (256, 1024), 1)
        allowed = ((seg_q == code_k) & (jnp.abs(row - col) <= WINDOW)) | (row == col)
        masked = jnp.where(allowed, 0.0, NEGATIVE)
        same = jnp.where(var_q == var_k, 1.0, 0.0)
        stats = jnp.zeros((256, 128), jnp.float32)
        lane = lax.broadcasted_iota(jnp.int32, (256, 128), 1)
        for h in range(4):
            cols = slice(64 * h, 64 * h + 64)
            scores = lax.dot_general(
                q_ref[rows, cols] * 0.125, k_ref[:, cols], NT, preferred_element_type=jnp.float32
            )
            scores = scores + bias_ref[h] * same + masked
            top = jnp.max(scores, axis=1, keepdims=True)
            weight = jnp.exp(scores - top)
            total = jnp.sum(weight, axis=1, keepdims=True)
            mixed = jnp.dot(
                weight.astype(jnp.bfloat16), v_ref[:, cols], preferred_element_type=jnp.float32
            )
            o_ref[rows, cols] = (mixed / total).astype(jnp.bfloat16)
            stats = jnp.where(lane == h, top + jnp.log(total), stats)
        lse_ref[rows, :] = stats


def attention_back_kernel(
    q_ref, k_ref, v_ref, do_ref, lse_ref, cos_ref, sin_ref, idc_ref, idr_ref, bias_ref,
    dqkv_ref, dbias_ref, dq_acc, dk_acc, dv_acc,
):
    dk_acc[...] = jnp.zeros_like(dk_acc)
    dv_acc[...] = jnp.zeros_like(dv_acc)
    dbias_ref[...] = jnp.zeros_like(dbias_ref)

    @pl.loop(0, 4)
    def _(block):
        start = pl.multiple_of(block * 256, 256)
        rows = pl.ds(start, 256)
        code_k, var_k = idc_ref[:, 2:3], idc_ref[:, 1:2]
        seg_q, var_q = idr_ref[2:3, rows], idr_ref[1:2, rows]
        row = lax.broadcasted_iota(jnp.int32, (1024, 256), 0)
        col = start + lax.broadcasted_iota(jnp.int32, (1024, 256), 1)
        allowed = ((seg_q == code_k) & (jnp.abs(row - col) <= WINDOW)) | (row == col)
        masked = jnp.where(allowed, 0.0, NEGATIVE)
        same = jnp.where(var_q == var_k, 1.0, 0.0)
        for h in range(4):
            cols = slice(64 * h, 64 * h + 64)
            q_h, k_h, v_h = q_ref[rows, cols] * 0.125, k_ref[:, cols], v_ref[:, cols]
            do_h = do_ref[rows, cols]
            scores = lax.dot_general(k_h, q_h, NT, preferred_element_type=jnp.float32)
            scores = scores + bias_ref[h] * same + masked
            prob = jnp.exp(scores - lse_ref[h : h + 1, rows])
            dv_acc[:, cols] += jnp.dot(
                prob.astype(jnp.bfloat16), do_h, preferred_element_type=jnp.float32
            )
            dprob = lax.dot_general(v_h, do_h, NT, preferred_element_type=jnp.float32)
            mean = jnp.sum(prob * dprob, axis=0, keepdims=True)
            dscore = (prob * (dprob - mean)).astype(jnp.bfloat16)
            dbias_ref[h : h + 1, :] += jnp.sum(
                dscore.astype(jnp.float32) * same, axis=0, keepdims=True
            )
            dk_acc[:, cols] += jnp.dot(dscore, q_h, preferred_element_type=jnp.float32)
            dq_acc[rows, cols] = lax.dot_general(
                dscore, k_h, TN, preferred_element_type=jnp.float32
            ) * 0.125

    @pl.loop(0, 4)
    def _(block):
        rows = pl.ds(pl.multiple_of(block * 256, 256), 256)
        cos_t, sin_t = cos_ref[rows, :], sin_ref[rows, :]
        for pair in (0, 1):
            cols = slice(128 * pair, 128 * pair + 128)
            for base, acc in ((0, dq_acc), (256, dk_acc)):
                g = acc[rows, cols]
                dqkv_ref[rows, base + 128 * pair : base + 128 * pair + 128] = (
                    g * cos_t - swap_halves(g) * sin_t
                ).astype(jnp.bfloat16)
        dqkv_ref[rows, 512:768] = dv_acc[rows, :].astype(jnp.bfloat16)


def local_call(kernel, outs, scratch, specs, vmem):
    return pl.pallas_call(
        kernel,
        out_shape=outs,
        in_specs=specs,
        out_specs=[VM] * len(outs),
        scratch_shapes=scratch,
        compiler_params=pltpu.CompilerParams(vmem_limit_bytes=vmem),
    )


SM = pl.BlockSpec(memory_space=pltpu.SMEM)


def wide(ref, first, rows):
    return jnp.concatenate([ref[first, rows, :], ref[first + 1, rows, :]], axis=1)


def store_wide(ref, first, rows, value):
    ref[first, rows, :] = value[:, :128]
    ref[first + 1, rows, :] = value[:, 128:]


EVERY = slice(None)


def ffn_kernel(
    a_ref, g_ref, wg_ref, wu_ref, wd_ref,
    da_ref, out_ref, gg_ref, gu_ref, gd_ref,
    turned, da_acc, out_acc, hidden_s, dgate_s, dup_s,
):
    step, last = pl.program_id(0), pl.num_programs(0) - 1

    @pl.when(step == 0)
    def _():
        @pl.loop(0, 4)
        def _(t):
            rows = pl.ds(pl.multiple_of(t * 256, 256), 256)
            for d in range(4):
                cols = slice(256 * d, 256 * d + 256)
                turned[cols, rows] = a_ref[rows, cols].T

    wg, wu = wide(wg_ref, 0, EVERY), wide(wu_ref, 0, EVERY)
    wd = jnp.concatenate([wd_ref[b] for b in range(8)], axis=1)

    @pl.loop(0, 4)
    def _(t):
        rows = pl.ds(pl.multiple_of(t * 256, 256), 256)
        a, g = a_ref[rows, :], g_ref[rows, :]
        gate, up, dh = dot(a, wg), dot(a, wu), dot(g, wd, NT)
        sig = 1.0 / (1.0 + jnp.exp(-gate))
        gate_sig = gate * sig
        hidden = (gate_sig * up).astype(jnp.bfloat16)
        dgate = (dh * up * (sig + gate_sig * (1.0 - sig))).astype(jnp.bfloat16)
        dup = (dh * gate_sig).astype(jnp.bfloat16)
        hidden_s[rows, :] = hidden
        dgate_s[rows, :] = dgate
        dup_s[rows, :] = dup
        da = dot(dgate, wg, NT) + dot(dup, wu, NT)
        out = dot(hidden, wd)

        @pl.when(step == 0)
        def _():
            da_acc[rows, :] = da
            out_acc[rows, :] = out

        @pl.when(step > 0)
        def _():
            da_acc[rows, :] += da
            out_acc[rows, :] += out

    @pl.loop(0, 4)
    def _(d):
        rows = pl.ds(pl.multiple_of(d * 256, 256), 256)
        a_t = turned[rows, :]
        store_wide(gg_ref, 0, rows, dot(a_t, dgate_s[...], out=jnp.bfloat16))
        store_wide(gu_ref, 0, rows, dot(a_t, dup_s[...], out=jnp.bfloat16))

    h_t = hidden_s[...].T
    for d in range(4):
        store_wide(gd_ref, 2 * d, EVERY, dot(h_t, g_ref[:, 256 * d : 256 * d + 256], out=jnp.bfloat16))

    @pl.when(step == last)
    def _():
        da_ref[...] = da_acc[...].astype(jnp.bfloat16)
        out_ref[...] = out_acc[...].astype(jnp.bfloat16)


def ffn(a2, g_low, weights):
    tile = (2, 1024, 128)
    grads = [
        pl.BlockSpec(tile, lambda f: (f, 0, 0)),
        pl.BlockSpec(tile, lambda f: (f, 0, 0)),
        pl.BlockSpec((8, 256, 128), lambda f: (0, f, 0)),
    ]
    whole = pl.BlockSpec((1024, 1024), lambda f: (0, 0))
    return pl.pallas_call(
        ffn_kernel,
        grid=(4,),
        out_shape=[bf16(1024, 1024)] * 2 + [bf16(8, 1024, 128)] * 3,
        in_specs=[
            whole,
            whole,
            pl.BlockSpec(tile, lambda f: (f, 0, 0)),
            pl.BlockSpec(tile, lambda f: (f, 1, 0)),
            pl.BlockSpec((8, 256, 128), lambda f: (0, 8 + f, 0)),
        ],
        out_specs=[whole, whole] + grads,
        scratch_shapes=[pltpu.VMEM((1024, 1024), jnp.bfloat16)]
        + [pltpu.VMEM((1024, 1024), jnp.float32)] * 2
        + [pltpu.VMEM((1024, 256), jnp.bfloat16)] * 3,
        compiler_params=pltpu.CompilerParams(vmem_limit_bytes=52 << 20),
        name="ffn",
    )(a2, g_low, weights, weights, weights)


def attention(proj, cos_t, sin_t, id_cols, id_rows, bias):
    return local_call(
        attention_kernel, [bf16(1024, 256)] * 4 + [f32(1024, 128)], [], [VM] * 5 + [SM], 48 << 20
    )(proj, cos_t, sin_t, id_cols, id_rows, bias)


def attention_back(q, k, v, do, lse, cos_t, sin_t, id_cols, id_rows, bias):
    return local_call(
        attention_back_kernel,
        [bf16(1024, 768), f32(8, 256)],
        [pltpu.VMEM((1024, 256), jnp.float32)] * 3,
        [VM] * 9 + [SM],
        48 << 20,
    )(q, k, v, do, lse, cos_t, sin_t, id_cols, id_rows, bias)


SLOTS = (
    (0, 1, 2, 4, 5, 6, 8, 9, 10, 12, 13, 14),
    (0, 2, 3, 4, 6, 7, 8, 10, 11, 12, 14, 15),
)


def dot(a, b, dims=None, out=jnp.float32):
    dims = (((1,), (0,)), ((), ())) if dims is None else dims
    return lax.dot_general(a, b, dims, preferred_element_type=jnp.float32).astype(out)


def on_group(
    tokens, segment_ids, variate_ids, time_ids, pad_mask, cotangent,
    w_qkv, w_out, w_gate, w_up, w_down, gain_attn, gain_ffn, variate_bias,
):
    i = lax.axis_index("dp")
    low_half = i < 2
    gain_one, gain_two = gain_attn.astype(jnp.float32), gain_ffn.astype(jnp.float32)

    packed = jnp.pad(w_qkv, ((0, 0), (0, 128))).reshape(256, 2, 4, 64)
    packed = packed.transpose(2, 0, 1, 3).reshape(4, 256, 128)
    ids = jnp.stack([segment_ids, variate_ids, time_ids, pad_mask], axis=1)
    ids = jnp.pad(ids, ((0, 0), (0, 4), (0, 0)))
    own_tok, own_cot, own_ids, attn_block, ffn_block = front(
        [tokens, cotangent, ids, packed, w_out, w_gate, w_up, w_down], 1
    )
    attn_w = lax.all_gather(attn_block, "seq")
    ffn_w = lax.all_gather(ffn_block, "seq")
    all_tok, all_cot, all_ids = gather_group([own_tok, own_cot, own_ids], 4)
    all_tok = all_tok.reshape(1024, 1024)
    g_low = all_cot.reshape(1024, 1024)
    id_seq = all_ids.transpose(1, 0, 2).reshape(8, 1024)
    seg, var, time, pad = id_seq[0], id_seq[1], id_seq[2], id_seq[3]
    code = jnp.where(pad == 1, seg, -1)
    id_rows = jnp.stack([code, var, seg] + [seg] * 5)
    id_cols = jnp.pad(jnp.stack([seg, var, code], axis=1), ((0, 0), (0, 125)))
    frequency = jnp.exp(-jnp.log(10000.0) * jnp.arange(32, dtype=jnp.float32) / 32)
    angles = time.astype(jnp.float32)[:, None] * frequency[None, :]
    cos_h, sin_h = jnp.cos(angles), jnp.sin(angles)
    cos_t = jnp.concatenate([cos_h] * 4, axis=1)
    sin_t = jnp.concatenate([-sin_h, sin_h] * 2, axis=1)
    bias = jnp.where(
        jnp.arange(4)[None, :] == i, variate_bias.astype(jnp.float32).reshape(4, 4), 0.0
    ).sum(axis=1)

    resid = all_tok.astype(jnp.float32)
    a1 = (resid * norm_scale(resid) * gain_one).astype(jnp.bfloat16)

    slots = attn_w[:, :1024].reshape(8, 1024, 2, 64)

    def column(m):
        first, second = SLOTS[0][m], SLOTS[1][m]
        return jnp.where(
            low_half, slots[first // 2, :, first % 2], slots[second // 2, :, second % 2]
        )

    w_heads = jnp.concatenate([column(m) for m in range(12)], axis=1)
    w_mix = attn_w[:, 1024:].transpose(1, 0, 2).reshape(256, 1024)
    proj = dot(a1, w_heads)
    q, k, v, attended, lse = attention(proj, cos_t, sin_t, id_cols, id_rows, bias)
    lse_rows = lse[:, :8].T
    part = dot(attended, w_mix, out=jnp.bfloat16).reshape(8, 128, 1024)
    (branch,) = reduce_group([part], 5)

    own = own_tok.reshape(256, 1024).astype(jnp.float32)
    inv_one = norm_scale(own)
    mid = own + branch.reshape(256, 1024)
    inv_two = norm_scale(mid)
    a2_own = (mid * inv_two * gain_two).astype(jnp.bfloat16)
    (a2,) = gather_group([a2_own.reshape(2, 128, 1024)], 6)
    a2 = a2.reshape(1024, 1024)

    da2_part, out_part, g_gate, g_up, g_down = ffn(a2, g_low, ffn_w)
    ffn_grads = jnp.concatenate([g_gate, g_up, g_down], axis=1)
    ffn_sum = lax.psum_scatter(ffn_grads, "seq", scatter_dimension=0)
    da2, ffn_out = reduce_group([da2_part.reshape(8, 128, 1024), out_part.reshape(8, 128, 1024)], 7)

    def blocks(g):
        return g.astype(jnp.bfloat16).reshape(-1, 8, 128).transpose(1, 0, 2)

    da2 = da2.reshape(256, 1024)
    output = (mid + ffn_out.reshape(256, 1024)).astype(jnp.bfloat16)
    grad_gain_two = jnp.sum(da2 * mid * inv_two, axis=0)
    own_cot = own_cot.reshape(256, 1024).astype(jnp.float32)
    e2 = own_cot + norm_back(da2 * gain_two, mid, inv_two)
    (ez,) = gather_group([e2.astype(jnp.bfloat16).reshape(2, 128, 1024)], 8)
    ez = ez.reshape(1024, 1024)
    do = dot(ez, w_mix, NT, jnp.bfloat16)
    dqkv, dbias = attention_back(q, k, v, do, lse_rows, cos_t, sin_t, id_cols, id_rows, bias)
    da1_part = dot(dqkv, w_heads, NT, jnp.bfloat16).reshape(8, 128, 1024)
    (da1,) = reduce_group([da1_part], 9)
    da1 = da1.reshape(256, 1024)
    grad_gain_one = jnp.sum(da1 * own * inv_one, axis=0)
    input_grad = (e2 + norm_back(da1 * gain_one, own, inv_one)).astype(jnp.bfloat16)
    output, input_grad = send_home(
        [output.reshape(2, 128, 1024), input_grad.reshape(2, 128, 1024)], 10
    )

    grad_heads = dot(a1, dqkv, TN, jnp.bfloat16).reshape(1024, 12, 64)
    grad_mix = dot(attended, ez, TN)
    nothing = jnp.zeros((1024, 64), jnp.bfloat16)

    def slot_grad(slot):
        picks = [
            grad_heads[:, SLOTS[half].index(slot)] if slot in SLOTS[half] else nothing
            for half in (0, 1)
        ]
        return jnp.where(low_half, picks[0], picks[1])

    grad_slots = jnp.stack(
        [
            jnp.concatenate([slot_grad(2 * b), slot_grad(2 * b + 1)], axis=1)
            for b in range(8)
        ]
    )
    attn_grads = jnp.concatenate([grad_slots, blocks(grad_mix)], axis=1)
    attn_sum = lax.psum_scatter(attn_grads, "seq", scatter_dimension=0)

    bias_grads = jnp.where(
        jnp.arange(4)[None, :] == i, jnp.sum(dbias[:4], axis=1)[:, None], 0.0
    ).reshape(16)
    small = jnp.concatenate(
        [grad_gain_one, grad_gain_two, jnp.pad(bias_grads, (0, 1024 - 16))]
    ).reshape(24, 128)
    small = small_sum(small, 11).reshape(3, 1024)

    g_gate, g_up, g_down = exchange(
        lambda ins, outs, me, other, seq: grad_pieces("ffn", ins[0], outs, me, other, seq),
        [ffn_sum], [bf16(256, 512), bf16(256, 512), bf16(1024, 128)], 4, 12,
    )
    g_qkv, g_out = exchange(
        lambda ins, outs, me, other, seq: grad_pieces("attention", ins[0], outs, me, other, seq),
        [attn_sum], [bf16(4, 256, 128), bf16(256, 128)], 2, 13,
    )
    g_qkv = g_qkv.reshape(4, 256, 2, 64).transpose(1, 2, 0, 3).reshape(256, 512)[:, :384]
    up32 = lambda g: g.astype(jnp.float32)
    return (
        output, input_grad, up32(g_qkv), up32(g_out), up32(g_gate), up32(g_up), up32(g_down),
        small[0], small[1], small[2, :16],
    )


def solution(mesh):
    in_specs = (
        P("dp", "seq", None),
        P("dp", "seq"),
        P("dp", "seq"),
        P("dp", "seq"),
        P("dp", "seq"),
        P("dp", "seq", None),
        P("dp", "seq"),
        P("dp", "seq"),
        P("dp", "seq"),
        P("dp", "seq"),
        P("dp", "seq"),
        P(),
        P(),
        P(),
    )
    out_specs = (
        P("dp", "seq", None),
        P("dp", "seq", None),
        P("dp", "seq"),
        P("dp", "seq"),
        P("dp", "seq"),
        P("dp", "seq"),
        P("dp", "seq"),
        P(),
        P(),
        P(),
    )
    grouped = mesh.shape["dp"] == 4 and mesh.shape["seq"] == 8
    return jax.shard_map(
        on_group if grouped else on_device, mesh=mesh, in_specs=in_specs, out_specs=out_specs, check_vma=False
    )
```

```python
import functools

import jax
import jax.numpy as jnp
from jax import lax
from jax.experimental import pallas as pl
from jax.experimental.pallas import tpu as pltpu
from jax.sharding import PartitionSpec as P


HEADS = 16
HEAD_DIM = 64
WINDOW = 512


EPSILON = 1e-06
NEGATIVE = -1e30


def passed_along(block, axis, distance):
    devices = range(lax.axis_size(axis))
    route = [(i - distance, i) for i in devices if i - distance in devices]
    return lax.ppermute(block, axis, route)


def norm_scale(hidden):
    return lax.rsqrt(jnp.mean(hidden * hidden, axis=-1, keepdims=True) + EPSILON)


def norm_back(grad_in, hidden, inv_rms):
    return inv_rms * grad_in - hidden * inv_rms * inv_rms * inv_rms * jnp.mean(
        grad_in * hidden, axis=-1, keepdims=True
    )


def rope_tables(time_row, half_dim):
    frequency = jnp.exp(-jnp.log(10000.0) * jnp.arange(half_dim, dtype=jnp.float32) / half_dim)
    angles = time_row.astype(jnp.float32)[:, None] * frequency[None, :]
    return (jnp.cos(angles)[:, None, :], jnp.sin(angles)[:, None, :])


def rotate(values_in, cos_table, sine_table):
    half_dim = cos_table.shape[-1]
    first_half = values_in[..., :half_dim]
    second_half = values_in[..., half_dim:]
    return jnp.concatenate(
        [
            first_half * cos_table - second_half * sine_table,
            second_half * cos_table + first_half * sine_table,
        ],
        axis=-1,
    )


def rotate_back(grad_in, cos_table, sine_table):
    half_dim = cos_table.shape[-1]
    first_half = grad_in[..., :half_dim]
    second_half = grad_in[..., half_dim:]
    return jnp.concatenate(
        [
            first_half * cos_table + second_half * sine_table,
            second_half * cos_table - first_half * sine_table,
        ],
        axis=-1,
    )


def masked_scores(query_rot, keys_all, labels_own, labels_keys, var_bias, hop_count):
    row_count = query_rot.shape[0]
    key_count = keys_all.shape[0]
    offsets = (
        jnp.arange(key_count)[None, :] - hop_count * row_count - jnp.arange(row_count)[:, None]
    )
    allowed = (
        (jnp.abs(offsets) <= WINDOW)
        & (labels_own[0][:, None] == labels_keys[0][None, :])
        & ((labels_keys[2][None, :] == 1) | (offsets == 0))
    )
    same_var = (labels_own[1][:, None] == labels_keys[1][None, :]).astype(jnp.float32)
    scores = jnp.einsum(
        "qhd,khd->hqk", query_rot, keys_all, preferred_element_type=jnp.float32
    ) * HEAD_DIM ** (-0.5)
    scores = scores + var_bias[:, None, None] * same_var[None]
    return (jnp.where(allowed[None], scores, NEGATIVE), same_var)


def fetch_weights(shards):
    row_blocks = (
        lax.all_gather(shards[0], "dp", axis=0, tiled=True),
        lax.all_gather(shards[1], "dp", axis=0, tiled=True),
        lax.all_gather(shards[2], "dp", axis=0, tiled=True),
        lax.all_gather(shards[3], "dp", axis=0, tiled=True),
        lax.all_gather(shards[4], "dp", axis=0, tiled=True),
    )
    return (
        lax.all_gather(row_blocks[0], "seq", axis=1, tiled=True),
        lax.all_gather(row_blocks[1], "seq", axis=1, tiled=True),
        lax.all_gather(row_blocks[2], "seq", axis=1, tiled=True),
        lax.all_gather(row_blocks[3], "seq", axis=1, tiled=True),
        lax.all_gather(row_blocks[4], "seq", axis=1, tiled=True),
    )


def fetch_keep(shards):
    row_blocks = (
        lax.all_gather(shards[0], "dp", axis=0, tiled=True),
        lax.all_gather(shards[1], "dp", axis=0, tiled=True),
        lax.all_gather(shards[2], "dp", axis=0, tiled=True),
        lax.all_gather(shards[3], "dp", axis=0, tiled=True),
        lax.all_gather(shards[4], "dp", axis=0, tiled=True),
    )
    return (
        lax.all_gather(row_blocks[0], "seq", axis=1, tiled=True),
        lax.all_gather(row_blocks[1], "seq", axis=1, tiled=True),
        lax.all_gather(row_blocks[2], "seq", axis=1, tiled=True),
        lax.all_gather(row_blocks[3], "seq", axis=1, tiled=True),
        lax.all_gather(row_blocks[4], "seq", axis=1, tiled=True),
    )


def reduce_last(grads_full):
    col_sums = (
        lax.psum_scatter(grads_full[0], "seq", scatter_dimension=1, tiled=True),
        lax.psum_scatter(grads_full[1], "seq", scatter_dimension=1, tiled=True),
        lax.psum_scatter(grads_full[2], "seq", scatter_dimension=1, tiled=True),
        lax.psum_scatter(grads_full[3], "seq", scatter_dimension=1, tiled=True),
        lax.psum_scatter(grads_full[4], "seq", scatter_dimension=1, tiled=True),
    )
    return (
        lax.psum_scatter(
            col_sums[0].astype(jnp.bfloat16), "dp", scatter_dimension=0, tiled=True
        ).astype(jnp.float32),
        lax.psum_scatter(
            col_sums[1].astype(jnp.bfloat16), "dp", scatter_dimension=0, tiled=True
        ).astype(jnp.float32),
        lax.psum_scatter(
            col_sums[2].astype(jnp.bfloat16), "dp", scatter_dimension=0, tiled=True
        ).astype(jnp.float32),
        lax.psum_scatter(
            col_sums[3].astype(jnp.bfloat16), "dp", scatter_dimension=0, tiled=True
        ).astype(jnp.float32),
        lax.psum_scatter(
            col_sums[4].astype(jnp.bfloat16), "dp", scatter_dimension=0, tiled=True
        ).astype(jnp.float32),
    )


def weight_grads(pieces):
    (
        normed_one,
        grad_qkv,
        attended,
        grad_branch,
        normed_two,
        grad_gate,
        grad_up,
        hidden,
        grad_ffn,
    ) = pieces
    grad_w_qkv = jnp.einsum("td,tf->df", normed_one, grad_qkv, preferred_element_type=jnp.float32)
    grad_w_out = jnp.einsum("ti,to->io", attended, grad_branch, preferred_element_type=jnp.float32)
    grad_w_gate = jnp.einsum("td,tf->df", normed_two, grad_gate, preferred_element_type=jnp.float32)
    grad_w_up = jnp.einsum("td,tf->df", normed_two, grad_up, preferred_element_type=jnp.float32)
    grad_w_down = jnp.einsum("tf,td->fd", hidden, grad_ffn, preferred_element_type=jnp.float32)
    return (grad_w_qkv, grad_w_out, grad_w_gate, grad_w_up, grad_w_down)


def on_device(
    tokens,
    segment_ids,
    variate_ids,
    time_ids,
    pad_mask,
    cotangent,
    w_qkv,
    w_out,
    w_gate,
    w_up,
    w_down,
    gain_attn,
    gain_ffn,
    variate_bias,
):
    micro_count, row_count, model_width = tokens.shape
    hop_count = -(-WINDOW // row_count)
    key_count = (2 * hop_count + 1) * row_count
    shards = (w_qkv, w_out, w_gate, w_up, w_down)
    var_bias = variate_bias.astype(jnp.float32)
    gain_one = gain_attn.astype(jnp.float32)
    gain_two = gain_ffn.astype(jnp.float32)
    bias_total = jnp.zeros(var_bias.shape, jnp.float32)
    gain_one_total = jnp.zeros(gain_one.shape, jnp.float32)
    gain_two_total = jnp.zeros(gain_two.shape, jnp.float32)
    grad_totals = None
    saved = []
    outputs = []
    input_grads = []
    held_weights = fetch_weights(shards)
    for micro_step in range(micro_count):
        if micro_step == 0:
            weights = held_weights
        else:
            weights = fetch_keep(shards)
        resid_in = tokens[micro_step].astype(jnp.float32)
        inv_one = norm_scale(resid_in)
        normed_one = (resid_in * inv_one * gain_one).astype(jnp.bfloat16)
        qkv_proj = jnp.dot(normed_one, weights[0], preferred_element_type=jnp.float32)
        cos_table, sine_table = rope_tables(time_ids[micro_step], HEAD_DIM // 2)
        query_rot = rotate(
            qkv_proj[:, :model_width].reshape(row_count, HEADS, HEAD_DIM), cos_table, sine_table
        ).astype(jnp.bfloat16)
        key_rot = rotate(
            qkv_proj[:, model_width : 2 * model_width].reshape(row_count, HEADS, HEAD_DIM),
            cos_table,
            sine_table,
        ).astype(jnp.bfloat16)
        value_own = qkv_proj[:, 2 * model_width :].astype(jnp.bfloat16)
        kv_own = jnp.stack([key_rot.reshape(row_count, model_width), value_own])
        labels_own = jnp.stack(
            [segment_ids[micro_step], variate_ids[micro_step], pad_mask[micro_step]]
        )
        kv_slots = []
        label_slots = []
        for slot_index in range(2 * hop_count + 1):
            offset = slot_index - hop_count
            if offset == 0:
                kv_slots.append(kv_own)
                label_slots.append(labels_own)
            else:
                kv_slots.append(passed_along(kv_own, "seq", -offset))
                label_slots.append(passed_along(labels_own, "seq", -offset))
        kv_all = jnp.concatenate(kv_slots, axis=1)
        labels_keys = jnp.concatenate(label_slots, axis=1)
        keys_all = kv_all[0].reshape(key_count, HEADS, HEAD_DIM)
        values_all = kv_all[1].reshape(key_count, HEADS, HEAD_DIM)
        scores, same_var = masked_scores(
            query_rot, keys_all, labels_own, labels_keys, var_bias, hop_count
        )
        maxima = jnp.max(scores, axis=-1, keepdims=True)
        exp_shift = jnp.exp(scores - maxima)
        denom_sum = jnp.sum(exp_shift, axis=-1, keepdims=True)
        log_norm = maxima + jnp.log(denom_sum)
        prob_low = (exp_shift / denom_sum).astype(jnp.bfloat16)
        attended = jnp.einsum(
            "hqk,khd->qhd", prob_low, values_all, preferred_element_type=jnp.float32
        )
        attended = attended.reshape(row_count, model_width).astype(jnp.bfloat16)
        resid_mid = resid_in + jnp.dot(attended, weights[1], preferred_element_type=jnp.float32)
        inv_two = norm_scale(resid_mid)
        normed_two = (resid_mid * inv_two * gain_two).astype(jnp.bfloat16)
        gate_proj = jnp.dot(normed_two, weights[2], preferred_element_type=jnp.float32)
        up_proj = jnp.dot(normed_two, weights[3], preferred_element_type=jnp.float32)
        gate_sig = jax.nn.sigmoid(gate_proj)
        hidden = (gate_proj * gate_sig * up_proj).astype(jnp.bfloat16)
        ffn_out = jnp.dot(hidden, weights[4], preferred_element_type=jnp.float32)
        outputs.append((resid_mid + ffn_out).astype(jnp.bfloat16))
        grad_out = cotangent[micro_step].astype(jnp.float32)
        grad_ffn = grad_out.astype(jnp.bfloat16)
        grad_hidden = jnp.einsum(
            "td,fd->tf", grad_ffn, weights[4], preferred_element_type=jnp.float32
        )
        grad_gate = (
            grad_hidden * up_proj * gate_sig * (1.0 + gate_proj * (1.0 - gate_sig))
        ).astype(jnp.bfloat16)
        grad_up = (grad_hidden * gate_proj * gate_sig).astype(jnp.bfloat16)
        grad_normed_two = jnp.einsum(
            "tf,df->td", grad_gate, weights[2], preferred_element_type=jnp.float32
        )
        grad_normed_two = grad_normed_two + jnp.einsum(
            "tf,df->td", grad_up, weights[3], preferred_element_type=jnp.float32
        )
        gain_two_total = gain_two_total + jnp.sum(grad_normed_two * resid_mid * inv_two, axis=0)
        grad_mid = grad_out + norm_back(grad_normed_two * gain_two, resid_mid, inv_two)
        grad_branch = grad_mid.astype(jnp.bfloat16)
        grad_attended = jnp.einsum(
            "to,io->ti", grad_branch, weights[1], preferred_element_type=jnp.float32
        )
        grad_attended = grad_attended.astype(jnp.bfloat16).reshape(row_count, HEADS, HEAD_DIM)
        scores, same_var = masked_scores(
            query_rot, keys_all, labels_own, labels_keys, var_bias, hop_count
        )
        prob_full = jnp.exp(scores - log_norm)
        prob_low = prob_full.astype(jnp.bfloat16)
        grad_values = jnp.einsum(
            "hqk,qhd->khd", prob_low, grad_attended, preferred_element_type=jnp.float32
        )
        grad_prob = jnp.einsum(
            "qhd,khd->hqk", grad_attended, values_all, preferred_element_type=jnp.float32
        )
        grad_scores = prob_full * (
            grad_prob - jnp.sum(prob_full * grad_prob, axis=-1, keepdims=True)
        )
        grad_scores = grad_scores.astype(jnp.bfloat16)
        bias_total = bias_total + jnp.sum(
            grad_scores.astype(jnp.float32) * same_var[None], axis=(1, 2)
        )
        grad_query = jnp.einsum(
            "hqk,khd->qhd", grad_scores, keys_all, preferred_element_type=jnp.float32
        ) * HEAD_DIM ** (-0.5)
        grad_keys = jnp.einsum(
            "hqk,qhd->khd", grad_scores, query_rot, preferred_element_type=jnp.float32
        ) * HEAD_DIM ** (-0.5)
        grad_kv = jnp.stack(
            [grad_keys.reshape(key_count, model_width), grad_values.reshape(key_count, model_width)]
        )
        grad_kv_own = grad_kv[:, hop_count * row_count : (hop_count + 1) * row_count]
        for slot_index in range(2 * hop_count + 1):
            offset = slot_index - hop_count
            if offset != 0:
                slot_grad = grad_kv[:, slot_index * row_count : (slot_index + 1) * row_count]
                grad_kv_own = grad_kv_own + passed_along(
                    slot_grad.astype(jnp.bfloat16), "seq", offset
                ).astype(slot_grad.dtype)
        grad_q_plain = rotate_back(grad_query, cos_table, sine_table).reshape(
            row_count, model_width
        )
        grad_k_plain = rotate_back(
            grad_kv_own[0].reshape(row_count, HEADS, HEAD_DIM), cos_table, sine_table
        ).reshape(row_count, model_width)
        grad_qkv = jnp.concatenate([grad_q_plain, grad_k_plain, grad_kv_own[1]], axis=1).astype(
            jnp.bfloat16
        )
        grad_normed_one = jnp.einsum(
            "tf,df->td", grad_qkv, weights[0], preferred_element_type=jnp.float32
        )
        gain_one_total = gain_one_total + jnp.sum(grad_normed_one * resid_in * inv_one, axis=0)
        grad_input = grad_mid + norm_back(grad_normed_one * gain_one, resid_in, inv_one)
        input_grads.append(grad_input.astype(jnp.bfloat16))
        pieces = (
            normed_one,
            grad_qkv,
            attended,
            grad_branch,
            normed_two,
            grad_gate,
            grad_up,
            hidden,
            grad_ffn,
        )
        saved.append(pieces)
    joined = tuple(
        (
            jnp.concatenate([entry[index] for entry in saved], axis=0)
            for index in range(len(saved[0]))
        )
    )
    grad_totals = reduce_last(weight_grads(joined))
    bias_sum, gain_one_sum, gain_two_sum = lax.psum(
        (bias_total, gain_one_total, gain_two_total), ("dp", "seq")
    )
    return (
        jnp.stack(outputs),
        jnp.stack(input_grads),
        grad_totals[0],
        grad_totals[1],
        grad_totals[2],
        grad_totals[3],
        grad_totals[4],
        gain_one_sum,
        gain_two_sum,
        bias_sum,
    )


MESH = pl.DeviceIdType.MESH
VM = pl.BlockSpec(memory_space=pltpu.VMEM)
HB = pl.BlockSpec(memory_space=pl.ANY)
SM = pl.BlockSpec(memory_space=pltpu.SMEM)
DMA = pltpu.SemaphoreType.DMA
NT = (((1,), (1,)), ((), ()))
TN = (((0,), (0,)), ((), ()))
EVERY = slice(None)


def bf16(*shape):
    return jax.ShapeDtypeStruct(shape, jnp.bfloat16)


def f32(*shape):
    return jax.ShapeDtypeStruct(shape, jnp.float32)


def dot(a, b, dims=None, out=jnp.float32):
    dims = (((1,), (0,)), ((), ())) if dims is None else dims
    return lax.dot_general(a, b, dims, preferred_element_type=jnp.float32).astype(out)


def at(dp, seq):
    return {"dp": dp, "seq": seq}


def place():
    return lax.axis_index("dp"), lax.axis_index("seq")


def ring(i):
    return i + 1 - 2 * lax.rem(i, 2), lax.rem(i + 2, 4)


def owned(i, s):
    return 4 * lax.rem(i, 2) + 2 * s + i // 2


def keeper(j):
    return 2 * lax.rem(j, 2) + j // 4


def send(src, dst, send_sem, recv_sem, peer):
    return pltpu.make_async_remote_copy(
        src_ref=src,
        dst_ref=dst,
        send_sem=send_sem,
        recv_sem=recv_sem,
        device_id=peer,
        device_id_type=MESH,
    )


def landed(ref, sem):
    pltpu.make_async_copy(ref, ref, sem).wait()


def meet(peers, home=False):
    i, j = place()
    barrier = pltpu.get_barrier_semaphore()
    for peer in peers:
        pl.semaphore_signal(barrier, inc=1, device_id=peer, device_id_type=MESH)
    if home:
        target, stays = keeper(j), keeper(j) == i
        for s in (0, 1):

            @pl.when(jnp.logical_not(stays & (owned(i, s) == j)))
            def _():
                pl.semaphore_signal(
                    barrier, inc=1, device_id=at(target, owned(i, s)), device_id_type=MESH
                )

        pl.semaphore_wait(barrier, len(peers) + jnp.where(stays, 1, 2))
    else:
        pl.semaphore_wait(barrier, len(peers))


def dp_peers():
    i, j = place()
    return [at(lax.rem(i + step, 4), j) for step in (1, 2, 3)]


def seq_peers():
    i, j = place()
    z, y = j // 2, lax.rem(j, 2)
    return [at(i, 2 * lax.rem(z + step, 4) + y) for step in (1, 2, 3)] + [at(i, 2 * z + 1 - y)]


class Home:
    def __init__(self, ins, outs, sems, slotted):
        self.ins, self.outs, self.slotted = ins, outs, slotted
        self.send_sem, self.recv_sem = sems

    @staticmethod
    def sems(count):
        return [DMA((count, 2)), DMA((count, 2))]

    def target(self, a, s):
        i, _ = place()
        return self.outs[a].at[s if self.slotted else owned(i, s)]

    def start(self, a, s):
        i, j = place()
        slot = lax.rem(j // 2, 2)
        src, dst = self.ins[a].at[s], self.outs[a].at[slot if self.slotted else j]
        here = (keeper(j) == i) & (owned(i, s) == j)

        @pl.when(jnp.logical_not(here))
        def _():
            peer = at(keeper(j), owned(i, s))
            send(src, dst, self.send_sem.at[a, s], self.recv_sem.at[a, slot], peer).start()

        @pl.when(here)
        def _():
            pltpu.make_async_copy(src, dst, self.recv_sem.at[a, slot]).start()

    def wait(self, a, s):
        landed(self.target(a, s), self.recv_sem.at[a, s])

    def finish(self, a):
        i, j = place()
        for s in (0, 1):

            @pl.when(jnp.logical_not((keeper(j) == i) & (owned(i, s) == j)))
            def _():
                landed(self.ins[a].at[s], self.send_sem.at[a, s])


class GroupGather:
    def __init__(self, outs, sems):
        self.outs = outs
        self.s_core, self.r_core, self.s_x, self.r_x, self.s_on, self.r_on = sems

    @staticmethod
    def sems(count):
        return [DMA((count, 2))] * 6

    def push(self, a, s):
        i, j = place()
        core, across = ring(i)
        block = self.outs[a].at[owned(i, s)]
        send(block, block, self.s_x.at[a, s], self.r_x.at[a, s], at(across, j)).start()
        send(block, block, self.s_core.at[a, s], self.r_core.at[a, s], at(core, j)).start()

    def relay(self, a, s):
        i, j = place()
        core, across = ring(i)
        block = self.outs[a].at[owned(across, s)]
        landed(block, self.r_x.at[a, s])
        send(block, block, self.s_on.at[a, s], self.r_on.at[a, s], at(core, j)).start()

    def finish(self, a):
        i, _ = place()
        core, _ = ring(i)
        for s in (0, 1):
            landed(self.outs[a].at[owned(core, s)], self.r_core.at[a, s])
            landed(self.outs[a].at[owned(lax.rem(core + 2, 4), s)], self.r_on.at[a, s])
        for s in (0, 1):
            for sem in (self.s_x, self.s_core, self.s_on):
                landed(self.outs[a].at[s], sem.at[a, s])


class GroupSum:
    def __init__(self, parts, scratch):
        self.parts = parts
        self.near, self.out, self.far = scratch[:3]
        self.s_core, self.r_core, self.s_x, self.r_x = scratch[3:]

    @staticmethod
    def scratch(count):
        block = (128, 1024)
        return [
            pltpu.VMEM((count, 2, 2) + block, jnp.bfloat16),
            pltpu.VMEM((count, 2) + block, jnp.bfloat16),
            pltpu.VMEM((count, 2) + block, jnp.bfloat16),
            DMA((count, 2, 2)),
            DMA((count, 2, 2)),
            DMA((count, 2)),
            DMA((count, 2)),
        ]

    def start(self, a):
        i, j = place()
        core, _ = ring(i)
        for side, owner in ((0, lax.rem(core + 2, 4)), (1, core)):
            for s in (0, 1):
                send(
                    self.parts[a].at[owned(owner, s)],
                    self.near.at[a, side, s],
                    self.s_core.at[a, side, s],
                    self.r_core.at[a, side, s],
                    at(core, j),
                ).start()

    def cross(self, a, s):
        i, j = place()
        _, across = ring(i)
        landed(self.near.at[a, 0, s], self.r_core.at[a, 0, s])
        both = self.parts[a][owned(across, s)].astype(jnp.float32)
        both = both + self.near[a, 0, s].astype(jnp.float32)
        self.out[a, s] = both.astype(jnp.bfloat16)
        send(
            self.out.at[a, s], self.far.at[a, s], self.s_x.at[a, s], self.r_x.at[a, s], at(across, j)
        ).start()

    def total(self, a, s):
        i, _ = place()
        landed(self.near.at[a, 1, s], self.r_core.at[a, 1, s])
        both = self.parts[a][owned(i, s)].astype(jnp.float32)
        both = both + self.near[a, 1, s].astype(jnp.float32)
        landed(self.far.at[a, s], self.r_x.at[a, s])
        return both + self.far[a, s].astype(jnp.float32)

    def finish(self, a):
        for s in (0, 1):
            landed(self.out.at[a, s], self.s_x.at[a, s])
            for side in (0, 1):
                landed(self.near.at[a, side, s], self.s_core.at[a, side, s])


class Exchange:
    def __init__(self, pieces, sems):
        self.pieces = pieces
        self.send_sem, self.recv_sem, self.own_sem = sems
        self.copies = []

    @staticmethod
    def sems(count):
        return [DMA((3, count)), DMA((3, count)), DMA((count,))]

    def start(self):
        i, j = place()
        for step in (2, 3, 1):
            other = lax.rem(i + step, 4)
            for index, (src, dst) in enumerate(self.pieces(i, other)):
                copy = send(
                    src,
                    dst,
                    self.send_sem.at[step - 1, index],
                    self.recv_sem.at[step - 1, index],
                    at(other, j),
                )
                copy.start()
                self.copies.append(copy)
        for index, (src, dst) in enumerate(self.pieces(i, i)):
            copy = pltpu.make_async_copy(src, dst, self.own_sem.at[index])
            copy.start()
            self.copies.append(copy)

    def wait(self):
        for copy in self.copies:
            copy.wait()


class SeqGather:
    def __init__(self, full, chunks, sems):
        self.full, self.chunks = full, chunks
        self.s_z, self.r_z, self.s_y, self.r_y = sems

    @staticmethod
    def sems(count):
        return [DMA((count, 3)), DMA((count, 3)), DMA((count, 4)), DMA((count, 4))]

    def block(self, chunk, z, y):
        start, size = self.chunks[chunk]
        return self.full.at[2 * z + y, pl.ds(start, size)]

    def start(self, chunk):
        i, j = place()
        z, y = j // 2, lax.rem(j, 2)
        own = self.block(chunk, z, y)
        for dz in (2, 1, 3):
            peer = at(i, 2 * lax.rem(z + dz, 4) + y)
            send(own, own, self.s_z.at[chunk, dz - 1], self.r_z.at[chunk, dz - 1], peer).start()
        send(own, own, self.s_y.at[chunk, 0], self.r_y.at[chunk, 0], at(i, 2 * z + 1 - y)).start()

    def forward(self, chunk, dz):
        i, j = place()
        z, y = j // 2, lax.rem(j, 2)
        block = self.block(chunk, lax.rem(z + 4 - dz, 4), y)
        landed(block, self.r_z.at[chunk, dz - 1])
        peer = at(i, 2 * z + 1 - y)
        send(block, block, self.s_y.at[chunk, dz], self.r_y.at[chunk, dz], peer).start()

    def finish(self, chunk):
        _, j = place()
        z, y = j // 2, lax.rem(j, 2)
        own = self.block(chunk, z, y)
        for dz in (0, 1, 2, 3):
            landed(self.block(chunk, lax.rem(z + 4 - dz, 4), 1 - y), self.r_y.at[chunk, dz])
            landed(own, self.s_y.at[chunk, dz])
            if dz:
                landed(own, self.s_z.at[chunk, dz - 1])


class SeqSum:
    def __init__(self, parts, mine, chunks, scratch):
        self.parts, self.mine, self.chunks = parts, mine, chunks
        self.near, self.out, self.far = scratch[:3]
        self.s_y, self.r_y, self.s_z, self.r_z = scratch[3:]

    @staticmethod
    def scratch(rows, count):
        return [
            pltpu.VMEM((4, rows, 128), jnp.bfloat16),
            pltpu.VMEM((3, rows, 128), jnp.bfloat16),
            pltpu.VMEM((3, rows, 128), jnp.bfloat16),
            DMA((count, 4)),
            DMA((count, 4)),
            DMA((count, 3)),
            DMA((count, 3)),
        ]

    def rows(self, chunk):
        return pl.ds(*self.chunks[chunk])

    def start(self, chunk):
        i, j = place()
        z, y = j // 2, lax.rem(j, 2)
        rows = self.rows(chunk)
        for dz in (2, 1, 3, 0):
            send(
                self.parts.at[2 * lax.rem(z + dz, 4) + 1 - y, rows],
                self.near.at[dz, rows],
                self.s_y.at[chunk, dz],
                self.r_y.at[chunk, dz],
                at(i, 2 * z + 1 - y),
            ).start()

    def cross(self, chunk, dz):
        i, j = place()
        z, y = j // 2, lax.rem(j, 2)
        start, size = self.chunks[chunk]
        rows = self.rows(chunk)
        landed(self.near.at[dz, rows], self.r_y.at[chunk, dz])
        self.add(2 * lax.rem(z + dz, 4) + y, dz, start, size)
        send(
            self.out.at[dz - 1, rows],
            self.far.at[dz - 1, rows],
            self.s_z.at[chunk, dz - 1],
            self.r_z.at[chunk, dz - 1],
            at(i, 2 * lax.rem(z + dz, 4) + y),
        ).start()

    def add(self, block, dz, start, size):
        @pl.loop(0, size // 256)
        def _(t):
            rows = pl.ds(pl.multiple_of(start + t * 256, 256), 256)
            both = self.mine[block // 2, rows, :].astype(jnp.float32)
            both = both + self.near[dz, rows, :].astype(jnp.float32)
            self.out[dz - 1, rows, :] = both.astype(jnp.bfloat16)

    def finish(self, chunk, store):
        _, j = place()
        start, size = self.chunks[chunk]
        rows = self.rows(chunk)
        landed(self.near.at[0, rows], self.r_y.at[chunk, 0])
        for dz in (1, 2, 3):
            landed(self.far.at[dz - 1, rows], self.r_z.at[chunk, dz - 1])

        @pl.loop(0, size // 256)
        def _(t):
            part = pl.ds(pl.multiple_of(start + t * 256, 256), 256)
            total = self.mine[j // 2, part, :].astype(jnp.float32)
            total = total + self.near[0, part, :].astype(jnp.float32)
            for dz in (1, 2, 3):
                total = total + self.far[dz - 1, part, :].astype(jnp.float32)
            store(part, total)

    def drain(self, chunk):
        rows = self.rows(chunk)
        for dz in (0, 1, 2, 3):
            landed(self.near.at[dz, rows], self.s_y.at[chunk, dz])
            if dz:
                landed(self.out.at[dz - 1, rows], self.s_z.at[chunk, dz - 1])


def swap_halves(x):
    lane = lax.broadcasted_iota(jnp.int32, x.shape, 1)
    width = x.shape[1]
    return jnp.where(lane % 64 < 32, pltpu.roll(x, width - 32, 1), pltpu.roll(x, 32, 1))


def angle_tables(table):
    lane = lax.broadcasted_iota(jnp.int32, table.shape, 1)
    by_32, by_64, by_96 = (pltpu.roll(table, shift, 1) for shift in (32, 64, 96))
    first, second, third = lane < 32, lane < 64, lane < 96
    cos_t = jnp.where(first, table, jnp.where(second, by_32, jnp.where(third, by_64, by_96)))
    sin_t = jnp.where(first, -by_96, jnp.where(second, table, jnp.where(third, -by_32, by_64)))
    return cos_t, sin_t


SLOTS = (
    (0, 1, 2, 4, 5, 6, 8, 9, 10, 12, 13, 14),
    (0, 2, 3, 4, 6, 7, 8, 10, 11, 12, 14, 15),
)


def attention_pieces(packed, w_out, dst):
    def pieces(me, other):
        _, j = place()
        spot = lax.rem(other + 2 * lax.rem(j, 2), 4)
        return [
            (packed.at[spot], dst.at[j, pl.ds(256 * me, 256)]),
            (w_out.at[pl.ds(64 * other, 64)], dst.at[j, pl.ds(1024 + 64 * me, 64)]),
        ]

    return pieces


def ffn_pieces(w_gate, w_up, w_down, dst):
    def pieces(me, other):
        _, j = place()
        columns = pl.ds(pl.multiple_of(128 * other, 128), 128)
        pairs = [
            (w_gate.at[:, columns], dst.at[j, pl.ds(256 * me, 256)]),
            (w_up.at[:, columns], dst.at[j, pl.ds(1024 + 256 * me, 256)]),
        ]
        for half in (0, 1):
            pairs.append(
                (
                    w_down.at[pl.ds(512 * half + 128 * other, 128)],
                    dst.at[j, pl.ds(2048 + 256 * me + 128 * half, 128)],
                )
            )
        return pairs

    return pieces


def head_weights(full, wh_ref, wm_ref, low_half):
    def column(m, rows):
        first, second = SLOTS[0][m], SLOTS[1][m]
        one = full[first // 2, rows, 64 * (first % 2) : 64 * (first % 2) + 64]
        two = full[second // 2, rows, 64 * (second % 2) : 64 * (second % 2) + 64]
        return jnp.where(low_half, one, two)

    @pl.loop(0, 4)
    def _(t):
        rows = pl.ds(pl.multiple_of(t * 256, 256), 256)
        for m in range(0, 12, 2):
            wh_ref[rows, 64 * m : 64 * m + 128] = jnp.concatenate(
                [column(m, rows), column(m + 1, rows)], axis=1
            )

    for b in range(8):
        wm_ref[:, 128 * b : 128 * b + 128] = full[b, 1024:1280, :]


def norm_rows(hidden):
    return lax.rsqrt(jnp.mean(hidden * hidden, axis=1, keepdims=True) + EPSILON)


FFN_CHUNKS = ((0, 1024), (1024, 1024), (2048, 1024))


def open_kernel(*refs):
    (tok, cot, tab, idr, packed, w_out, w_gate, w_up, w_down, gain_one, gain_two, bias), refs = (
        refs[:12],
        refs[12:],
    )
    (
        tok_all, cot_all, tab_all, idr_all, a1_ref, q_ref, k_ref, v_ref, o_ref, lse_ref,
        wh_ref, wm_ref, mid_ref, a2_all, ffn_all,
    ), refs = refs[:15], refs[15:]
    (attn_all, part, cos_ref, sin_ref, rows_ref), refs = refs[:5], refs[5:]
    home_sems, refs = refs[:2], refs[2:]
    gather_sems, refs = refs[:6], refs[6:]
    a2_sems, refs = refs[:6], refs[6:]
    sum_scratch, refs = refs[:7], refs[7:]
    spread_a, spread_f, refs = refs[:3], refs[3:6], refs[6:]
    chain_a, chain_f = refs[:4], refs[4:8]

    i, _ = place()
    home = Home((tok, tab, idr, cot), (tok_all, tab_all, idr_all, cot_all), home_sems, False)
    group = GroupGather((tok_all, tab_all, idr_all, cot_all), gather_sems)
    spread = Exchange(attention_pieces(packed, w_out, attn_all), spread_a)
    spread_ffn = Exchange(ffn_pieces(w_gate, w_up, w_down, ffn_all), spread_f)
    attn_w = SeqGather(attn_all, ((0, 1280),), chain_a)
    ffn_w = SeqGather(ffn_all, FFN_CHUNKS, chain_f)
    branch = GroupSum((part,), sum_scratch)
    second = GroupGather((a2_all,), a2_sems)

    meet(dp_peers() + seq_peers(), home=True)
    for a in (0, 1, 2):
        for s in (0, 1):
            home.start(a, s)
    spread.start()
    spread_ffn.start()
    spread.wait()
    attn_w.start(0)
    for a in (0, 1, 2):
        for s in (0, 1):
            home.wait(a, s)
            group.push(a, s)
    for s in (0, 1):
        home.start(3, s)
    spread_ffn.wait()
    for chunk in range(3):
        ffn_w.start(chunk)
    for a in (0, 1, 2):
        for s in (0, 1):
            group.relay(a, s)
    for a in (0, 1, 2):
        group.finish(a)
        home.finish(a)

    for b in range(8):
        rows_ref[:, 128 * b : 128 * b + 128] = idr_all[b]

    @pl.loop(0, 8)
    def _(b):
        rows = pl.ds(pl.multiple_of(b * 128, 128), 128)
        hidden = tok_all[b].astype(jnp.float32)
        a1_ref[rows, :] = (hidden * norm_rows(hidden) * gain_one[...]).astype(jnp.bfloat16)
        cos_t, sin_t = angle_tables(tab_all[b])
        cos_ref[rows, :] = cos_t
        sin_ref[rows, :] = sin_t

    for dz in (1, 2, 3):
        attn_w.forward(0, dz)
    for s in (0, 1):
        home.wait(3, s)
        group.push(3, s)
    attn_w.finish(0)
    head_weights(attn_all, wh_ref, wm_ref, i < 2)

    @pl.loop(0, 4)
    def _(t):
        rows = pl.ds(pl.multiple_of(t * 256, 256), 256)
        proj = dot(a1_ref[rows, :], wh_ref[...])
        cos_t, sin_t = cos_ref[rows, :], sin_ref[rows, :]
        for pair in (0, 1):
            cols = slice(128 * pair, 128 * pair + 128)
            for base, out in ((0, q_ref), (256, k_ref)):
                x = proj[:, base + 128 * pair : base + 128 * pair + 128]
                out[rows, cols] = (x * cos_t + swap_halves(x) * sin_t).astype(jnp.bfloat16)
        v_ref[rows, :] = proj[:, 512:768].astype(jnp.bfloat16)

    for s in (0, 1):
        group.relay(3, s)

    @pl.loop(0, 4)
    def _(t):
        start = pl.multiple_of(t * 256, 256)
        rows = pl.ds(start, 256)
        columns = tab_all[pl.ds(2 * t, 2)].reshape(256, 128)
        seg_q, var_q = columns[:, 64:65], columns[:, 65:66]
        code_k, var_k = rows_ref[0:1, :], rows_ref[1:2, :]
        row = start + lax.broadcasted_iota(jnp.int32, (256, 1024), 0)
        col = lax.broadcasted_iota(jnp.int32, (256, 1024), 1)
        allowed = ((seg_q == code_k) & (jnp.abs(row - col) <= WINDOW)) | (row == col)
        masked = jnp.where(allowed, 0.0, NEGATIVE)
        same = jnp.where(var_q == var_k, 1.0, 0.0)
        stats = jnp.zeros((256, 128), jnp.float32)
        lane = lax.broadcasted_iota(jnp.int32, (256, 128), 1)
        for h in range(4):
            cols = slice(64 * h, 64 * h + 64)
            scores = dot(q_ref[rows, cols] * 0.125, k_ref[:, cols], NT)
            scores = scores + bias[h] * same + masked
            top = jnp.max(scores, axis=1, keepdims=True)
            weight = jnp.exp(scores - top)
            total = jnp.sum(weight, axis=1, keepdims=True)
            mixed = dot(weight.astype(jnp.bfloat16), v_ref[:, cols])
            o_ref[rows, cols] = (mixed / total).astype(jnp.bfloat16)
            stats = jnp.where(lane == h, top + jnp.log(total), stats)
        lse_ref[:, rows] = stats.T[:8]
        part[pl.ds(2 * t, 2)] = dot(o_ref[rows, :], wm_ref[...], out=jnp.bfloat16).reshape(2, 128, 1024)

    branch.start(0)
    for dz in (1, 2, 3):
        ffn_w.forward(0, dz)
    for s in (0, 1):
        branch.cross(0, s)
    for s in (0, 1):
        block = owned(i, s)
        mid = tok_all[block].astype(jnp.float32) + branch.total(0, s)
        mid_ref[s] = mid
        a2_all[block] = (mid * norm_rows(mid) * gain_two[...]).astype(jnp.bfloat16)
        second.push(0, s)
    for dz in (1, 2, 3):
        ffn_w.forward(1, dz)
    for s in (0, 1):
        second.relay(0, s)
    branch.finish(0)
    second.finish(0)
    group.finish(3)
    home.finish(3)
    for dz in (1, 2, 3):
        ffn_w.forward(2, dz)
    for chunk in range(3):
        ffn_w.finish(chunk)


def open_phase(arrays):
    f32_rows = pltpu.VMEM((1024, 128), jnp.float32)
    return pl.pallas_call(
        open_kernel,
        out_shape=[
            bf16(8, 128, 1024),
            bf16(8, 128, 1024),
            f32(8, 128, 128),
            f32(8, 8, 128),
            bf16(1024, 1024),
            bf16(1024, 256),
            bf16(1024, 256),
            bf16(1024, 256),
            bf16(1024, 256),
            f32(8, 1024),
            bf16(1024, 768),
            bf16(256, 1024),
            f32(2, 128, 1024),
            bf16(8, 128, 1024),
            bf16(8, 3072, 128),
        ],
        in_specs=[VM, HB, VM, VM, VM, VM, HB, HB, HB, VM, VM, SM],
        out_specs=[VM, HB] + [VM] * 12 + [HB],
        scratch_shapes=[
            pltpu.VMEM((8, 1280, 128), jnp.bfloat16),
            pltpu.VMEM((8, 128, 1024), jnp.bfloat16),
            f32_rows,
            f32_rows,
            pltpu.VMEM((8, 1024), jnp.float32),
        ]
        + Home.sems(4)
        + GroupGather.sems(4)
        + GroupGather.sems(1)
        + GroupSum.scratch(1)
        + Exchange.sems(2)
        + Exchange.sems(4)
        + SeqGather.sems(1)
        + SeqGather.sems(3),
        compiler_params=pltpu.CompilerParams(
            collective_id=1, has_side_effects=True, vmem_limit_bytes=56 << 20
        ),
        name="open_phase",
    )(*arrays)


def comm_call(kernel, outs, scratch, collective_id, in_count, vmem=None):
    return pl.pallas_call(
        kernel,
        out_shape=outs,
        in_specs=[VM] * in_count,
        out_specs=[VM] * len(outs),
        scratch_shapes=scratch,
        compiler_params=pltpu.CompilerParams(
            collective_id=collective_id, has_side_effects=True, vmem_limit_bytes=vmem
        ),
    )


def grad_pieces(kind, src, dst, me, other, seq):
    if kind == "attention":
        g_qkv, g_out = dst
        place = lax.rem(me + 2 * lax.rem(seq, 2), 4)
        return [
            (src.at[pl.ds(256 * other, 256)], g_qkv.at[place]),
            (src.at[pl.ds(1024 + 64 * other, 64)], g_out.at[pl.ds(64 * me, 64)]),
        ]
    g_gate, g_up, g_down = dst
    columns = pl.ds(pl.multiple_of(128 * me, 128), 128)
    pairs = [
        (src.at[pl.ds(256 * other, 256)], g_gate.at[:, columns]),
        (src.at[pl.ds(1024 + 256 * other, 256)], g_up.at[:, columns]),
    ]
    for half in (0, 1):
        pairs.append(
            (
                src.at[pl.ds(2048 + 256 * other + 128 * half, 128)],
                g_down.at[pl.ds(512 * half + 128 * me, 128)],
            )
        )
    return pairs


def exchange_kernel(pieces, n_in, n_out, *refs):
    ins, outs = refs[:n_in], refs[n_in : n_in + n_out]
    send_sem, recv_sem, own_sem = refs[n_in + n_out :]
    me, seq = lax.axis_index("dp"), lax.axis_index("seq")
    others = [lax.rem(me + step, 4) for step in (1, 2, 3)]
    meet([at(other, seq) for other in others])
    copies = []
    for step, other in enumerate(others):
        for index, (src, dst) in enumerate(pieces(ins, outs, me, other, seq)):
            copy = send(
                src, dst, send_sem.at[step, index], recv_sem.at[step, index], at(other, seq)
            )
            copy.start()
            copies.append(copy)
    own = [
        pltpu.make_async_copy(src, dst, own_sem.at[index])
        for index, (src, dst) in enumerate(pieces(ins, outs, me, me, seq))
    ]
    for copy in own:
        copy.start()
    for copy in own:
        copy.wait()
    for copy in copies:
        copy.wait()


def exchange(pieces, ins, outs, count, collective_id):
    kernel = functools.partial(exchange_kernel, pieces, len(ins), len(outs))
    return comm_call(
        kernel, outs, [DMA((3, count)), DMA((3, count)), DMA((count,))], collective_id, len(ins)
    )(*ins)


def home_kernel(count, *refs):
    ins, outs = refs[:count], refs[count : 2 * count]
    home = Home(ins, outs, refs[2 * count :], True)
    meet([], home=True)
    for a in range(count):
        for s in (0, 1):
            home.start(a, s)
    for a in range(count):
        for s in (0, 1):
            home.wait(a, s)
        home.finish(a)


def send_home(arrays, collective_id):
    count = len(arrays)
    return comm_call(
        functools.partial(home_kernel, count),
        [jax.ShapeDtypeStruct(v.shape, v.dtype) for v in arrays],
        Home.sems(count),
        collective_id,
        count,
    )(*arrays)


def local_call(kernel, outs, scratch, specs, vmem):
    return pl.pallas_call(
        kernel,
        out_shape=outs,
        in_specs=specs,
        out_specs=[VM] * len(outs),
        scratch_shapes=scratch,
        compiler_params=pltpu.CompilerParams(vmem_limit_bytes=vmem),
    )


def gather_kernel(count, *refs):
    ins, outs = refs[:count], refs[count : 2 * count]
    own_sem, s_core, r_core, s_x, r_x, s_on, r_on = refs[2 * count :]
    i, j = lax.axis_index("dp"), lax.axis_index("seq")
    core, across = ring(i)
    diagonal = lax.rem(core + 2, 4)
    meet([at(core, j), at(across, j)])
    pending = []
    for a in range(count):
        for s in (0, 1):
            for sems, peer in (((s_x, r_x), across), ((s_core, r_core), core)):
                copy = send(
                    ins[a].at[s],
                    outs[a].at[owned(i, s)],
                    sems[0].at[a, s],
                    sems[1].at[a, s],
                    at(peer, j),
                )
                copy.start()
                pending.append(copy)
            copy = pltpu.make_async_copy(ins[a].at[s], outs[a].at[owned(i, s)], own_sem.at[a, s])
            copy.start()
            pending.append(copy)
    onward = []
    for a in range(count):
        for s in (0, 1):
            block = outs[a].at[owned(across, s)]
            pltpu.make_async_copy(ins[a].at[s], block, r_x.at[a, s]).wait()
            copy = send(block, block, s_on.at[a, s], r_on.at[a, s], at(core, j))
            copy.start()
            onward.append(copy)
    for a in range(count):
        for s in (0, 1):
            pltpu.make_async_copy(ins[a].at[s], outs[a].at[owned(core, s)], r_core.at[a, s]).wait()
            pltpu.make_async_copy(ins[a].at[s], outs[a].at[owned(diagonal, s)], r_on.at[a, s]).wait()
    for index, copy in enumerate(pending):
        if index % 3 == 2:
            copy.wait()
        else:
            copy.wait_send()
    for copy in onward:
        copy.wait_send()


def gather_group(arrays, collective_id):
    count = len(arrays)
    return comm_call(
        functools.partial(gather_kernel, count),
        [jax.ShapeDtypeStruct((8,) + v.shape[1:], v.dtype) for v in arrays],
        [DMA((count, 2))] * 7,
        collective_id,
        count,
    )(*arrays)


def reduce_kernel(count, *refs):
    ins, outs = refs[:count], refs[count : 2 * count]
    from_core, to_x, from_x, s_core, r_core, s_x, r_x = refs[2 * count :]
    i, j = lax.axis_index("dp"), lax.axis_index("seq")
    core, across = ring(i)
    diagonal = lax.rem(core + 2, 4)
    meet([at(core, j), at(across, j)])
    pending = []
    for a in range(count):
        for side, owner in ((0, diagonal), (1, core)):
            for s in (0, 1):
                copy = send(
                    ins[a].at[owned(owner, s)],
                    from_core.at[a, side, s],
                    s_core.at[a, side, s],
                    r_core.at[a, side, s],
                    at(core, j),
                )
                copy.start()
                pending.append(copy)
    across_copies = []
    for a in range(count):
        for s in (0, 1):
            pltpu.make_async_copy(
                ins[a].at[s], from_core.at[a, 0, s], r_core.at[a, 0, s]
            ).wait()
            both = ins[a][owned(across, s)].astype(jnp.float32) + from_core[a, 0, s].astype(
                jnp.float32
            )
            to_x[a, s] = both.astype(jnp.bfloat16)
            copy = send(
                to_x.at[a, s], from_x.at[a, s], s_x.at[a, s], r_x.at[a, s], at(across, j)
            )
            copy.start()
            across_copies.append(copy)
    for a in range(count):
        for s in (0, 1):
            pltpu.make_async_copy(
                ins[a].at[s], from_core.at[a, 1, s], r_core.at[a, 1, s]
            ).wait()
            outs[a][s] = ins[a][owned(i, s)].astype(jnp.float32) + from_core[a, 1, s].astype(
                jnp.float32
            )
    for a in range(count):
        for s in (0, 1):
            pltpu.make_async_copy(ins[a].at[s], from_x.at[a, s], r_x.at[a, s]).wait()
            outs[a][s] = outs[a][s] + from_x[a, s].astype(jnp.float32)
    for copy in pending + across_copies:
        copy.wait_send()


def reduce_group(arrays, collective_id):
    count = len(arrays)
    _, rows, width = arrays[0].shape
    block = (rows, width)
    return comm_call(
        functools.partial(reduce_kernel, count),
        [f32(2, rows, width) for _ in arrays],
        [
            pltpu.VMEM((count, 2, 2) + block, jnp.bfloat16),
            pltpu.VMEM((count, 2) + block, jnp.bfloat16),
            pltpu.VMEM((count, 2) + block, jnp.bfloat16),
            DMA((count, 2, 2)),
            DMA((count, 2, 2)),
            DMA((count, 2)),
            DMA((count, 2)),
        ],
        collective_id,
        count,
    )(*arrays)


def small_sum_kernel(x_ref, o_ref, first, second, s_sem, r_sem, s_sem2, r_sem2):
    i, j = lax.axis_index("dp"), lax.axis_index("seq")
    groups = [at(lax.rem(i + step, 4), j) for step in (1, 2, 3)]
    chains = [at(i, lax.rem(j + step, 8)) for step in range(1, 8)]
    meet(groups + chains)
    copies = []
    for step, peer in enumerate(groups):
        copy = send(x_ref, first.at[i], s_sem.at[step], r_sem.at[step], peer)
        copy.start()
        copies.append(copy)
    first[i] = x_ref[...]
    for copy in copies:
        copy.wait()
    second[j] = (first[0] + first[1]) + (first[2] + first[3])
    copies = []
    for step, peer in enumerate(chains):
        copy = send(second.at[j], second.at[j], s_sem2.at[step], r_sem2.at[step], peer)
        copy.start()
        copies.append(copy)
    for copy in copies:
        copy.wait()
    total = second[0]
    for step in range(1, 8):
        total = total + second[step]
    o_ref[...] = total


def small_sum(x, collective_id):
    return comm_call(
        small_sum_kernel,
        [jax.ShapeDtypeStruct(x.shape, x.dtype)],
        [
            pltpu.VMEM((4,) + x.shape, x.dtype),
            pltpu.VMEM((8,) + x.shape, x.dtype),
            DMA((3,)),
            DMA((3,)),
            DMA((7,)),
            DMA((7,)),
        ],
        collective_id,
        1,
    )(x)[0]


def wide(ref, first, rows):
    return jnp.concatenate([ref[first, rows, :], ref[first + 1, rows, :]], axis=1)


def store_wide(ref, first, rows, value):
    ref[first, rows, :] = value[:, :128]
    ref[first + 1, rows, :] = value[:, 128:]


def ffn_kernel(
    a_ref, g_ref, wg_ref, wu_ref, wd_ref,
    da_ref, out_ref, gg_ref, gu_ref, gd_ref,
    turned, da_acc, out_acc, hidden_s, dgate_s, dup_s,
):
    step, last = pl.program_id(0), pl.num_programs(0) - 1

    @pl.when(step == 0)
    def _():
        @pl.loop(0, 4)
        def _(t):
            rows = pl.ds(pl.multiple_of(t * 256, 256), 256)
            for d in range(4):
                cols = slice(256 * d, 256 * d + 256)
                turned[cols, rows] = a_ref[rows, cols].T

    wg, wu = wide(wg_ref, 0, EVERY), wide(wu_ref, 0, EVERY)
    wd = jnp.concatenate([wd_ref[b] for b in range(8)], axis=1)

    @pl.loop(0, 4)
    def _(t):
        rows = pl.ds(pl.multiple_of(t * 256, 256), 256)
        a, g = a_ref[rows, :], g_ref[rows, :]
        gate, up, dh = dot(a, wg), dot(a, wu), dot(g, wd, NT)
        sig = 1.0 / (1.0 + jnp.exp(-gate))
        gate_sig = gate * sig
        hidden = (gate_sig * up).astype(jnp.bfloat16)
        dgate = (dh * up * (sig + gate_sig * (1.0 - sig))).astype(jnp.bfloat16)
        dup = (dh * gate_sig).astype(jnp.bfloat16)
        hidden_s[rows, :] = hidden
        dgate_s[rows, :] = dgate
        dup_s[rows, :] = dup
        da = dot(dgate, wg, NT) + dot(dup, wu, NT)
        out = dot(hidden, wd)

        @pl.when(step == 0)
        def _():
            da_acc[rows, :] = da
            out_acc[rows, :] = out

        @pl.when(step > 0)
        def _():
            da_acc[rows, :] += da
            out_acc[rows, :] += out

    @pl.loop(0, 4)
    def _(d):
        rows = pl.ds(pl.multiple_of(d * 256, 256), 256)
        a_t = turned[rows, :]
        store_wide(gg_ref, 0, rows, dot(a_t, dgate_s[...], out=jnp.bfloat16))
        store_wide(gu_ref, 0, rows, dot(a_t, dup_s[...], out=jnp.bfloat16))

    h_t = hidden_s[...].T
    for d in range(4):
        store_wide(gd_ref, 2 * d, EVERY, dot(h_t, g_ref[:, 256 * d : 256 * d + 256], out=jnp.bfloat16))

    @pl.when(step == last)
    def _():
        da_ref[...] = da_acc[...].astype(jnp.bfloat16)
        out_ref[...] = out_acc[...].astype(jnp.bfloat16)


def ffn(a2, g_low, weights):
    tile = (2, 1024, 128)
    grads = [
        pl.BlockSpec(tile, lambda f: (f, 0, 0)),
        pl.BlockSpec(tile, lambda f: (f, 0, 0)),
        pl.BlockSpec((8, 256, 128), lambda f: (0, f, 0)),
    ]
    whole = pl.BlockSpec((1024, 1024), lambda f: (0, 0))
    return pl.pallas_call(
        ffn_kernel,
        grid=(4,),
        out_shape=[bf16(1024, 1024)] * 2 + [bf16(8, 1024, 128)] * 3,
        in_specs=[
            whole,
            whole,
            pl.BlockSpec(tile, lambda f: (f, 0, 0)),
            pl.BlockSpec(tile, lambda f: (f, 1, 0)),
            pl.BlockSpec((8, 256, 128), lambda f: (0, 8 + f, 0)),
        ],
        out_specs=[whole, whole] + grads,
        scratch_shapes=[pltpu.VMEM((1024, 1024), jnp.bfloat16)]
        + [pltpu.VMEM((1024, 1024), jnp.float32)] * 2
        + [pltpu.VMEM((1024, 256), jnp.bfloat16)] * 3,
        compiler_params=pltpu.CompilerParams(vmem_limit_bytes=52 << 20),
        name="ffn",
    )(a2, g_low, weights, weights, weights)


def attention_back_kernel(
    q_ref, k_ref, v_ref, do_ref, lse_ref, cos_ref, sin_ref, idc_ref, idr_ref, bias_ref,
    dqkv_ref, dbias_ref, dq_acc, dk_acc, dv_acc,
):
    dk_acc[...] = jnp.zeros_like(dk_acc)
    dv_acc[...] = jnp.zeros_like(dv_acc)
    dbias_ref[...] = jnp.zeros_like(dbias_ref)

    @pl.loop(0, 4)
    def _(block):
        start = pl.multiple_of(block * 256, 256)
        rows = pl.ds(start, 256)
        code_k, var_k = idc_ref[:, 2:3], idc_ref[:, 1:2]
        seg_q, var_q = idr_ref[2:3, rows], idr_ref[1:2, rows]
        row = lax.broadcasted_iota(jnp.int32, (1024, 256), 0)
        col = start + lax.broadcasted_iota(jnp.int32, (1024, 256), 1)
        allowed = ((seg_q == code_k) & (jnp.abs(row - col) <= WINDOW)) | (row == col)
        masked = jnp.where(allowed, 0.0, NEGATIVE)
        same = jnp.where(var_q == var_k, 1.0, 0.0)
        for h in range(4):
            cols = slice(64 * h, 64 * h + 64)
            q_h, k_h, v_h = q_ref[rows, cols] * 0.125, k_ref[:, cols], v_ref[:, cols]
            do_h = do_ref[rows, cols]
            scores = lax.dot_general(k_h, q_h, NT, preferred_element_type=jnp.float32)
            scores = scores + bias_ref[h] * same + masked
            prob = jnp.exp(scores - lse_ref[h : h + 1, rows])
            dv_acc[:, cols] += jnp.dot(
                prob.astype(jnp.bfloat16), do_h, preferred_element_type=jnp.float32
            )
            dprob = lax.dot_general(v_h, do_h, NT, preferred_element_type=jnp.float32)
            mean = jnp.sum(prob * dprob, axis=0, keepdims=True)
            dscore = (prob * (dprob - mean)).astype(jnp.bfloat16)
            dbias_ref[h : h + 1, :] += jnp.sum(
                dscore.astype(jnp.float32) * same, axis=0, keepdims=True
            )
            dk_acc[:, cols] += jnp.dot(dscore, q_h, preferred_element_type=jnp.float32)
            dq_acc[rows, cols] = lax.dot_general(
                dscore, k_h, TN, preferred_element_type=jnp.float32
            ) * 0.125

    @pl.loop(0, 4)
    def _(block):
        rows = pl.ds(pl.multiple_of(block * 256, 256), 256)
        cos_t, sin_t = cos_ref[rows, :], sin_ref[rows, :]
        for pair in (0, 1):
            cols = slice(128 * pair, 128 * pair + 128)
            for base, acc in ((0, dq_acc), (256, dk_acc)):
                g = acc[rows, cols]
                dqkv_ref[rows, base + 128 * pair : base + 128 * pair + 128] = (
                    g * cos_t - swap_halves(g) * sin_t
                ).astype(jnp.bfloat16)
        dqkv_ref[rows, 512:768] = dv_acc[rows, :].astype(jnp.bfloat16)


def attention_back(q, k, v, do, lse, cos_t, sin_t, id_cols, id_rows, bias):
    return local_call(
        attention_back_kernel,
        [bf16(1024, 768), f32(8, 256)],
        [pltpu.VMEM((1024, 256), jnp.float32)] * 3,
        [VM] * 9 + [SM],
        48 << 20,
    )(q, k, v, do, lse, cos_t, sin_t, id_cols, id_rows, bias)


def on_group(
    tokens, segment_ids, variate_ids, time_ids, pad_mask, cotangent,
    w_qkv, w_out, w_gate, w_up, w_down, gain_attn, gain_ffn, variate_bias,
):
    i = lax.axis_index("dp")
    low_half = i < 2
    gain_one, gain_two = gain_attn.astype(jnp.float32), gain_ffn.astype(jnp.float32)

    packed = jnp.pad(w_qkv, ((0, 0), (0, 128))).reshape(256, 2, 4, 64)
    packed = packed.transpose(2, 0, 1, 3).reshape(4, 256, 128)
    frequency = jnp.exp(-jnp.log(10000.0) * jnp.arange(32, dtype=jnp.float32) / 32)
    angles = time_ids.astype(jnp.float32)[..., None] * frequency
    code_ids = jnp.where(pad_mask == 1, segment_ids, -1)
    labels = jnp.stack([segment_ids, variate_ids, code_ids], axis=-1).astype(jnp.float32)
    tables = jnp.concatenate(
        [jnp.cos(angles), jnp.sin(angles), labels, jnp.zeros((2, 128, 61), jnp.float32)], axis=-1
    )
    label_rows = jnp.stack([code_ids, variate_ids, segment_ids] + [segment_ids] * 5, axis=1)
    bias = jnp.where(
        jnp.arange(4)[None, :] == i, variate_bias.astype(jnp.float32).reshape(4, 4), 0.0
    ).sum(axis=1)
    (
        tok_all, cot_all, tab_all, idr_all, a1, q, k, v, attended, lse_rows,
        w_heads, w_mix, mid, a2, ffn_w,
    ) = open_phase(
        [
            tokens, cotangent, tables, label_rows.astype(jnp.float32), packed, w_out, w_gate, w_up, w_down,
            gain_one[None], gain_two[None], bias,
        ]
    )
    g_low = cot_all.reshape(1024, 1024)
    a2 = a2.reshape(1024, 1024)
    mid = mid.reshape(256, 1024)
    inv_two = norm_scale(mid)

    def mine(blocks):
        return jnp.concatenate(
            [lax.dynamic_index_in_dim(blocks, owned(i, s), 0, False) for s in (0, 1)]
        ).astype(jnp.float32)

    own, own_cot = mine(tok_all), mine(cot_all)
    inv_one = norm_scale(own)
    table = tab_all.reshape(1024, 128)
    cos_t = jnp.concatenate([table[:, :32]] * 4, axis=1)
    sin_t = jnp.concatenate([-table[:, 32:64], table[:, 32:64]] * 2, axis=1)
    id_cols = jnp.pad(table[:, 64:67], ((0, 0), (0, 125)))
    id_rows = idr_all.transpose(1, 0, 2).reshape(8, 1024)
    da2_part, out_part, g_gate, g_up, g_down = ffn(a2, g_low, ffn_w)
    ffn_grads = jnp.concatenate([g_gate, g_up, g_down], axis=1)
    ffn_sum = lax.psum_scatter(ffn_grads, "seq", scatter_dimension=0)
    da2, ffn_out = reduce_group([da2_part.reshape(8, 128, 1024), out_part.reshape(8, 128, 1024)], 7)

    def blocks(g):
        return g.astype(jnp.bfloat16).reshape(-1, 8, 128).transpose(1, 0, 2)

    da2 = da2.reshape(256, 1024)
    output = (mid + ffn_out.reshape(256, 1024)).astype(jnp.bfloat16)
    grad_gain_two = jnp.sum(da2 * mid * inv_two, axis=0)
    e2 = own_cot + norm_back(da2 * gain_two, mid, inv_two)
    (ez,) = gather_group([e2.astype(jnp.bfloat16).reshape(2, 128, 1024)], 8)
    ez = ez.reshape(1024, 1024)
    do = dot(ez, w_mix, NT, jnp.bfloat16)
    dqkv, dbias = attention_back(q, k, v, do, lse_rows, cos_t, sin_t, id_cols, id_rows, bias)
    da1_part = dot(dqkv, w_heads, NT, jnp.bfloat16).reshape(8, 128, 1024)
    (da1,) = reduce_group([da1_part], 9)
    da1 = da1.reshape(256, 1024)
    grad_gain_one = jnp.sum(da1 * own * inv_one, axis=0)
    input_grad = (e2 + norm_back(da1 * gain_one, own, inv_one)).astype(jnp.bfloat16)
    output, input_grad = send_home(
        [output.reshape(2, 128, 1024), input_grad.reshape(2, 128, 1024)], 10
    )

    grad_heads = dot(a1, dqkv, TN, jnp.bfloat16).reshape(1024, 12, 64)
    grad_mix = dot(attended, ez, TN)
    nothing = jnp.zeros((1024, 64), jnp.bfloat16)

    def slot_grad(slot):
        picks = [
            grad_heads[:, SLOTS[half].index(slot)] if slot in SLOTS[half] else nothing
            for half in (0, 1)
        ]
        return jnp.where(low_half, picks[0], picks[1])

    grad_slots = jnp.stack(
        [
            jnp.concatenate([slot_grad(2 * b), slot_grad(2 * b + 1)], axis=1)
            for b in range(8)
        ]
    )
    attn_grads = jnp.concatenate([grad_slots, blocks(grad_mix)], axis=1)
    attn_sum = lax.psum_scatter(attn_grads, "seq", scatter_dimension=0)

    bias_grads = jnp.where(
        jnp.arange(4)[None, :] == i, jnp.sum(dbias[:4], axis=1)[:, None], 0.0
    ).reshape(16)
    small = jnp.concatenate(
        [grad_gain_one, grad_gain_two, jnp.pad(bias_grads, (0, 1024 - 16))]
    ).reshape(24, 128)
    small = small_sum(small, 11).reshape(3, 1024)

    g_gate, g_up, g_down = exchange(
        lambda ins, outs, me, other, seq: grad_pieces("ffn", ins[0], outs, me, other, seq),
        [ffn_sum], [bf16(256, 512), bf16(256, 512), bf16(1024, 128)], 4, 12,
    )
    g_qkv, g_out = exchange(
        lambda ins, outs, me, other, seq: grad_pieces("attention", ins[0], outs, me, other, seq),
        [attn_sum], [bf16(4, 256, 128), bf16(256, 128)], 2, 13,
    )
    g_qkv = g_qkv.reshape(4, 256, 2, 64).transpose(1, 2, 0, 3).reshape(256, 512)[:, :384]
    up32 = lambda g: g.astype(jnp.float32)
    return (
        output, input_grad, up32(g_qkv), up32(g_out), up32(g_gate), up32(g_up), up32(g_down),
        small[0], small[1], small[2, :16],
    )


def solution(mesh):
    in_specs = (
        P("dp", "seq", None),
        P("dp", "seq"),
        P("dp", "seq"),
        P("dp", "seq"),
        P("dp", "seq"),
        P("dp", "seq", None),
        P("dp", "seq"),
        P("dp", "seq"),
        P("dp", "seq"),
        P("dp", "seq"),
        P("dp", "seq"),
        P(),
        P(),
        P(),
    )
    out_specs = (
        P("dp", "seq", None),
        P("dp", "seq", None),
        P("dp", "seq"),
        P("dp", "seq"),
        P("dp", "seq"),
        P("dp", "seq"),
        P("dp", "seq"),
        P(),
        P(),
        P(),
    )
    grouped = mesh.shape["dp"] == 4 and mesh.shape["seq"] == 8
    return jax.shard_map(
        on_group if grouped else on_device, mesh=mesh, in_specs=in_specs, out_specs=out_specs, check_vma=False
    )
```

```python
import functools

import jax
import jax.numpy as jnp
from jax import lax
from jax.experimental import pallas as pl
from jax.experimental.pallas import tpu as pltpu
from jax.sharding import PartitionSpec as P

HEADS = 16
HEAD_DIM = 64
WINDOW = 512


EPSILON = 1e-06
NEGATIVE = -1e30


def passed_along(block, axis, distance):
    devices = range(lax.axis_size(axis))
    route = [(i - distance, i) for i in devices if i - distance in devices]
    return lax.ppermute(block, axis, route)


def norm_scale(hidden):
    return lax.rsqrt(jnp.mean(hidden * hidden, axis=-1, keepdims=True) + EPSILON)


def norm_back(grad_in, hidden, inv_rms):
    return inv_rms * grad_in - hidden * inv_rms * inv_rms * inv_rms * jnp.mean(
        grad_in * hidden, axis=-1, keepdims=True
    )


def rope_tables(time_row, half_dim):
    frequency = jnp.exp(-jnp.log(10000.0) * jnp.arange(half_dim, dtype=jnp.float32) / half_dim)
    angles = time_row.astype(jnp.float32)[:, None] * frequency[None, :]
    return (jnp.cos(angles)[:, None, :], jnp.sin(angles)[:, None, :])


def rotate(values_in, cos_table, sine_table):
    half_dim = cos_table.shape[-1]
    first_half = values_in[..., :half_dim]
    second_half = values_in[..., half_dim:]
    return jnp.concatenate(
        [
            first_half * cos_table - second_half * sine_table,
            second_half * cos_table + first_half * sine_table,
        ],
        axis=-1,
    )


def rotate_back(grad_in, cos_table, sine_table):
    half_dim = cos_table.shape[-1]
    first_half = grad_in[..., :half_dim]
    second_half = grad_in[..., half_dim:]
    return jnp.concatenate(
        [
            first_half * cos_table + second_half * sine_table,
            second_half * cos_table - first_half * sine_table,
        ],
        axis=-1,
    )


def masked_scores(query_rot, keys_all, labels_own, labels_keys, var_bias, hop_count):
    row_count = query_rot.shape[0]
    key_count = keys_all.shape[0]
    offsets = (
        jnp.arange(key_count)[None, :] - hop_count * row_count - jnp.arange(row_count)[:, None]
    )
    allowed = (
        (jnp.abs(offsets) <= WINDOW)
        & (labels_own[0][:, None] == labels_keys[0][None, :])
        & ((labels_keys[2][None, :] == 1) | (offsets == 0))
    )
    same_var = (labels_own[1][:, None] == labels_keys[1][None, :]).astype(jnp.float32)
    scores = jnp.einsum(
        "qhd,khd->hqk", query_rot, keys_all, preferred_element_type=jnp.float32
    ) * HEAD_DIM ** (-0.5)
    scores = scores + var_bias[:, None, None] * same_var[None]
    return (jnp.where(allowed[None], scores, NEGATIVE), same_var)


def fetch_weights(shards):
    row_blocks = (
        lax.all_gather(shards[0], "dp", axis=0, tiled=True),
        lax.all_gather(shards[1], "dp", axis=0, tiled=True),
        lax.all_gather(shards[2], "dp", axis=0, tiled=True),
        lax.all_gather(shards[3], "dp", axis=0, tiled=True),
        lax.all_gather(shards[4], "dp", axis=0, tiled=True),
    )
    return (
        lax.all_gather(row_blocks[0], "seq", axis=1, tiled=True),
        lax.all_gather(row_blocks[1], "seq", axis=1, tiled=True),
        lax.all_gather(row_blocks[2], "seq", axis=1, tiled=True),
        lax.all_gather(row_blocks[3], "seq", axis=1, tiled=True),
        lax.all_gather(row_blocks[4], "seq", axis=1, tiled=True),
    )


def fetch_keep(shards):
    row_blocks = (
        lax.all_gather(shards[0], "dp", axis=0, tiled=True),
        lax.all_gather(shards[1], "dp", axis=0, tiled=True),
        lax.all_gather(shards[2], "dp", axis=0, tiled=True),
        lax.all_gather(shards[3], "dp", axis=0, tiled=True),
        lax.all_gather(shards[4], "dp", axis=0, tiled=True),
    )
    return (
        lax.all_gather(row_blocks[0], "seq", axis=1, tiled=True),
        lax.all_gather(row_blocks[1], "seq", axis=1, tiled=True),
        lax.all_gather(row_blocks[2], "seq", axis=1, tiled=True),
        lax.all_gather(row_blocks[3], "seq", axis=1, tiled=True),
        lax.all_gather(row_blocks[4], "seq", axis=1, tiled=True),
    )


def reduce_last(grads_full):
    col_sums = (
        lax.psum_scatter(grads_full[0], "seq", scatter_dimension=1, tiled=True),
        lax.psum_scatter(grads_full[1], "seq", scatter_dimension=1, tiled=True),
        lax.psum_scatter(grads_full[2], "seq", scatter_dimension=1, tiled=True),
        lax.psum_scatter(grads_full[3], "seq", scatter_dimension=1, tiled=True),
        lax.psum_scatter(grads_full[4], "seq", scatter_dimension=1, tiled=True),
    )
    return (
        lax.psum_scatter(
            col_sums[0].astype(jnp.bfloat16), "dp", scatter_dimension=0, tiled=True
        ).astype(jnp.float32),
        lax.psum_scatter(
            col_sums[1].astype(jnp.bfloat16), "dp", scatter_dimension=0, tiled=True
        ).astype(jnp.float32),
        lax.psum_scatter(
            col_sums[2].astype(jnp.bfloat16), "dp", scatter_dimension=0, tiled=True
        ).astype(jnp.float32),
        lax.psum_scatter(
            col_sums[3].astype(jnp.bfloat16), "dp", scatter_dimension=0, tiled=True
        ).astype(jnp.float32),
        lax.psum_scatter(
            col_sums[4].astype(jnp.bfloat16), "dp", scatter_dimension=0, tiled=True
        ).astype(jnp.float32),
    )


def weight_grads(pieces):
    (
        normed_one,
        grad_qkv,
        attended,
        grad_branch,
        normed_two,
        grad_gate,
        grad_up,
        hidden,
        grad_ffn,
    ) = pieces
    grad_w_qkv = jnp.einsum("td,tf->df", normed_one, grad_qkv, preferred_element_type=jnp.float32)
    grad_w_out = jnp.einsum("ti,to->io", attended, grad_branch, preferred_element_type=jnp.float32)
    grad_w_gate = jnp.einsum("td,tf->df", normed_two, grad_gate, preferred_element_type=jnp.float32)
    grad_w_up = jnp.einsum("td,tf->df", normed_two, grad_up, preferred_element_type=jnp.float32)
    grad_w_down = jnp.einsum("tf,td->fd", hidden, grad_ffn, preferred_element_type=jnp.float32)
    return (grad_w_qkv, grad_w_out, grad_w_gate, grad_w_up, grad_w_down)


def on_device(
    tokens,
    segment_ids,
    variate_ids,
    time_ids,
    pad_mask,
    cotangent,
    w_qkv,
    w_out,
    w_gate,
    w_up,
    w_down,
    gain_attn,
    gain_ffn,
    variate_bias,
):
    micro_count, row_count, model_width = tokens.shape
    hop_count = -(-WINDOW // row_count)
    key_count = (2 * hop_count + 1) * row_count
    shards = (w_qkv, w_out, w_gate, w_up, w_down)
    var_bias = variate_bias.astype(jnp.float32)
    gain_one = gain_attn.astype(jnp.float32)
    gain_two = gain_ffn.astype(jnp.float32)
    bias_total = jnp.zeros(var_bias.shape, jnp.float32)
    gain_one_total = jnp.zeros(gain_one.shape, jnp.float32)
    gain_two_total = jnp.zeros(gain_two.shape, jnp.float32)
    grad_totals = None
    saved = []
    outputs = []
    input_grads = []
    held_weights = fetch_weights(shards)
    for micro_step in range(micro_count):
        if micro_step == 0:
            weights = held_weights
        else:
            weights = fetch_keep(shards)
        resid_in = tokens[micro_step].astype(jnp.float32)
        inv_one = norm_scale(resid_in)
        normed_one = (resid_in * inv_one * gain_one).astype(jnp.bfloat16)
        qkv_proj = jnp.dot(normed_one, weights[0], preferred_element_type=jnp.float32)
        cos_table, sine_table = rope_tables(time_ids[micro_step], HEAD_DIM // 2)
        query_rot = rotate(
            qkv_proj[:, :model_width].reshape(row_count, HEADS, HEAD_DIM), cos_table, sine_table
        ).astype(jnp.bfloat16)
        key_rot = rotate(
            qkv_proj[:, model_width : 2 * model_width].reshape(row_count, HEADS, HEAD_DIM),
            cos_table,
            sine_table,
        ).astype(jnp.bfloat16)
        value_own = qkv_proj[:, 2 * model_width :].astype(jnp.bfloat16)
        kv_own = jnp.stack([key_rot.reshape(row_count, model_width), value_own])
        labels_own = jnp.stack(
            [segment_ids[micro_step], variate_ids[micro_step], pad_mask[micro_step]]
        )
        kv_slots = []
        label_slots = []
        for slot_index in range(2 * hop_count + 1):
            offset = slot_index - hop_count
            if offset == 0:
                kv_slots.append(kv_own)
                label_slots.append(labels_own)
            else:
                kv_slots.append(passed_along(kv_own, "seq", -offset))
                label_slots.append(passed_along(labels_own, "seq", -offset))
        kv_all = jnp.concatenate(kv_slots, axis=1)
        labels_keys = jnp.concatenate(label_slots, axis=1)
        keys_all = kv_all[0].reshape(key_count, HEADS, HEAD_DIM)
        values_all = kv_all[1].reshape(key_count, HEADS, HEAD_DIM)
        scores, same_var = masked_scores(
            query_rot, keys_all, labels_own, labels_keys, var_bias, hop_count
        )
        maxima = jnp.max(scores, axis=-1, keepdims=True)
        exp_shift = jnp.exp(scores - maxima)
        denom_sum = jnp.sum(exp_shift, axis=-1, keepdims=True)
        log_norm = maxima + jnp.log(denom_sum)
        prob_low = (exp_shift / denom_sum).astype(jnp.bfloat16)
        attended = jnp.einsum(
            "hqk,khd->qhd", prob_low, values_all, preferred_element_type=jnp.float32
        )
        attended = attended.reshape(row_count, model_width).astype(jnp.bfloat16)
        resid_mid = resid_in + jnp.dot(attended, weights[1], preferred_element_type=jnp.float32)
        inv_two = norm_scale(resid_mid)
        normed_two = (resid_mid * inv_two * gain_two).astype(jnp.bfloat16)
        gate_proj = jnp.dot(normed_two, weights[2], preferred_element_type=jnp.float32)
        up_proj = jnp.dot(normed_two, weights[3], preferred_element_type=jnp.float32)
        gate_sig = jax.nn.sigmoid(gate_proj)
        hidden = (gate_proj * gate_sig * up_proj).astype(jnp.bfloat16)
        ffn_out = jnp.dot(hidden, weights[4], preferred_element_type=jnp.float32)
        outputs.append((resid_mid + ffn_out).astype(jnp.bfloat16))
        grad_out = cotangent[micro_step].astype(jnp.float32)
        grad_ffn = grad_out.astype(jnp.bfloat16)
        grad_hidden = jnp.einsum(
            "td,fd->tf", grad_ffn, weights[4], preferred_element_type=jnp.float32
        )
        grad_gate = (
            grad_hidden * up_proj * gate_sig * (1.0 + gate_proj * (1.0 - gate_sig))
        ).astype(jnp.bfloat16)
        grad_up = (grad_hidden * gate_proj * gate_sig).astype(jnp.bfloat16)
        grad_normed_two = jnp.einsum(
            "tf,df->td", grad_gate, weights[2], preferred_element_type=jnp.float32
        )
        grad_normed_two = grad_normed_two + jnp.einsum(
            "tf,df->td", grad_up, weights[3], preferred_element_type=jnp.float32
        )
        gain_two_total = gain_two_total + jnp.sum(grad_normed_two * resid_mid * inv_two, axis=0)
        grad_mid = grad_out + norm_back(grad_normed_two * gain_two, resid_mid, inv_two)
        grad_branch = grad_mid.astype(jnp.bfloat16)
        grad_attended = jnp.einsum(
            "to,io->ti", grad_branch, weights[1], preferred_element_type=jnp.float32
        )
        grad_attended = grad_attended.astype(jnp.bfloat16).reshape(row_count, HEADS, HEAD_DIM)
        scores, same_var = masked_scores(
            query_rot, keys_all, labels_own, labels_keys, var_bias, hop_count
        )
        prob_full = jnp.exp(scores - log_norm)
        prob_low = prob_full.astype(jnp.bfloat16)
        grad_values = jnp.einsum(
            "hqk,qhd->khd", prob_low, grad_attended, preferred_element_type=jnp.float32
        )
        grad_prob = jnp.einsum(
            "qhd,khd->hqk", grad_attended, values_all, preferred_element_type=jnp.float32
        )
        grad_scores = prob_full * (
            grad_prob - jnp.sum(prob_full * grad_prob, axis=-1, keepdims=True)
        )
        grad_scores = grad_scores.astype(jnp.bfloat16)
        bias_total = bias_total + jnp.sum(
            grad_scores.astype(jnp.float32) * same_var[None], axis=(1, 2)
        )
        grad_query = jnp.einsum(
            "hqk,khd->qhd", grad_scores, keys_all, preferred_element_type=jnp.float32
        ) * HEAD_DIM ** (-0.5)
        grad_keys = jnp.einsum(
            "hqk,qhd->khd", grad_scores, query_rot, preferred_element_type=jnp.float32
        ) * HEAD_DIM ** (-0.5)
        grad_kv = jnp.stack(
            [grad_keys.reshape(key_count, model_width), grad_values.reshape(key_count, model_width)]
        )
        grad_kv_own = grad_kv[:, hop_count * row_count : (hop_count + 1) * row_count]
        for slot_index in range(2 * hop_count + 1):
            offset = slot_index - hop_count
            if offset != 0:
                slot_grad = grad_kv[:, slot_index * row_count : (slot_index + 1) * row_count]
                grad_kv_own = grad_kv_own + passed_along(
                    slot_grad.astype(jnp.bfloat16), "seq", offset
                ).astype(slot_grad.dtype)
        grad_q_plain = rotate_back(grad_query, cos_table, sine_table).reshape(
            row_count, model_width
        )
        grad_k_plain = rotate_back(
            grad_kv_own[0].reshape(row_count, HEADS, HEAD_DIM), cos_table, sine_table
        ).reshape(row_count, model_width)
        grad_qkv = jnp.concatenate([grad_q_plain, grad_k_plain, grad_kv_own[1]], axis=1).astype(
            jnp.bfloat16
        )
        grad_normed_one = jnp.einsum(
            "tf,df->td", grad_qkv, weights[0], preferred_element_type=jnp.float32
        )
        gain_one_total = gain_one_total + jnp.sum(grad_normed_one * resid_in * inv_one, axis=0)
        grad_input = grad_mid + norm_back(grad_normed_one * gain_one, resid_in, inv_one)
        input_grads.append(grad_input.astype(jnp.bfloat16))
        pieces = (
            normed_one,
            grad_qkv,
            attended,
            grad_branch,
            normed_two,
            grad_gate,
            grad_up,
            hidden,
            grad_ffn,
        )
        saved.append(pieces)
    joined = tuple(
        (
            jnp.concatenate([entry[index] for entry in saved], axis=0)
            for index in range(len(saved[0]))
        )
    )
    grad_totals = reduce_last(weight_grads(joined))
    bias_sum, gain_one_sum, gain_two_sum = lax.psum(
        (bias_total, gain_one_total, gain_two_total), ("dp", "seq")
    )
    return (
        jnp.stack(outputs),
        jnp.stack(input_grads),
        grad_totals[0],
        grad_totals[1],
        grad_totals[2],
        grad_totals[3],
        grad_totals[4],
        gain_one_sum,
        gain_two_sum,
        bias_sum,
    )


MESH = pl.DeviceIdType.MESH
VM = pl.BlockSpec(memory_space=pltpu.VMEM)
HB = pl.BlockSpec(memory_space=pl.ANY)
SM = pl.BlockSpec(memory_space=pltpu.SMEM)
DMA = pltpu.SemaphoreType.DMA
NT = (((1,), (1,)), ((), ()))
TN = (((0,), (0,)), ((), ()))
EVERY = slice(None)


def bf16(*shape):
    return jax.ShapeDtypeStruct(shape, jnp.bfloat16)


def f32(*shape):
    return jax.ShapeDtypeStruct(shape, jnp.float32)


def dot(a, b, dims=None, out=jnp.float32):
    dims = (((1,), (0,)), ((), ())) if dims is None else dims
    return lax.dot_general(a, b, dims, preferred_element_type=jnp.float32).astype(out)


def at(dp, seq):
    return {"dp": dp, "seq": seq}


def place():
    return lax.axis_index("dp"), lax.axis_index("seq")


def ring(i):
    return i + 1 - 2 * lax.rem(i, 2), lax.rem(i + 2, 4)


def owned(i, s):
    return 4 * lax.rem(i, 2) + 2 * s + i // 2


def keeper(j):
    return 2 * lax.rem(j, 2) + j // 4


def send(src, dst, send_sem, recv_sem, peer):
    return pltpu.make_async_remote_copy(
        src_ref=src,
        dst_ref=dst,
        send_sem=send_sem,
        recv_sem=recv_sem,
        device_id=peer,
        device_id_type=MESH,
    )


def landed(ref, sem):
    pltpu.make_async_copy(ref, ref, sem).wait()


def meet(peers, home=False):
    i, j = place()
    barrier = pltpu.get_barrier_semaphore()
    for peer in peers:
        pl.semaphore_signal(barrier, inc=1, device_id=peer, device_id_type=MESH)
    if home:
        target, stays = keeper(j), keeper(j) == i
        for s in (0, 1):

            @pl.when(jnp.logical_not(stays & (owned(i, s) == j)))
            def _():
                pl.semaphore_signal(
                    barrier, inc=1, device_id=at(target, owned(i, s)), device_id_type=MESH
                )

        pl.semaphore_wait(barrier, len(peers) + jnp.where(stays, 1, 2))
    else:
        pl.semaphore_wait(barrier, len(peers))


def dp_peers():
    i, j = place()
    return [at(lax.rem(i + step, 4), j) for step in (1, 2, 3)]


def seq_peers():
    i, j = place()
    z, y = j // 2, lax.rem(j, 2)
    return [at(i, 2 * lax.rem(z + step, 4) + y) for step in (1, 2, 3)] + [at(i, 2 * z + 1 - y)]


class Home:
    def __init__(self, ins, outs, sems, slotted):
        self.ins, self.outs, self.slotted = ins, outs, slotted
        self.send_sem, self.recv_sem = sems

    @staticmethod
    def sems(count):
        return [DMA((count, 2)), DMA((count, 2))]

    def target(self, a, s):
        i, _ = place()
        return self.outs[a].at[s if self.slotted else owned(i, s)]

    def start(self, a, s):
        i, j = place()
        slot = lax.rem(j // 2, 2)
        src, dst = self.ins[a].at[s], self.outs[a].at[slot if self.slotted else j]
        here = (keeper(j) == i) & (owned(i, s) == j)

        @pl.when(jnp.logical_not(here))
        def _():
            peer = at(keeper(j), owned(i, s))
            send(src, dst, self.send_sem.at[a, s], self.recv_sem.at[a, slot], peer).start()

        @pl.when(here)
        def _():
            pltpu.make_async_copy(src, dst, self.recv_sem.at[a, slot]).start()

    def wait(self, a, s):
        landed(self.target(a, s), self.recv_sem.at[a, s])

    def finish(self, a):
        i, j = place()
        for s in (0, 1):

            @pl.when(jnp.logical_not((keeper(j) == i) & (owned(i, s) == j)))
            def _():
                landed(self.ins[a].at[s], self.send_sem.at[a, s])


class GroupGather:
    def __init__(self, outs, sems):
        self.outs = outs
        self.s_core, self.r_core, self.s_x, self.r_x, self.s_on, self.r_on = sems

    @staticmethod
    def sems(count):
        return [DMA((count, 2))] * 6

    def push(self, a, s):
        i, j = place()
        core, across = ring(i)
        block = self.outs[a].at[owned(i, s)]
        send(block, block, self.s_x.at[a, s], self.r_x.at[a, s], at(across, j)).start()
        send(block, block, self.s_core.at[a, s], self.r_core.at[a, s], at(core, j)).start()

    def relay(self, a, s):
        i, j = place()
        core, across = ring(i)
        block = self.outs[a].at[owned(across, s)]
        landed(block, self.r_x.at[a, s])
        send(block, block, self.s_on.at[a, s], self.r_on.at[a, s], at(core, j)).start()

    def finish(self, a):
        i, _ = place()
        core, _ = ring(i)
        for s in (0, 1):
            landed(self.outs[a].at[owned(core, s)], self.r_core.at[a, s])
            landed(self.outs[a].at[owned(lax.rem(core + 2, 4), s)], self.r_on.at[a, s])
        for s in (0, 1):
            for sem in (self.s_x, self.s_core, self.s_on):
                landed(self.outs[a].at[s], sem.at[a, s])


class GroupSum:
    def __init__(self, parts, buffers, sems):
        self.parts = parts
        self.near, self.far = buffers
        self.s_core, self.r_core, self.s_x, self.r_x = sems

    @staticmethod
    def buffers():
        block = (128, 1024)
        return [pltpu.VMEM((2, 2) + block, jnp.bfloat16), pltpu.VMEM((2,) + block, jnp.bfloat16)]

    @staticmethod
    def sems():
        return [DMA((2, 2)), DMA((2, 2)), DMA((2,)), DMA((2,))]

    def start(self, s):
        i, j = place()
        core, _ = ring(i)
        for side, owner in ((0, lax.rem(core + 2, 4)), (1, core)):
            send(
                self.parts.at[owned(owner, s)],
                self.near.at[side, s],
                self.s_core.at[side, s],
                self.r_core.at[side, s],
                at(core, j),
            ).start()

    def cross(self, s):
        i, j = place()
        _, across = ring(i)
        landed(self.near.at[0, s], self.r_core.at[0, s])
        both = self.parts[owned(across, s)].astype(jnp.float32)
        both = both + self.near[0, s].astype(jnp.float32)
        self.near[0, s] = both.astype(jnp.bfloat16)
        send(
            self.near.at[0, s], self.far.at[s], self.s_x.at[s], self.r_x.at[s], at(across, j)
        ).start()

    def total(self, s):
        i, _ = place()
        landed(self.near.at[1, s], self.r_core.at[1, s])
        both = self.parts[owned(i, s)].astype(jnp.float32) + self.near[1, s].astype(jnp.float32)
        landed(self.far.at[s], self.r_x.at[s])
        return both + self.far[s].astype(jnp.float32)

    def finish(self):
        for s in (0, 1):
            landed(self.near.at[0, s], self.s_x.at[s])
            for side in (0, 1):
                landed(self.near.at[side, s], self.s_core.at[side, s])


class Exchange:
    def __init__(self, pieces, sems):
        self.pieces = pieces
        self.send_sem, self.recv_sem, self.own_sem = sems
        self.copies = []

    @staticmethod
    def sems(count):
        return [DMA((3, count)), DMA((3, count)), DMA((count,))]

    def start(self):
        i, j = place()
        for step in (2, 3, 1):
            other = lax.rem(i + step, 4)
            for index, (src, dst) in enumerate(self.pieces(i, other)):
                copy = send(
                    src,
                    dst,
                    self.send_sem.at[step - 1, index],
                    self.recv_sem.at[step - 1, index],
                    at(other, j),
                )
                copy.start()
                self.copies.append(copy)
        for index, (src, dst) in enumerate(self.pieces(i, i)):
            copy = pltpu.make_async_copy(src, dst, self.own_sem.at[index])
            copy.start()
            self.copies.append(copy)

    def wait(self):
        for copy in self.copies:
            copy.wait()


class SeqGather:
    def __init__(self, full, chunks, sems):
        self.full, self.chunks = full, chunks
        self.s_z, self.r_z, self.s_y, self.r_y = sems

    @staticmethod
    def sems(count):
        return [DMA((count, 3)), DMA((count, 3)), DMA((count, 4)), DMA((count, 4))]

    def block(self, chunk, z, y):
        start, size = self.chunks[chunk]
        return self.full.at[2 * z + y, pl.ds(start, size)]

    def start(self, chunk):
        i, j = place()
        z, y = j // 2, lax.rem(j, 2)
        own = self.block(chunk, z, y)
        for dz in (2, 1, 3):
            peer = at(i, 2 * lax.rem(z + dz, 4) + y)
            send(own, own, self.s_z.at[chunk, dz - 1], self.r_z.at[chunk, dz - 1], peer).start()
        send(own, own, self.s_y.at[chunk, 0], self.r_y.at[chunk, 0], at(i, 2 * z + 1 - y)).start()

    def forward(self, chunk, dz):
        i, j = place()
        z, y = j // 2, lax.rem(j, 2)
        block = self.block(chunk, lax.rem(z + 4 - dz, 4), y)
        landed(block, self.r_z.at[chunk, dz - 1])
        peer = at(i, 2 * z + 1 - y)
        send(block, block, self.s_y.at[chunk, dz], self.r_y.at[chunk, dz], peer).start()

    def arrived(self, chunk, dz):
        _, j = place()
        z, y = j // 2, lax.rem(j, 2)
        landed(self.block(chunk, lax.rem(z + 4 - dz, 4), 1 - y), self.r_y.at[chunk, dz])

    def drain(self, chunk):
        _, j = place()
        own = self.block(chunk, j // 2, lax.rem(j, 2))
        for dz in (0, 1, 2, 3):
            landed(own, self.s_y.at[chunk, dz])
            if dz:
                landed(own, self.s_z.at[chunk, dz - 1])

    def finish(self, chunk):
        for dz in (0, 1, 2, 3):
            self.arrived(chunk, dz)
        self.drain(chunk)


class SeqSum:
    def __init__(self, parts, chunks, scratch):
        self.parts, self.chunks = parts, chunks
        self.near, self.far = scratch[:2]
        self.s_y, self.r_y, self.s_z, self.r_z = scratch[2:]

    @staticmethod
    def scratch(rows, count):
        return [
            pltpu.VMEM((4, rows, 128), jnp.bfloat16),
            pltpu.VMEM((3, rows, 128), jnp.bfloat16),
            DMA((count, 4)),
            DMA((count, 4)),
            DMA((count, 3)),
            DMA((count, 3)),
        ]

    def start(self, chunk, dz):
        i, j = place()
        z, y = j // 2, lax.rem(j, 2)
        rows = pl.ds(*self.chunks[chunk])
        send(
            self.parts.at[2 * lax.rem(z + dz, 4) + 1 - y, rows],
            self.near.at[dz, rows],
            self.s_y.at[chunk, dz],
            self.r_y.at[chunk, dz],
            at(i, 2 * z + 1 - y),
        ).start()

    def each(self, chunk, body):
        start, size = self.chunks[chunk]

        @pl.loop(0, size // 256)
        def _(t):
            body(pl.ds(pl.multiple_of(start + t * 256, 256), 256))

    def cross(self, chunk, dz):
        i, j = place()
        z, y = j // 2, lax.rem(j, 2)
        rows = pl.ds(*self.chunks[chunk])
        target = lax.rem(z + dz, 4)
        landed(self.near.at[dz, rows], self.r_y.at[chunk, dz])

        def add(part):
            both = self.parts[2 * target + y, part, :].astype(jnp.float32)
            both = both + self.near[dz, part, :].astype(jnp.float32)
            self.near[dz, part, :] = both.astype(jnp.bfloat16)

        self.each(chunk, add)
        send(
            self.near.at[dz, rows],
            self.far.at[dz - 1, rows],
            self.s_z.at[chunk, dz - 1],
            self.r_z.at[chunk, dz - 1],
            at(i, 2 * target + y),
        ).start()

    def finish(self, chunk):
        _, j = place()
        rows = pl.ds(*self.chunks[chunk])
        landed(self.near.at[0, rows], self.r_y.at[chunk, 0])
        for dz in (1, 2, 3):
            landed(self.far.at[dz - 1, rows], self.r_z.at[chunk, dz - 1])

        def add(part):
            total = self.parts[j, part, :].astype(jnp.float32)
            total = total + self.near[0, part, :].astype(jnp.float32)
            for dz in (1, 2, 3):
                total = total + self.far[dz - 1, part, :].astype(jnp.float32)
            self.near[0, part, :] = total.astype(jnp.bfloat16)

        self.each(chunk, add)

    def drain(self, chunk):
        rows = pl.ds(*self.chunks[chunk])
        for dz in (0, 1, 2, 3):
            landed(self.near.at[dz, rows], self.s_y.at[chunk, dz])
            if dz:
                landed(self.near.at[dz, rows], self.s_z.at[chunk, dz - 1])


class SmallSum:
    def __init__(self, value, scratch):
        self.value = value
        self.stages, self.sems = scratch[:3], scratch[3:]

    @staticmethod
    def scratch(shape):
        return [pltpu.VMEM((count,) + shape, jnp.float32) for count in (4, 4, 2)] + [
            DMA((count,)) for count in (3, 3, 3, 3, 1, 1)
        ]

    def run(self):
        i, j = place()
        z, y = j // 2, lax.rem(j, 2)
        rounds = (
            (i, dp_peers()),
            (z, seq_peers()[:3]),
            (y, seq_peers()[3:]),
        )
        total = self.value[...]
        for stage, (spot, peers) in enumerate(rounds):
            held = self.stages[stage]
            held[spot] = total
            for step, peer in enumerate(peers):
                send(
                    held.at[spot],
                    held.at[spot],
                    self.sems[2 * stage].at[step],
                    self.sems[2 * stage + 1].at[step],
                    peer,
                ).start()
            for step in range(len(peers)):
                landed(held.at[0], self.sems[2 * stage + 1].at[step])
                landed(held.at[0], self.sems[2 * stage].at[step])
            total = held[0]
            for index in range(1, held.shape[0]):
                total = total + held[index]
        return total


def swap_halves(x):
    lane = lax.broadcasted_iota(jnp.int32, x.shape, 1)
    width = x.shape[1]
    return jnp.where(lane % 64 < 32, pltpu.roll(x, width - 32, 1), pltpu.roll(x, 32, 1))


def angle_tables(table):
    lane = lax.broadcasted_iota(jnp.int32, table.shape, 1)
    by_32, by_64, by_96 = (pltpu.roll(table, shift, 1) for shift in (32, 64, 96))
    first, second, third = lane < 32, lane < 64, lane < 96
    cos_t = jnp.where(first, table, jnp.where(second, by_32, jnp.where(third, by_64, by_96)))
    sin_t = jnp.where(first, -by_96, jnp.where(second, table, jnp.where(third, -by_32, by_64)))
    return cos_t, sin_t


SLOTS = (
    (0, 1, 2, 4, 5, 6, 8, 9, 10, 12, 13, 14),
    (0, 2, 3, 4, 6, 7, 8, 10, 11, 12, 14, 15),
)


def attention_pieces(packed, w_out, dst):
    def pieces(me, other):
        _, j = place()
        spot = lax.rem(other + 2 * lax.rem(j, 2), 4)
        return [
            (packed.at[spot], dst.at[j, pl.ds(256 * me, 256)]),
            (w_out.at[pl.ds(64 * other, 64)], dst.at[j, pl.ds(1024 + 64 * me, 64)]),
        ]

    return pieces


def ffn_pieces(w_gate, w_up, w_down, dst):
    def pieces(me, other):
        _, j = place()
        columns = pl.ds(pl.multiple_of(128 * other, 128), 128)
        pairs = [
            (w_gate.at[:, columns], dst.at[j, pl.ds(256 * me, 256)]),
            (w_up.at[:, columns], dst.at[j, pl.ds(1024 + 256 * me, 256)]),
        ]
        for half in (0, 1):
            pairs.append(
                (
                    w_down.at[pl.ds(512 * half + 128 * other, 128)],
                    dst.at[j, pl.ds(2048 + 256 * me + 128 * half, 128)],
                )
            )
        return pairs

    return pieces


def head_weights(full, wh_ref, wm_ref, low_half):
    def column(m, rows):
        first, second = SLOTS[0][m], SLOTS[1][m]
        one = full[first // 2, rows, 64 * (first % 2) : 64 * (first % 2) + 64]
        two = full[second // 2, rows, 64 * (second % 2) : 64 * (second % 2) + 64]
        return jnp.where(low_half, one, two)

    @pl.loop(0, 4)
    def _(t):
        rows = pl.ds(pl.multiple_of(t * 256, 256), 256)
        for m in range(0, 12, 2):
            wh_ref[rows, 64 * m : 64 * m + 128] = jnp.concatenate(
                [column(m, rows), column(m + 1, rows)], axis=1
            )

    for b in range(8):
        wm_ref[:, 128 * b : 128 * b + 128] = full[b, 1024:1280, :]


def norm_rows(hidden):
    return lax.rsqrt(jnp.mean(hidden * hidden, axis=1, keepdims=True) + EPSILON)


def return_attention(src, g_qkv, g_out):
    def pieces(me, other):
        _, j = place()
        spot = lax.rem(me + 2 * lax.rem(j, 2), 4)
        return [
            (src.at[pl.ds(256 * other, 256)], g_qkv.at[spot]),
            (src.at[pl.ds(1024 + 64 * other, 64)], g_out.at[pl.ds(64 * me, 64)]),
        ]

    return pieces


def return_ffn(src, g_gate, g_up, g_down):
    def pieces(me, other):
        columns = pl.ds(pl.multiple_of(128 * me, 128), 128)
        pairs = [
            (src.at[pl.ds(256 * other, 256)], g_gate.at[:, columns]),
            (src.at[pl.ds(1024 + 256 * other, 256)], g_up.at[:, columns]),
        ]
        for half in (0, 1):
            pairs.append(
                (
                    src.at[pl.ds(2048 + 256 * other + 128 * half, 128)],
                    g_down.at[pl.ds(512 * half + 128 * me, 128)],
                )
            )
        return pairs

    return pieces


def back_rows(grad_in, hidden, inv_rms):
    mean = jnp.mean(grad_in * hidden, axis=1, keepdims=True)
    return inv_rms * grad_in - hidden * (inv_rms * inv_rms * inv_rms * mean)


def slot_columns(grads, slot, low_half):
    picks = []
    for row in SLOTS:
        if slot in row:
            m = row.index(slot)
            picks.append(grads[:, 64 * m : 64 * m + 64])
        else:
            picks.append(jnp.zeros((grads.shape[0], 64), jnp.float32))
    return jnp.where(low_half, picks[0], picks[1])


FFN_CHUNKS = ((2048, 1024), (0, 2048))
GRAD_CHUNKS = ((0, 2048), (2048, 1024))
ATTENTION_CHUNKS = ((0, 1024), (1024, 256))
ARRIVAL = (2, 1, 3)


def wide(ref, first, rows):
    return jnp.concatenate([ref[first, rows, :], ref[first + 1, rows, :]], axis=1)


def store_wide(ref, first, rows, value):
    ref[first, rows, :] = value[:, :128]
    ref[first + 1, rows, :] = value[:, 128:]


def two(ref, t, cols=slice(None)):
    value = ref[pl.ds(2 * t, 2), :, cols]
    return value.reshape(256, value.shape[2])


def layer_kernel(*refs):
    (tok, cot, tab, idr, packed, w_out, w_gate, w_up, w_down, gain_one, gain_two, bias), refs = (
        refs[:12],
        refs[12:],
    )
    (output, input_grad, g_gate, g_up, g_down, g_qkv, g_out, small_out), refs = refs[:8], refs[8:]
    (
        tok_all, cot_all, tab_all, idr_all, tok_own, attn_all, wh_ref, wm_ref, q_ref, k_ref, v_ref,
        o_ref, lse_ref, rows_ref, part, mid_ref, a2_all, turned, ffn_all, ffn_g, hidden_s, dgate_s,
        dup_s, e2_ref, dq_acc, dk_acc, dv_acc, out_own, in_own, dbias, small,
        r_gate, r_up, r_down, r_qkv, r_out,
    ), refs = refs[:36], refs[36:]
    home_in, refs = refs[:2], refs[2:]
    home_out, refs = refs[:2], refs[2:]
    gather_in, refs = refs[:6], refs[6:]
    gather_a2, refs = refs[:6], refs[6:]
    gather_ez, refs = refs[:6], refs[6:]
    buffers, refs = refs[:2], refs[2:]
    out_buffers, refs = refs[:2], refs[2:]
    sum_sems, refs = [refs[4 * n : 4 * n + 4] for n in range(4)], refs[16:]
    spread_a, spread_f, back_a, back_f = [refs[3 * n : 3 * n + 3] for n in range(4)]
    refs = refs[12:]
    chain_a, chain_f, refs = refs[:4], refs[4:8], refs[8:]
    fold_f, fold_a, refs = refs[:6], refs[6:12], refs[12:]
    small_scratch = refs

    i, j = place()
    z, y = j // 2, lax.rem(j, 2)
    mine_first = 2 * (1 - lax.rem(i, 2))
    low_half = i < 2

    def turn(u):
        return lax.rem(mine_first + u, 4)

    ez_all, dqkv_ref, do_ref, out_part = dgate_s, dup_s, hidden_s, turned
    home = Home((tok, tab, idr, cot), (tok_all, tab_all, idr_all, cot_all), home_in, False)
    group = GroupGather((tok_all, tab_all, idr_all, cot_all), gather_in)
    spread = Exchange(attention_pieces(packed, w_out, attn_all), spread_a)
    spread_ffn = Exchange(ffn_pieces(w_gate, w_up, w_down, ffn_all), spread_f)
    attn_w = SeqGather(attn_all, ((0, 1280),), chain_a)
    ffn_w = SeqGather(ffn_all, FFN_CHUNKS, chain_f)
    branch = GroupSum(part, buffers, sum_sems[0])
    second = GroupGather((a2_all,), gather_a2)
    da_sum = GroupSum(part, buffers, sum_sems[1])
    out_sum = GroupSum(out_part, out_buffers, sum_sems[2])
    da1_sum = GroupSum(part, buffers, sum_sems[3])
    third = GroupGather((ez_all,), gather_ez)
    leave = Home((out_own, in_own), (output, input_grad), home_out, True)
    ffn_fold = SeqSum(ffn_g, GRAD_CHUNKS, fold_f)
    attn_fold = SeqSum(attn_all, ATTENTION_CHUNKS, fold_a)
    ffn_back = Exchange(return_ffn(fold_f[0].at[0], r_gate, r_up, r_down), back_f)
    attn_back = Exchange(return_attention(fold_a[0].at[0], r_qkv, r_out), back_a)

    meet(dp_peers() + seq_peers(), home=True)
    for a in (0, 1, 2):
        for s in (0, 1):
            home.start(a, s)
    spread.start()
    spread_ffn.start()
    spread.wait()
    attn_w.start(0)
    for a in (0, 1, 2):
        for s in (0, 1):
            home.wait(a, s)
            group.push(a, s)
    spread_ffn.wait()
    ffn_w.start(0)
    for s in (0, 1):
        home.start(3, s)
    ffn_w.start(1)
    for s in (0, 1):
        tok_own[s] = tok_all[owned(i, s)]
    for a in (0, 1, 2):
        for s in (0, 1):
            group.relay(a, s)
    for a in (0, 1, 2):
        group.finish(a)
        home.finish(a)
    for b in range(8):
        rows_ref[:, 128 * b : 128 * b + 128] = idr_all[b]

    @pl.loop(0, 8)
    def _(b):
        hidden = tok_all[b].astype(jnp.float32)
        tok_all[b] = (hidden * norm_rows(hidden) * gain_one[...]).astype(jnp.bfloat16)

    a1_all = tok_all
    for dz in ARRIVAL:
        attn_w.forward(0, dz)
    attn_w.finish(0)
    head_weights(attn_all, wh_ref, wm_ref, low_half)

    @pl.loop(0, 4)
    def _(t):
        rows = pl.ds(pl.multiple_of(t * 256, 256), 256)
        proj = dot(two(a1_all, t), wh_ref[...])
        cos_t, sin_t = angle_tables(two(tab_all, t))
        for pair in (0, 1):
            cols = slice(128 * pair, 128 * pair + 128)
            for base, out in ((0, q_ref), (256, k_ref)):
                x = proj[:, base + 128 * pair : base + 128 * pair + 128]
                out[rows, cols] = (x * cos_t + swap_halves(x) * sin_t).astype(jnp.bfloat16)
        v_ref[rows, :] = proj[:, 512:768].astype(jnp.bfloat16)

    @pl.loop(0, 4)
    def _(u):
        t = turn(u)
        start = pl.multiple_of(t * 256, 256)
        rows = pl.ds(start, 256)
        columns = two(tab_all, t)
        seg_q, var_q = columns[:, 64:65], columns[:, 65:66]
        code_k, var_k = rows_ref[0:1, :], rows_ref[1:2, :]
        row = start + lax.broadcasted_iota(jnp.int32, (256, 1024), 0)
        col = lax.broadcasted_iota(jnp.int32, (256, 1024), 1)
        allowed = ((seg_q == code_k) & (jnp.abs(row - col) <= WINDOW)) | (row == col)
        masked = jnp.where(allowed, 0.0, NEGATIVE)
        same = jnp.where(var_q == var_k, 1.0, 0.0)
        stats = jnp.zeros((256, 128), jnp.float32)
        lane = lax.broadcasted_iota(jnp.int32, (256, 128), 1)
        for h in range(4):
            cols = slice(64 * h, 64 * h + 64)
            scores = dot(q_ref[rows, cols] * 0.125, k_ref[:, cols], NT)
            scores = scores + bias[h] * same + masked
            top = jnp.max(scores, axis=1, keepdims=True)
            weight = jnp.exp(scores - top)
            total = jnp.sum(weight, axis=1, keepdims=True)
            mixed = dot(weight.astype(jnp.bfloat16), v_ref[:, cols])
            o_ref[rows, cols] = (mixed / total).astype(jnp.bfloat16)
            stats = jnp.where(lane == h, top + jnp.log(total), stats)
        lse_ref[:, rows] = stats.T[:8]
        part[pl.ds(2 * t, 2)] = dot(o_ref[rows, :], wm_ref[...], out=jnp.bfloat16).reshape(2, 128, 1024)
        for s in (0, 1):

            @pl.when(u == s)
            def _():
                branch.start(s)

            @pl.when(u == s + 2)
            def _():
                branch.cross(s)

        @pl.when(u == 1)
        def _():
            for dz in ARRIVAL:
                ffn_w.forward(0, dz)

    for s in (0, 1):
        home.wait(3, s)
        group.push(3, s)
    for s in (0, 1):
        block = owned(i, s)
        mid = tok_own[s].astype(jnp.float32) + branch.total(s)
        mid_ref[s] = mid
        a2_all[block] = (mid * norm_rows(mid) * gain_two[...]).astype(jnp.bfloat16)
        second.push(0, s)
    branch.finish()
    ffn_w.forward(1, 2)
    for s in (0, 1):
        group.relay(3, s)
    for s in (0, 1):
        second.relay(0, s)
    ffn_w.forward(1, 1)
    group.finish(3)
    home.finish(3)
    second.finish(0)
    ffn_w.finish(0)

    @pl.loop(0, 4)
    def _(t):
        for d in range(4):
            turned[2 * d : 2 * d + 2, :, pl.ds(pl.multiple_of(256 * t, 256), 256)] = (
                two(a2_all, t, slice(256 * d, 256 * d + 256)).T.reshape(2, 128, 256)
            )

    def unit(dz):
        f = lax.rem(z + 4 - dz, 4)
        cols = pl.ds(pl.multiple_of(256 * f, 256), 256)
        wg, wu = wide(ffn_all, 2 * f, slice(0, 1024)), wide(ffn_all, 2 * f, slice(1024, 2048))
        down = pl.ds(pl.multiple_of(2048 + 256 * f, 256), 256)
        wd = jnp.concatenate([ffn_all[b, down, :] for b in range(8)], axis=1)

        @pl.loop(0, 4)
        def _(t):
            a, g = two(a2_all, t), two(cot_all, t)
            gate, up, dh = dot(a, wg), dot(a, wu), dot(g, wd, NT)
            sig = 1.0 / (1.0 + jnp.exp(-gate))
            gate_sig = gate * sig
            into = (pl.ds(2 * t, 2), slice(None), cols)
            hidden_s[into] = (gate_sig * up).astype(jnp.bfloat16).reshape(2, 128, 256)
            dgate = dh * up * (sig + gate_sig * (1.0 - sig))
            dgate_s[into] = dgate.astype(jnp.bfloat16).reshape(2, 128, 256)
            dup_s[into] = (dh * gate_sig).astype(jnp.bfloat16).reshape(2, 128, 256)

        @pl.loop(0, 4)
        def _(d):
            rows = pl.ds(pl.multiple_of(d * 256, 256), 256)
            rows_up = pl.ds(pl.multiple_of(1024 + d * 256, 256), 256)
            a_t = two(turned, d)
            dgate, dup = dgate_s[:, :, cols].reshape(1024, 256), dup_s[:, :, cols].reshape(1024, 256)
            store_wide(ffn_g, 2 * f, rows, dot(a_t, dgate, out=jnp.bfloat16))
            store_wide(ffn_g, 2 * f, rows_up, dot(a_t, dup, out=jnp.bfloat16))

        h_t = hidden_s[:, :, cols].reshape(1024, 256).T
        for d in range(4):
            g = cot_all[:, :, 256 * d : 256 * d + 256].reshape(1024, 256)
            store_wide(ffn_g, 2 * d, down, dot(h_t, g, out=jnp.bfloat16))

    @pl.loop(0, 4)
    def _(step):
        dz = jnp.where(step == 1, 2, jnp.where(step == 2, 1, step))
        for n, here in enumerate((0, 2, 1, 3)):

            @pl.when(step == n)
            def _():
                if n == 3:
                    ffn_w.forward(1, 3)
                ffn_w.arrived(1, here)

        unit(dz)
        for n, there in enumerate((0, 2, 3, 1)):

            @pl.when(step == n)
            def _():
                ffn_fold.start(0, there)

    for dz in (2, 3, 1, 0):
        ffn_fold.start(1, dz)
    ffn_w.drain(1)

    def product(left, t, first_row):
        total = None
        for p in range(4):
            piece = dot(
                two(left, t, slice(256 * p, 256 * p + 256)),
                wide(ffn_all, 2 * p, slice(first_row, first_row + 1024)),
                NT,
            )
            total = piece if total is None else total + piece
        return total

    @pl.loop(0, 4)
    def _(u):
        t = turn(u)
        value = product(dgate_s, t, 0) + product(dup_s, t, 1024)
        part[pl.ds(2 * t, 2)] = value.astype(jnp.bfloat16).reshape(2, 128, 1024)
        for s in (0, 1):

            @pl.when(u == s)
            def _():
                da_sum.start(s)

            @pl.when(u == s + 2)
            def _():
                da_sum.cross(s)

    @pl.loop(0, 4)
    def _(u):
        t = turn(u)
        hidden = two(hidden_s, t)
        for d in range(4):
            w = wide(ffn_all, 2 * d, slice(2048, 3072))
            out_part[pl.ds(2 * t, 2), :, 256 * d : 256 * d + 256] = dot(
                hidden, w, out=jnp.bfloat16
            ).reshape(2, 128, 256)
        for s in (0, 1):

            @pl.when(u == s)
            def _():
                out_sum.start(s)

    gain_rows = jnp.zeros((1, 1024), jnp.float32)
    for s in (0, 1):
        mid = mid_ref[s]
        inv = norm_rows(mid)
        da2 = da_sum.total(s)
        gain_rows = gain_rows + jnp.sum(da2 * (mid * inv), axis=0, keepdims=True)
        e2 = cot_all[owned(i, s)].astype(jnp.float32) + back_rows(da2 * gain_two[...], mid, inv)
        e2_ref[s] = e2
        ez_all[owned(i, s)] = e2.astype(jnp.bfloat16)
        third.push(0, s)
    for b in range(8):
        small[8 + b : 9 + b, :] = gain_rows[:, 128 * b : 128 * b + 128]
    for s in (0, 1):
        out_sum.cross(s)
    da_sum.finish()
    ffn_fold.cross(0, 2)
    for s in (0, 1):
        third.relay(0, s)
    third.finish(0)

    @pl.loop(0, 4)
    def _(t):
        do_ref[pl.ds(2 * t, 2), :, 0:256] = dot(two(ez_all, t), wm_ref[...], NT, jnp.bfloat16).reshape(
            2, 128, 256
        )

    for d in range(4):
        ez = ez_all[:, :, 256 * d : 256 * d + 256].reshape(1024, 256)
        store_wide(attn_all, 2 * d, slice(1024, 1280), dot(o_ref[...], ez, TN, jnp.bfloat16))
    for dz in (2, 3, 1, 0):
        attn_fold.start(1, dz)
    ffn_fold.cross(0, 3)
    for s in (0, 1):
        out_own[s] = (mid_ref[s] + out_sum.total(s)).astype(jnp.bfloat16)
        leave.start(0, s)

    def unturn(acc, base, t, rows):
        cos_t, sin_t = angle_tables(two(tab_all, t))
        for pair in (0, 1):
            g = acc[rows, 128 * pair : 128 * pair + 128]
            dqkv_ref[pl.ds(2 * t, 2), :, base + 128 * pair : base + 128 * pair + 128] = (
                (g * cos_t - swap_halves(g) * sin_t).astype(jnp.bfloat16).reshape(2, 128, 128)
            )

    dk_acc[...] = jnp.zeros_like(dk_acc)
    dv_acc[...] = jnp.zeros_like(dv_acc)
    dbias[...] = jnp.zeros_like(dbias)

    @pl.loop(0, 4)
    def _(t):
        start = pl.multiple_of(t * 256, 256)
        rows = pl.ds(start, 256)
        columns = tab_all[...].reshape(1024, 128)
        var_k, code_k = columns[:, 65:66], columns[:, 66:67]
        pair = idr_all[pl.ds(2 * t, 2)]
        label = jnp.concatenate([pair[0], pair[1]], axis=1)
        seg_q, var_q = label[2:3, :], label[1:2, :]
        row = lax.broadcasted_iota(jnp.int32, (1024, 256), 0)
        col = start + lax.broadcasted_iota(jnp.int32, (1024, 256), 1)
        allowed = ((seg_q == code_k) & (jnp.abs(row - col) <= WINDOW)) | (row == col)
        masked = jnp.where(allowed, 0.0, NEGATIVE)
        same = jnp.where(var_q == var_k, 1.0, 0.0)
        for h in range(4):
            cols = slice(64 * h, 64 * h + 64)
            q_h, k_h, v_h = q_ref[rows, cols] * 0.125, k_ref[:, cols], v_ref[:, cols]
            do_h = two(do_ref, t, cols)
            scores = dot(k_h, q_h, NT) + bias[h] * same + masked
            prob = jnp.exp(scores - lse_ref[h : h + 1, rows])
            dv_acc[:, cols] += dot(prob.astype(jnp.bfloat16), do_h)
            dprob = dot(v_h, do_h, NT)
            mean = jnp.sum(prob * dprob, axis=0, keepdims=True)
            dscore = (prob * (dprob - mean)).astype(jnp.bfloat16)
            dbias[h : h + 1, :] += jnp.sum(dscore.astype(jnp.float32) * same, axis=0, keepdims=True)
            dk_acc[:, cols] += dot(dscore, q_h)
            dq_acc[:, cols] = dot(dscore, k_h, TN) * 0.125

        unturn(dq_acc, 0, t, slice(None))

        @pl.when(t == 0)
        def _():
            ffn_fold.cross(0, 1)

        @pl.when(t == 2)
        def _():
            ffn_fold.cross(1, 2)

    @pl.loop(0, 4)
    def _(t):
        rows = pl.ds(pl.multiple_of(t * 256, 256), 256)
        unturn(dk_acc, 256, t, rows)
        dqkv_ref[pl.ds(2 * t, 2), :, 512:768] = (
            dv_acc[rows, :].astype(jnp.bfloat16).reshape(2, 128, 256)
        )

    for d in range(4):
        block = slice(256 * d, 256 * d + 256)
        grads = dot(
            a1_all[:, :, block].reshape(1024, 256), dqkv_ref[:, :, 0:768].reshape(1024, 768), TN
        )
        for b in range(8):
            attn_all[b, block, :] = jnp.concatenate(
                [slot_columns(grads, 2 * b + e, low_half) for e in (0, 1)], axis=1
            ).astype(jnp.bfloat16)
    for dz in (2, 3, 1, 0):
        attn_fold.start(0, dz)
    for dz in (3, 1):
        ffn_fold.cross(1, dz)

    @pl.loop(0, 4)
    def _(u):
        t = turn(u)
        part[pl.ds(2 * t, 2)] = dot(
            two(dqkv_ref, t, slice(0, 768)), wh_ref[...], NT, jnp.bfloat16
        ).reshape(2, 128, 1024)
        for s in (0, 1):

            @pl.when(u == s)
            def _():
                da1_sum.start(s)

            @pl.when(u == s + 2)
            def _():
                da1_sum.cross(s)

    for dz in (2, 3, 1):
        attn_fold.cross(1, dz)
    gain_rows = jnp.zeros((1, 1024), jnp.float32)
    for s in (0, 1):
        hidden = tok_own[s].astype(jnp.float32)
        inv = norm_rows(hidden)
        da1 = da1_sum.total(s)
        gain_rows = gain_rows + jnp.sum(da1 * (hidden * inv), axis=0, keepdims=True)
        grad = e2_ref[s] + back_rows(da1 * gain_one[...], hidden, inv)
        in_own[s] = grad.astype(jnp.bfloat16)
        leave.start(1, s)
    for b in range(8):
        small[b : b + 1, :] = gain_rows[:, 128 * b : 128 * b + 128]
    lane = lax.broadcasted_iota(jnp.int32, (8, 128), 1)
    line = lax.broadcasted_iota(jnp.int32, (8, 128), 0)
    bias_row = jnp.zeros((8, 128), jnp.float32)
    for h in range(4):
        value = jnp.sum(dbias[h : h + 1, :], axis=1, keepdims=True)
        bias_row = jnp.where((line == 0) & (lane == 4 * h + i), value, bias_row)
    small[16:24, :] = bias_row

    for chunk in (0, 1):
        ffn_fold.finish(chunk)
    ffn_back.start()
    small_out[...] = SmallSum(small, small_scratch).run()
    for dz in (2, 3, 1):
        attn_fold.cross(0, dz)
    ffn_back.wait()
    g_gate[...] = r_gate[...].astype(jnp.float32)
    g_up[...] = r_up[...].astype(jnp.float32)
    g_down[...] = r_down[...].astype(jnp.float32)
    for chunk in (1, 0):
        attn_fold.finish(chunk)
    attn_back.start()
    out_sum.finish()
    da1_sum.finish()
    for a in (0, 1):
        for s in (0, 1):
            leave.wait(a, s)
        leave.finish(a)
    for chunk in (0, 1):
        ffn_fold.drain(chunk)
        attn_fold.drain(chunk)
    attn_back.wait()
    g_qkv[...] = r_qkv[...].astype(jnp.float32)
    g_out[...] = r_out[...].astype(jnp.float32)


def layer(arrays):
    def vmem(dtype, *shape):
        return pltpu.VMEM(shape, dtype)

    low, full = jnp.bfloat16, jnp.float32
    blocks = vmem(low, 8, 128, 1024)
    own = vmem(low, 2, 128, 1024)
    heads = vmem(low, 1024, 256)
    grads = vmem(full, 1024, 256)
    return pl.pallas_call(
        layer_kernel,
        out_shape=[
            bf16(2, 128, 1024),
            bf16(2, 128, 1024),
            f32(256, 512),
            f32(256, 512),
            f32(1024, 128),
            f32(4, 256, 128),
            f32(256, 128),
            f32(24, 128),
        ],
        in_specs=[HB, HB, VM, VM, VM, VM, HB, HB, HB, VM, VM, SM],
        out_specs=[HB] * 2 + [VM] * 6,
        scratch_shapes=[
            blocks,
            blocks,
            vmem(full, 8, 128, 128),
            vmem(full, 8, 8, 128),
            own,
            vmem(low, 8, 1280, 128),
            vmem(low, 1024, 768),
            vmem(low, 256, 1024),
            heads,
            heads,
            heads,
            heads,
            vmem(full, 8, 1024),
            vmem(full, 8, 1024),
            blocks,
            vmem(full, 2, 128, 1024),
            blocks,
            blocks,
            vmem(low, 8, 3072, 128),
            vmem(low, 8, 3072, 128),
            blocks,
            blocks,
            blocks,
            vmem(full, 2, 128, 1024),
            vmem(full, 256, 256),
            grads,
            grads,
            own,
            own,
            vmem(full, 8, 256),
            vmem(full, 24, 128),
            vmem(low, 256, 512),
            vmem(low, 256, 512),
            vmem(low, 1024, 128),
            vmem(low, 4, 256, 128),
            vmem(low, 256, 128),
        ]
        + Home.sems(4)
        + Home.sems(2)
        + GroupGather.sems(4)
        + GroupGather.sems(1)
        + GroupGather.sems(1)
        + GroupSum.buffers()
        + GroupSum.buffers()
        + GroupSum.sems() * 4
        + Exchange.sems(2)
        + Exchange.sems(4)
        + Exchange.sems(2)
        + Exchange.sems(4)
        + SeqGather.sems(1)
        + SeqGather.sems(2)
        + SeqSum.scratch(3072, 2)
        + SeqSum.scratch(1280, 2)
        + SmallSum.scratch((24, 128)),
        compiler_params=pltpu.CompilerParams(
            collective_id=1, has_side_effects=True, vmem_limit_bytes=67_043_328
        ),
        name="layer",
    )(*arrays)


def on_group(
    tokens, segment_ids, variate_ids, time_ids, pad_mask, cotangent,
    w_qkv, w_out, w_gate, w_up, w_down, gain_attn, gain_ffn, variate_bias,
):
    i = lax.axis_index("dp")
    gain_one = gain_attn.astype(jnp.float32)[None]
    gain_two = gain_ffn.astype(jnp.float32)[None]
    packed = jnp.pad(w_qkv, ((0, 0), (0, 128))).reshape(256, 2, 4, 64)
    packed = packed.transpose(2, 0, 1, 3).reshape(4, 256, 128)
    frequency = jnp.exp(-jnp.log(10000.0) * jnp.arange(32, dtype=jnp.float32) / 32)
    angles = time_ids.astype(jnp.float32)[..., None] * frequency
    code_ids = jnp.where(pad_mask == 1, segment_ids, -1)
    labels = jnp.stack([segment_ids, variate_ids, code_ids], axis=-1).astype(jnp.float32)
    tables = jnp.concatenate(
        [jnp.cos(angles), jnp.sin(angles), labels, jnp.zeros((2, 128, 61), jnp.float32)], axis=-1
    )
    label_rows = jnp.stack([code_ids, variate_ids, segment_ids] + [segment_ids] * 5, axis=1)
    bias = jnp.where(
        jnp.arange(4)[None, :] == i, variate_bias.astype(jnp.float32).reshape(4, 4), 0.0
    ).sum(axis=1)
    output, input_grad, g_gate, g_up, g_down, g_qkv, g_out, small = layer(
        [
            tokens, cotangent, tables, label_rows.astype(jnp.float32), packed, w_out, w_gate, w_up, w_down,
            gain_one, gain_two, bias,
        ]
    )
    g_qkv = g_qkv.reshape(4, 256, 2, 64).transpose(1, 2, 0, 3).reshape(256, 512)[:, :384]
    small = small.reshape(3, 1024)
    return (
        output, input_grad, g_qkv, g_out, g_gate, g_up, g_down, small[0], small[1], small[2, :16],
    )


def solution(mesh):
    in_specs = (
        P("dp", "seq", None),
        P("dp", "seq"),
        P("dp", "seq"),
        P("dp", "seq"),
        P("dp", "seq"),
        P("dp", "seq", None),
        P("dp", "seq"),
        P("dp", "seq"),
        P("dp", "seq"),
        P("dp", "seq"),
        P("dp", "seq"),
        P(),
        P(),
        P(),
    )
    out_specs = (
        P("dp", "seq", None),
        P("dp", "seq", None),
        P("dp", "seq"),
        P("dp", "seq"),
        P("dp", "seq"),
        P("dp", "seq"),
        P("dp", "seq"),
        P(),
        P(),
        P(),
    )
    grouped = mesh.shape["dp"] == 4 and mesh.shape["seq"] == 8
    return jax.shard_map(
        on_group if grouped else on_device, mesh=mesh, in_specs=in_specs, out_specs=out_specs, check_vma=False
    )
```

```python
import functools

import jax
import jax.numpy as jnp
from jax import lax
from jax.experimental import pallas as pl
from jax.experimental.pallas import tpu as pltpu
from jax.sharding import PartitionSpec as P

HEADS = 16
HEAD_DIM = 64
WINDOW = 512


EPSILON = 1e-06
NEGATIVE = -1e30


def passed_along(block, axis, distance):
    devices = range(lax.axis_size(axis))
    route = [(i - distance, i) for i in devices if i - distance in devices]
    return lax.ppermute(block, axis, route)


def norm_scale(hidden):
    return lax.rsqrt(jnp.mean(hidden * hidden, axis=-1, keepdims=True) + EPSILON)


def norm_back(grad_in, hidden, inv_rms):
    return inv_rms * grad_in - hidden * inv_rms * inv_rms * inv_rms * jnp.mean(
        grad_in * hidden, axis=-1, keepdims=True
    )


def rope_tables(time_row, half_dim):
    frequency = jnp.exp(-jnp.log(10000.0) * jnp.arange(half_dim, dtype=jnp.float32) / half_dim)
    angles = time_row.astype(jnp.float32)[:, None] * frequency[None, :]
    return (jnp.cos(angles)[:, None, :], jnp.sin(angles)[:, None, :])


def rotate(values_in, cos_table, sine_table):
    half_dim = cos_table.shape[-1]
    first_half = values_in[..., :half_dim]
    second_half = values_in[..., half_dim:]
    return jnp.concatenate(
        [
            first_half * cos_table - second_half * sine_table,
            second_half * cos_table + first_half * sine_table,
        ],
        axis=-1,
    )


def rotate_back(grad_in, cos_table, sine_table):
    half_dim = cos_table.shape[-1]
    first_half = grad_in[..., :half_dim]
    second_half = grad_in[..., half_dim:]
    return jnp.concatenate(
        [
            first_half * cos_table + second_half * sine_table,
            second_half * cos_table - first_half * sine_table,
        ],
        axis=-1,
    )


def masked_scores(query_rot, keys_all, labels_own, labels_keys, var_bias, hop_count):
    row_count = query_rot.shape[0]
    key_count = keys_all.shape[0]
    offsets = (
        jnp.arange(key_count)[None, :] - hop_count * row_count - jnp.arange(row_count)[:, None]
    )
    allowed = (
        (jnp.abs(offsets) <= WINDOW)
        & (labels_own[0][:, None] == labels_keys[0][None, :])
        & ((labels_keys[2][None, :] == 1) | (offsets == 0))
    )
    same_var = (labels_own[1][:, None] == labels_keys[1][None, :]).astype(jnp.float32)
    scores = jnp.einsum(
        "qhd,khd->hqk", query_rot, keys_all, preferred_element_type=jnp.float32
    ) * HEAD_DIM ** (-0.5)
    scores = scores + var_bias[:, None, None] * same_var[None]
    return (jnp.where(allowed[None], scores, NEGATIVE), same_var)


def fetch_weights(shards):
    row_blocks = (
        lax.all_gather(shards[0], "dp", axis=0, tiled=True),
        lax.all_gather(shards[1], "dp", axis=0, tiled=True),
        lax.all_gather(shards[2], "dp", axis=0, tiled=True),
        lax.all_gather(shards[3], "dp", axis=0, tiled=True),
        lax.all_gather(shards[4], "dp", axis=0, tiled=True),
    )
    return (
        lax.all_gather(row_blocks[0], "seq", axis=1, tiled=True),
        lax.all_gather(row_blocks[1], "seq", axis=1, tiled=True),
        lax.all_gather(row_blocks[2], "seq", axis=1, tiled=True),
        lax.all_gather(row_blocks[3], "seq", axis=1, tiled=True),
        lax.all_gather(row_blocks[4], "seq", axis=1, tiled=True),
    )


def fetch_keep(shards):
    row_blocks = (
        lax.all_gather(shards[0], "dp", axis=0, tiled=True),
        lax.all_gather(shards[1], "dp", axis=0, tiled=True),
        lax.all_gather(shards[2], "dp", axis=0, tiled=True),
        lax.all_gather(shards[3], "dp", axis=0, tiled=True),
        lax.all_gather(shards[4], "dp", axis=0, tiled=True),
    )
    return (
        lax.all_gather(row_blocks[0], "seq", axis=1, tiled=True),
        lax.all_gather(row_blocks[1], "seq", axis=1, tiled=True),
        lax.all_gather(row_blocks[2], "seq", axis=1, tiled=True),
        lax.all_gather(row_blocks[3], "seq", axis=1, tiled=True),
        lax.all_gather(row_blocks[4], "seq", axis=1, tiled=True),
    )


def reduce_last(grads_full):
    col_sums = (
        lax.psum_scatter(grads_full[0], "seq", scatter_dimension=1, tiled=True),
        lax.psum_scatter(grads_full[1], "seq", scatter_dimension=1, tiled=True),
        lax.psum_scatter(grads_full[2], "seq", scatter_dimension=1, tiled=True),
        lax.psum_scatter(grads_full[3], "seq", scatter_dimension=1, tiled=True),
        lax.psum_scatter(grads_full[4], "seq", scatter_dimension=1, tiled=True),
    )
    return (
        lax.psum_scatter(
            col_sums[0].astype(jnp.bfloat16), "dp", scatter_dimension=0, tiled=True
        ).astype(jnp.float32),
        lax.psum_scatter(
            col_sums[1].astype(jnp.bfloat16), "dp", scatter_dimension=0, tiled=True
        ).astype(jnp.float32),
        lax.psum_scatter(
            col_sums[2].astype(jnp.bfloat16), "dp", scatter_dimension=0, tiled=True
        ).astype(jnp.float32),
        lax.psum_scatter(
            col_sums[3].astype(jnp.bfloat16), "dp", scatter_dimension=0, tiled=True
        ).astype(jnp.float32),
        lax.psum_scatter(
            col_sums[4].astype(jnp.bfloat16), "dp", scatter_dimension=0, tiled=True
        ).astype(jnp.float32),
    )


def weight_grads(pieces):
    (
        normed_one,
        grad_qkv,
        attended,
        grad_branch,
        normed_two,
        grad_gate,
        grad_up,
        hidden,
        grad_ffn,
    ) = pieces
    grad_w_qkv = jnp.einsum("td,tf->df", normed_one, grad_qkv, preferred_element_type=jnp.float32)
    grad_w_out = jnp.einsum("ti,to->io", attended, grad_branch, preferred_element_type=jnp.float32)
    grad_w_gate = jnp.einsum("td,tf->df", normed_two, grad_gate, preferred_element_type=jnp.float32)
    grad_w_up = jnp.einsum("td,tf->df", normed_two, grad_up, preferred_element_type=jnp.float32)
    grad_w_down = jnp.einsum("tf,td->fd", hidden, grad_ffn, preferred_element_type=jnp.float32)
    return (grad_w_qkv, grad_w_out, grad_w_gate, grad_w_up, grad_w_down)


def on_device(
    tokens,
    segment_ids,
    variate_ids,
    time_ids,
    pad_mask,
    cotangent,
    w_qkv,
    w_out,
    w_gate,
    w_up,
    w_down,
    gain_attn,
    gain_ffn,
    variate_bias,
):
    micro_count, row_count, model_width = tokens.shape
    hop_count = -(-WINDOW // row_count)
    key_count = (2 * hop_count + 1) * row_count
    shards = (w_qkv, w_out, w_gate, w_up, w_down)
    var_bias = variate_bias.astype(jnp.float32)
    gain_one = gain_attn.astype(jnp.float32)
    gain_two = gain_ffn.astype(jnp.float32)
    bias_total = jnp.zeros(var_bias.shape, jnp.float32)
    gain_one_total = jnp.zeros(gain_one.shape, jnp.float32)
    gain_two_total = jnp.zeros(gain_two.shape, jnp.float32)
    grad_totals = None
    saved = []
    outputs = []
    input_grads = []
    held_weights = fetch_weights(shards)
    for micro_step in range(micro_count):
        if micro_step == 0:
            weights = held_weights
        else:
            weights = fetch_keep(shards)
        resid_in = tokens[micro_step].astype(jnp.float32)
        inv_one = norm_scale(resid_in)
        normed_one = (resid_in * inv_one * gain_one).astype(jnp.bfloat16)
        qkv_proj = jnp.dot(normed_one, weights[0], preferred_element_type=jnp.float32)
        cos_table, sine_table = rope_tables(time_ids[micro_step], HEAD_DIM // 2)
        query_rot = rotate(
            qkv_proj[:, :model_width].reshape(row_count, HEADS, HEAD_DIM), cos_table, sine_table
        ).astype(jnp.bfloat16)
        key_rot = rotate(
            qkv_proj[:, model_width : 2 * model_width].reshape(row_count, HEADS, HEAD_DIM),
            cos_table,
            sine_table,
        ).astype(jnp.bfloat16)
        value_own = qkv_proj[:, 2 * model_width :].astype(jnp.bfloat16)
        kv_own = jnp.stack([key_rot.reshape(row_count, model_width), value_own])
        labels_own = jnp.stack(
            [segment_ids[micro_step], variate_ids[micro_step], pad_mask[micro_step]]
        )
        kv_slots = []
        label_slots = []
        for slot_index in range(2 * hop_count + 1):
            offset = slot_index - hop_count
            if offset == 0:
                kv_slots.append(kv_own)
                label_slots.append(labels_own)
            else:
                kv_slots.append(passed_along(kv_own, "seq", -offset))
                label_slots.append(passed_along(labels_own, "seq", -offset))
        kv_all = jnp.concatenate(kv_slots, axis=1)
        labels_keys = jnp.concatenate(label_slots, axis=1)
        keys_all = kv_all[0].reshape(key_count, HEADS, HEAD_DIM)
        values_all = kv_all[1].reshape(key_count, HEADS, HEAD_DIM)
        scores, same_var = masked_scores(
            query_rot, keys_all, labels_own, labels_keys, var_bias, hop_count
        )
        maxima = jnp.max(scores, axis=-1, keepdims=True)
        exp_shift = jnp.exp(scores - maxima)
        denom_sum = jnp.sum(exp_shift, axis=-1, keepdims=True)
        log_norm = maxima + jnp.log(denom_sum)
        prob_low = (exp_shift / denom_sum).astype(jnp.bfloat16)
        attended = jnp.einsum(
            "hqk,khd->qhd", prob_low, values_all, preferred_element_type=jnp.float32
        )
        attended = attended.reshape(row_count, model_width).astype(jnp.bfloat16)
        resid_mid = resid_in + jnp.dot(attended, weights[1], preferred_element_type=jnp.float32)
        inv_two = norm_scale(resid_mid)
        normed_two = (resid_mid * inv_two * gain_two).astype(jnp.bfloat16)
        gate_proj = jnp.dot(normed_two, weights[2], preferred_element_type=jnp.float32)
        up_proj = jnp.dot(normed_two, weights[3], preferred_element_type=jnp.float32)
        gate_sig = jax.nn.sigmoid(gate_proj)
        hidden = (gate_proj * gate_sig * up_proj).astype(jnp.bfloat16)
        ffn_out = jnp.dot(hidden, weights[4], preferred_element_type=jnp.float32)
        outputs.append((resid_mid + ffn_out).astype(jnp.bfloat16))
        grad_out = cotangent[micro_step].astype(jnp.float32)
        grad_ffn = grad_out.astype(jnp.bfloat16)
        grad_hidden = jnp.einsum(
            "td,fd->tf", grad_ffn, weights[4], preferred_element_type=jnp.float32
        )
        grad_gate = (
            grad_hidden * up_proj * gate_sig * (1.0 + gate_proj * (1.0 - gate_sig))
        ).astype(jnp.bfloat16)
        grad_up = (grad_hidden * gate_proj * gate_sig).astype(jnp.bfloat16)
        grad_normed_two = jnp.einsum(
            "tf,df->td", grad_gate, weights[2], preferred_element_type=jnp.float32
        )
        grad_normed_two = grad_normed_two + jnp.einsum(
            "tf,df->td", grad_up, weights[3], preferred_element_type=jnp.float32
        )
        gain_two_total = gain_two_total + jnp.sum(grad_normed_two * resid_mid * inv_two, axis=0)
        grad_mid = grad_out + norm_back(grad_normed_two * gain_two, resid_mid, inv_two)
        grad_branch = grad_mid.astype(jnp.bfloat16)
        grad_attended = jnp.einsum(
            "to,io->ti", grad_branch, weights[1], preferred_element_type=jnp.float32
        )
        grad_attended = grad_attended.astype(jnp.bfloat16).reshape(row_count, HEADS, HEAD_DIM)
        scores, same_var = masked_scores(
            query_rot, keys_all, labels_own, labels_keys, var_bias, hop_count
        )
        prob_full = jnp.exp(scores - log_norm)
        prob_low = prob_full.astype(jnp.bfloat16)
        grad_values = jnp.einsum(
            "hqk,qhd->khd", prob_low, grad_attended, preferred_element_type=jnp.float32
        )
        grad_prob = jnp.einsum(
            "qhd,khd->hqk", grad_attended, values_all, preferred_element_type=jnp.float32
        )
        grad_scores = prob_full * (
            grad_prob - jnp.sum(prob_full * grad_prob, axis=-1, keepdims=True)
        )
        grad_scores = grad_scores.astype(jnp.bfloat16)
        bias_total = bias_total + jnp.sum(
            grad_scores.astype(jnp.float32) * same_var[None], axis=(1, 2)
        )
        grad_query = jnp.einsum(
            "hqk,khd->qhd", grad_scores, keys_all, preferred_element_type=jnp.float32
        ) * HEAD_DIM ** (-0.5)
        grad_keys = jnp.einsum(
            "hqk,qhd->khd", grad_scores, query_rot, preferred_element_type=jnp.float32
        ) * HEAD_DIM ** (-0.5)
        grad_kv = jnp.stack(
            [grad_keys.reshape(key_count, model_width), grad_values.reshape(key_count, model_width)]
        )
        grad_kv_own = grad_kv[:, hop_count * row_count : (hop_count + 1) * row_count]
        for slot_index in range(2 * hop_count + 1):
            offset = slot_index - hop_count
            if offset != 0:
                slot_grad = grad_kv[:, slot_index * row_count : (slot_index + 1) * row_count]
                grad_kv_own = grad_kv_own + passed_along(
                    slot_grad.astype(jnp.bfloat16), "seq", offset
                ).astype(slot_grad.dtype)
        grad_q_plain = rotate_back(grad_query, cos_table, sine_table).reshape(
            row_count, model_width
        )
        grad_k_plain = rotate_back(
            grad_kv_own[0].reshape(row_count, HEADS, HEAD_DIM), cos_table, sine_table
        ).reshape(row_count, model_width)
        grad_qkv = jnp.concatenate([grad_q_plain, grad_k_plain, grad_kv_own[1]], axis=1).astype(
            jnp.bfloat16
        )
        grad_normed_one = jnp.einsum(
            "tf,df->td", grad_qkv, weights[0], preferred_element_type=jnp.float32
        )
        gain_one_total = gain_one_total + jnp.sum(grad_normed_one * resid_in * inv_one, axis=0)
        grad_input = grad_mid + norm_back(grad_normed_one * gain_one, resid_in, inv_one)
        input_grads.append(grad_input.astype(jnp.bfloat16))
        pieces = (
            normed_one,
            grad_qkv,
            attended,
            grad_branch,
            normed_two,
            grad_gate,
            grad_up,
            hidden,
            grad_ffn,
        )
        saved.append(pieces)
    joined = tuple(
        (
            jnp.concatenate([entry[index] for entry in saved], axis=0)
            for index in range(len(saved[0]))
        )
    )
    grad_totals = reduce_last(weight_grads(joined))
    bias_sum, gain_one_sum, gain_two_sum = lax.psum(
        (bias_total, gain_one_total, gain_two_total), ("dp", "seq")
    )
    return (
        jnp.stack(outputs),
        jnp.stack(input_grads),
        grad_totals[0],
        grad_totals[1],
        grad_totals[2],
        grad_totals[3],
        grad_totals[4],
        gain_one_sum,
        gain_two_sum,
        bias_sum,
    )


MESH = pl.DeviceIdType.MESH
VM = pl.BlockSpec(memory_space=pltpu.VMEM)
HB = pl.BlockSpec(memory_space=pl.ANY)
SM = pl.BlockSpec(memory_space=pltpu.SMEM)
DMA = pltpu.SemaphoreType.DMA
NT = (((1,), (1,)), ((), ()))
TN = (((0,), (0,)), ((), ()))
EVERY = slice(None)


def bf16(*shape):
    return jax.ShapeDtypeStruct(shape, jnp.bfloat16)


def f32(*shape):
    return jax.ShapeDtypeStruct(shape, jnp.float32)


def dot(a, b, dims=None, out=jnp.float32):
    dims = (((1,), (0,)), ((), ())) if dims is None else dims
    return lax.dot_general(a, b, dims, preferred_element_type=jnp.float32).astype(out)


def at(dp, seq):
    return {"dp": dp, "seq": seq}


def place():
    return lax.axis_index("dp"), lax.axis_index("seq")


def ring(i):
    return i + 1 - 2 * lax.rem(i, 2), lax.rem(i + 2, 4)


def owned(i, s):
    return 4 * lax.rem(i, 2) + 2 * s + i // 2


def keeper(j):
    return 2 * lax.rem(j, 2) + j // 4


def send(src, dst, send_sem, recv_sem, peer):
    return pltpu.make_async_remote_copy(
        src_ref=src,
        dst_ref=dst,
        send_sem=send_sem,
        recv_sem=recv_sem,
        device_id=peer,
        device_id_type=MESH,
    )


def landed(ref, sem):
    pltpu.make_async_copy(ref, ref, sem).wait()


def meet(peers, home=False):
    i, j = place()
    barrier = pltpu.get_barrier_semaphore()
    for peer in peers:
        pl.semaphore_signal(barrier, inc=1, device_id=peer, device_id_type=MESH)
    if home:
        target, stays = keeper(j), keeper(j) == i
        for s in (0, 1):

            @pl.when(jnp.logical_not(stays & (owned(i, s) == j)))
            def _():
                pl.semaphore_signal(
                    barrier, inc=1, device_id=at(target, owned(i, s)), device_id_type=MESH
                )

        pl.semaphore_wait(barrier, len(peers) + jnp.where(stays, 1, 2))
    else:
        pl.semaphore_wait(barrier, len(peers))


def dp_peers():
    i, j = place()
    return [at(lax.rem(i + step, 4), j) for step in (1, 2, 3)]


def seq_peers():
    i, j = place()
    z, y = j // 2, lax.rem(j, 2)
    return [at(i, 2 * lax.rem(z + step, 4) + y) for step in (1, 2, 3)] + [at(i, 2 * z + 1 - y)]


class Home:
    def __init__(self, ins, outs, sems, slotted):
        self.ins, self.outs, self.slotted = ins, outs, slotted
        self.send_sem, self.recv_sem = sems

    @staticmethod
    def sems(count):
        return [DMA((count, 2)), DMA((count, 2))]

    def target(self, a, s):
        i, _ = place()
        return self.outs[a].at[s if self.slotted else owned(i, s)]

    def start(self, a, s):
        i, j = place()
        slot = lax.rem(j // 2, 2)
        src, dst = self.ins[a].at[s], self.outs[a].at[slot if self.slotted else j]
        here = (keeper(j) == i) & (owned(i, s) == j)

        @pl.when(jnp.logical_not(here))
        def _():
            peer = at(keeper(j), owned(i, s))
            send(src, dst, self.send_sem.at[a, s], self.recv_sem.at[a, slot], peer).start()

        @pl.when(here)
        def _():
            pltpu.make_async_copy(src, dst, self.recv_sem.at[a, slot]).start()

    def wait(self, a, s):
        landed(self.target(a, s), self.recv_sem.at[a, s])

    def finish(self, a):
        i, j = place()
        for s in (0, 1):

            @pl.when(jnp.logical_not((keeper(j) == i) & (owned(i, s) == j)))
            def _():
                landed(self.ins[a].at[s], self.send_sem.at[a, s])


class GroupGather:
    def __init__(self, outs, sems):
        self.outs = outs
        self.s_core, self.r_core, self.s_x, self.r_x, self.s_on, self.r_on = sems

    @staticmethod
    def sems(count):
        return [DMA((count, 2))] * 6

    def push(self, a, s):
        i, j = place()
        core, across = ring(i)
        block = self.outs[a].at[owned(i, s)]
        send(block, block, self.s_x.at[a, s], self.r_x.at[a, s], at(across, j)).start()
        send(block, block, self.s_core.at[a, s], self.r_core.at[a, s], at(core, j)).start()

    def relay(self, a, s):
        i, j = place()
        core, across = ring(i)
        block = self.outs[a].at[owned(across, s)]
        landed(block, self.r_x.at[a, s])
        send(block, block, self.s_on.at[a, s], self.r_on.at[a, s], at(core, j)).start()

    def finish(self, a):
        i, _ = place()
        core, _ = ring(i)
        for s in (0, 1):
            landed(self.outs[a].at[owned(core, s)], self.r_core.at[a, s])
            landed(self.outs[a].at[owned(lax.rem(core + 2, 4), s)], self.r_on.at[a, s])
        for s in (0, 1):
            for sem in (self.s_x, self.s_core, self.s_on):
                landed(self.outs[a].at[s], sem.at[a, s])


class GroupSum:
    def __init__(self, parts, buffers, sems):
        self.parts = parts
        self.near, self.far = buffers
        self.s_core, self.r_core, self.s_x, self.r_x = sems

    @staticmethod
    def buffers():
        block = (128, 1024)
        return [pltpu.VMEM((2, 2) + block, jnp.bfloat16), pltpu.VMEM((2,) + block, jnp.bfloat16)]

    @staticmethod
    def sems():
        return [DMA((2, 2)), DMA((2, 2)), DMA((2,)), DMA((2,))]

    def start(self, s):
        i, j = place()
        core, _ = ring(i)
        for side, owner in ((0, lax.rem(core + 2, 4)), (1, core)):
            send(
                self.parts.at[owned(owner, s)],
                self.near.at[side, s],
                self.s_core.at[side, s],
                self.r_core.at[side, s],
                at(core, j),
            ).start()

    def cross(self, s):
        i, j = place()
        _, across = ring(i)
        landed(self.near.at[0, s], self.r_core.at[0, s])
        both = self.parts[owned(across, s)].astype(jnp.float32)
        both = both + self.near[0, s].astype(jnp.float32)
        self.near[0, s] = both.astype(jnp.bfloat16)
        send(
            self.near.at[0, s], self.far.at[s], self.s_x.at[s], self.r_x.at[s], at(across, j)
        ).start()

    def total(self, s):
        i, _ = place()
        landed(self.near.at[1, s], self.r_core.at[1, s])
        both = self.parts[owned(i, s)].astype(jnp.float32) + self.near[1, s].astype(jnp.float32)
        landed(self.far.at[s], self.r_x.at[s])
        return both + self.far[s].astype(jnp.float32)

    def finish(self):
        for s in (0, 1):
            landed(self.near.at[0, s], self.s_x.at[s])
            for side in (0, 1):
                landed(self.near.at[side, s], self.s_core.at[side, s])


class Exchange:
    def __init__(self, pieces, sems):
        self.pieces = pieces
        self.send_sem, self.recv_sem, self.own_sem = sems
        self.copies = []

    @staticmethod
    def sems(count):
        return [DMA((3, count)), DMA((3, count)), DMA((count,))]

    def start(self):
        i, j = place()
        for step in (2, 3, 1):
            other = lax.rem(i + step, 4)
            for index, (src, dst) in enumerate(self.pieces(i, other)):
                copy = send(
                    src,
                    dst,
                    self.send_sem.at[step - 1, index],
                    self.recv_sem.at[step - 1, index],
                    at(other, j),
                )
                copy.start()
                self.copies.append(copy)
        for index, (src, dst) in enumerate(self.pieces(i, i)):
            copy = pltpu.make_async_copy(src, dst, self.own_sem.at[index])
            copy.start()
            self.copies.append(copy)

    def wait(self):
        for copy in self.copies:
            copy.wait()


ARRIVAL = ((1, 2, 3), (2, 0, 3), (1, 3, 0), (2, 1, 0))
LEAVING = ((2, 3, 1), (0, 2, 3), (3, 1, 0), (1, 0, 2))


def pick(table, z, n):
    row = [entry[n] for entry in table]
    return jnp.where(z == 0, row[0], jnp.where(z == 1, row[1], jnp.where(z == 2, row[2], row[3])))


def inner(z):
    return (z == 1) | (z == 2)


class SeqGather:
    def __init__(self, full, chunks, sems):
        self.full, self.chunks = full, chunks
        self.s_z, self.r_z, self.s_on, self.s_y, self.r_y = sems

    @staticmethod
    def sems(count):
        return [DMA((count, 2)), DMA((count, 4)), DMA((count, 4)), DMA((count, 4)), DMA((count, 4))]

    def block(self, chunk, z, y):
        start, size = self.chunks[chunk]
        return self.full.at[2 * z + y, pl.ds(start, size)]

    def start(self, chunk):
        i, j = place()
        z, y = j // 2, lax.rem(j, 2)
        own = self.block(chunk, z, y)
        first, second = pick(((2, 1), (2, 0), (1, 3), (1, 2)), z, 0), pick(
            ((2, 1), (2, 0), (1, 3), (1, 2)), z, 1
        )
        for n, target in enumerate((first, second)):
            peer = at(i, 2 * target + y)
            send(own, own, self.s_z.at[chunk, n], self.r_z.at[chunk, z], peer).start()
        send(own, own, self.s_y.at[chunk, z], self.r_y.at[chunk, z], at(i, 2 * z + 1 - y)).start()

    def forward(self, chunk, n):
        i, j = place()
        z, y = j // 2, lax.rem(j, 2)
        source = pick(ARRIVAL, z, n)
        block = self.block(chunk, source, y)
        landed(block, self.r_z.at[chunk, source])

        @pl.when(inner(z) & (source // 2 != z // 2) | inner(z) & inner(source))
        def _():
            send(
                block,
                block,
                self.s_on.at[chunk, source],
                self.r_z.at[chunk, source],
                at(i, 2 * jnp.where(z == 1, 0, 3) + y),
            ).start()

        peer = at(i, 2 * z + 1 - y)
        send(block, block, self.s_y.at[chunk, source], self.r_y.at[chunk, source], peer).start()

    def arrived(self, chunk, source):
        _, j = place()
        y = lax.rem(j, 2)
        landed(self.block(chunk, source, 1 - y), self.r_y.at[chunk, source])

    def drain(self, chunk):
        _, j = place()
        z = j // 2
        own = self.block(chunk, z, lax.rem(j, 2))
        for n in (0, 1):
            landed(own, self.s_z.at[chunk, n])
        landed(own, self.s_y.at[chunk, z])
        for n in (0, 1, 2):
            source = pick(ARRIVAL, z, n)
            landed(own, self.s_y.at[chunk, source])

            @pl.when(inner(z) & (source // 2 != z // 2) | inner(z) & inner(source))
            def _():
                landed(own, self.s_on.at[chunk, source])

    def finish(self, chunk):
        _, j = place()
        self.arrived(chunk, j // 2)
        for n in (0, 1, 2):
            self.arrived(chunk, pick(ARRIVAL, j // 2, n))
        self.drain(chunk)


class SeqSum:
    def __init__(self, parts, chunks, scratch):
        self.parts, self.chunks = parts, chunks
        self.near, self.far = scratch[:2]
        self.s_y, self.r_y, self.s_z, self.r_z = scratch[2:]

    @staticmethod
    def scratch(rows, count):
        return [
            pltpu.VMEM((4, rows, 128), jnp.bfloat16),
            pltpu.VMEM((4, rows, 128), jnp.bfloat16),
            DMA((count, 4)),
            DMA((count, 4)),
            DMA((count, 4)),
            DMA((count, 4)),
        ]

    def start(self, chunk, row):
        i, j = place()
        z, y = j // 2, lax.rem(j, 2)
        rows = pl.ds(*self.chunks[chunk])
        send(
            self.parts.at[2 * row + 1 - y, rows],
            self.near.at[row, rows],
            self.s_y.at[chunk, row],
            self.r_y.at[chunk, row],
            at(i, 2 * z + 1 - y),
        ).start()

    def start_rest(self, chunk):
        z = lax.axis_index("seq") // 2
        for n in (0, 1, 2):
            self.start(chunk, pick(LEAVING, z, n))

    def each(self, chunk, body):
        start, size = self.chunks[chunk]

        @pl.loop(0, size // 256)
        def _(t):
            body(pl.ds(pl.multiple_of(start + t * 256, 256), 256))

    def cross(self, chunk, n):
        i, j = place()
        z, y = j // 2, lax.rem(j, 2)
        rows = pl.ds(*self.chunks[chunk])
        row = pick(LEAVING, z, n)
        landed(self.near.at[row, rows], self.r_y.at[chunk, row])

        def add(part):
            both = self.parts[2 * row + y, part, :].astype(jnp.float32)
            both = both + self.near[row, part, :].astype(jnp.float32)
            self.near[row, part, :] = both.astype(jnp.bfloat16)

        def add_more(part):
            both = self.parts[2 * row + y, part, :].astype(jnp.float32)
            both = both + self.near[row, part, :].astype(jnp.float32)
            both = both + self.far[2 + lax.rem(row, 2), part, :].astype(jnp.float32)
            self.near[row, part, :] = both.astype(jnp.bfloat16)

        if n == 0:
            self.each(chunk, add)
        else:

            @pl.when(inner(z))
            def _():
                held = 2 + lax.rem(row, 2)
                landed(self.far.at[held, rows], self.r_z.at[chunk, held])
                self.each(chunk, add_more)

            @pl.when(jnp.logical_not(inner(z)))
            def _():
                self.each(chunk, add)

        beside = jnp.where(z == 0, 1, 2)
        target = jnp.where(inner(z), row, beside)
        spot = jnp.where(target == row, z // 2, 2 + lax.rem(row, 2))
        send(
            self.near.at[row, rows],
            self.far.at[spot, rows],
            self.s_z.at[chunk, row],
            self.r_z.at[chunk, spot],
            at(i, 2 * target + y),
        ).start()

    def finish(self, chunk):
        _, j = place()
        z = j // 2
        rows = pl.ds(*self.chunks[chunk])
        landed(self.near.at[z, rows], self.r_y.at[chunk, z])
        for spot in (0, 1):
            landed(self.far.at[spot, rows], self.r_z.at[chunk, spot])

        def add(part):
            total = self.parts[j, part, :].astype(jnp.float32)
            total = total + self.near[z, part, :].astype(jnp.float32)
            for spot in (0, 1):
                total = total + self.far[spot, part, :].astype(jnp.float32)
            self.near[z, part, :] = total.astype(jnp.bfloat16)

        self.each(chunk, add)

    def drain(self, chunk):
        z = lax.axis_index("seq") // 2
        rows = pl.ds(*self.chunks[chunk])
        landed(self.near.at[z, rows], self.s_y.at[chunk, z])
        for n in (0, 1, 2):
            row = pick(LEAVING, z, n)
            landed(self.near.at[row, rows], self.s_y.at[chunk, row])
            landed(self.near.at[row, rows], self.s_z.at[chunk, row])


class SmallSum:
    def __init__(self, value, scratch):
        self.value = value
        self.stages, self.sems = scratch[:3], scratch[3:]

    @staticmethod
    def scratch(shape):
        return [pltpu.VMEM((count,) + shape, jnp.float32) for count in (4, 4, 2)] + [
            DMA((count,)) for count in (3, 3, 3, 3, 1, 1)
        ]

    def round(self, stage):
        i, j = place()
        z, y = j // 2, lax.rem(j, 2)
        return ((i, dp_peers()), (z, seq_peers()[:3]), (y, seq_peers()[3:]))[stage]

    def start(self, stage):
        spot, peers = self.round(stage)
        held = self.stages[stage]
        held[spot] = self.value[...] if stage == 0 else self.total(stage - 1)
        for step, peer in enumerate(peers):
            send(
                held.at[spot],
                held.at[spot],
                self.sems[2 * stage].at[step],
                self.sems[2 * stage + 1].at[step],
                peer,
            ).start()

    def total(self, stage):
        held = self.stages[stage]
        for step in range(held.shape[0] - 1):
            landed(held.at[0], self.sems[2 * stage + 1].at[step])
            landed(held.at[0], self.sems[2 * stage].at[step])
        total = held[0]
        for index in range(1, held.shape[0]):
            total = total + held[index]
        return total


def swap_halves(x):
    lane = lax.broadcasted_iota(jnp.int32, x.shape, 1)
    width = x.shape[1]
    return jnp.where(lane % 64 < 32, pltpu.roll(x, width - 32, 1), pltpu.roll(x, 32, 1))


def angle_tables(table):
    lane = lax.broadcasted_iota(jnp.int32, table.shape, 1)
    by_32, by_64, by_96 = (pltpu.roll(table, shift, 1) for shift in (32, 64, 96))
    first, second, third = lane < 32, lane < 64, lane < 96
    cos_t = jnp.where(first, table, jnp.where(second, by_32, jnp.where(third, by_64, by_96)))
    sin_t = jnp.where(first, -by_96, jnp.where(second, table, jnp.where(third, -by_32, by_64)))
    return cos_t, sin_t


SLOTS = (
    (0, 1, 2, 4, 5, 6, 8, 9, 10, 12, 13, 14),
    (0, 2, 3, 4, 6, 7, 8, 10, 11, 12, 14, 15),
)


def attention_pieces(packed, w_out, dst):
    def pieces(me, other):
        _, j = place()
        spot = lax.rem(other + 2 * lax.rem(j, 2), 4)
        return [
            (packed.at[spot], dst.at[j, pl.ds(256 * me, 256)]),
            (w_out.at[pl.ds(64 * other, 64)], dst.at[j, pl.ds(1024 + 64 * me, 64)]),
        ]

    return pieces


def ffn_pieces(w_gate, w_up, w_down, dst):
    def pieces(me, other):
        _, j = place()
        columns = pl.ds(pl.multiple_of(128 * other, 128), 128)
        pairs = [
            (w_gate.at[:, columns], dst.at[j, pl.ds(256 * me, 256)]),
            (w_up.at[:, columns], dst.at[j, pl.ds(1024 + 256 * me, 256)]),
        ]
        for half in (0, 1):
            pairs.append(
                (
                    w_down.at[pl.ds(512 * half + 128 * other, 128)],
                    dst.at[j, pl.ds(2048 + 256 * me + 128 * half, 128)],
                )
            )
        return pairs

    return pieces


def head_weights(full, wh_ref, wm_ref, low_half):
    def column(m, rows):
        first, second = SLOTS[0][m], SLOTS[1][m]
        one = full[first // 2, rows, 64 * (first % 2) : 64 * (first % 2) + 64]
        two = full[second // 2, rows, 64 * (second % 2) : 64 * (second % 2) + 64]
        return jnp.where(low_half, one, two)

    @pl.loop(0, 4)
    def _(t):
        rows = pl.ds(pl.multiple_of(t * 256, 256), 256)
        for m in range(0, 12, 2):
            wh_ref[rows, 64 * m : 64 * m + 128] = jnp.concatenate(
                [column(m, rows), column(m + 1, rows)], axis=1
            )

    for b in range(8):
        wm_ref[:, 128 * b : 128 * b + 128] = full[b, 1024:1280, :]


def norm_rows(hidden):
    return lax.rsqrt(jnp.mean(hidden * hidden, axis=1, keepdims=True) + EPSILON)


def return_attention(src, g_qkv, g_out):
    def pieces(me, other):
        _, j = place()
        spot = lax.rem(me + 2 * lax.rem(j, 2), 4)
        return [
            (src.at[pl.ds(256 * other, 256)], g_qkv.at[spot]),
            (src.at[pl.ds(1024 + 64 * other, 64)], g_out.at[pl.ds(64 * me, 64)]),
        ]

    return pieces


def return_ffn(src, g_gate, g_up, g_down):
    def pieces(me, other):
        columns = pl.ds(pl.multiple_of(128 * me, 128), 128)
        pairs = [
            (src.at[pl.ds(256 * other, 256)], g_gate.at[:, columns]),
            (src.at[pl.ds(1024 + 256 * other, 256)], g_up.at[:, columns]),
        ]
        for half in (0, 1):
            pairs.append(
                (
                    src.at[pl.ds(2048 + 256 * other + 128 * half, 128)],
                    g_down.at[pl.ds(512 * half + 128 * me, 128)],
                )
            )
        return pairs

    return pieces


def back_rows(grad_in, hidden, inv_rms):
    mean = jnp.mean(grad_in * hidden, axis=1, keepdims=True)
    return inv_rms * grad_in - hidden * (inv_rms * inv_rms * inv_rms * mean)


def slot_columns(grads, slot, low_half):
    picks = []
    for row in SLOTS:
        if slot in row:
            m = row.index(slot)
            picks.append(grads[:, 64 * m : 64 * m + 64])
        else:
            picks.append(jnp.zeros((grads.shape[0], 64), jnp.float32))
    return jnp.where(low_half, picks[0], picks[1])


FFN_CHUNKS = ((2048, 1024), (0, 2048))
GRAD_CHUNKS = ((0, 2048), (2048, 1024))
ATTENTION_CHUNKS = ((0, 1024), (1024, 256))


def wide(ref, first, rows):
    return jnp.concatenate([ref[first, rows, :], ref[first + 1, rows, :]], axis=1)


def store_wide(ref, first, rows, value):
    ref[first, rows, :] = value[:, :128]
    ref[first + 1, rows, :] = value[:, 128:]


def two(ref, t, cols=slice(None)):
    value = ref[pl.ds(2 * t, 2), :, cols]
    return value.reshape(256, value.shape[2])


def layer_kernel(*refs):
    (tok, cot, tab, idr, packed, w_out, w_gate, w_up, w_down, gain_one, gain_two, bias), refs = (
        refs[:12],
        refs[12:],
    )
    (output, input_grad, g_gate, g_up, g_down, g_qkv, g_out, small_out), refs = refs[:8], refs[8:]
    (
        tok_all, cot_all, tab_all, idr_all, tok_own, attn_all, wh_ref, wm_ref, q_ref, k_ref, v_ref,
        o_ref, lse_ref, rows_ref, part, mid_ref, a2_all, turned, ffn_all, ffn_g, hidden_s, dgate_s,
        dup_s, e2_ref, dq_acc, dk_acc, dv_acc, out_own, in_own, dbias, small,
        r_gate, r_up, r_down, r_qkv, r_out,
    ), refs = refs[:36], refs[36:]
    home_in, refs = refs[:2], refs[2:]
    home_out, refs = refs[:2], refs[2:]
    gather_in, refs = refs[:6], refs[6:]
    gather_a2, refs = refs[:6], refs[6:]
    gather_ez, refs = refs[:6], refs[6:]
    buffers, refs = refs[:2], refs[2:]
    out_buffers, refs = refs[:2], refs[2:]
    sum_sems, refs = [refs[4 * n : 4 * n + 4] for n in range(4)], refs[16:]
    spread_a, spread_f, back_a, back_f = [refs[3 * n : 3 * n + 3] for n in range(4)]
    refs = refs[12:]
    chain_a, chain_f, refs = refs[:5], refs[5:10], refs[10:]
    fold_f, fold_a, refs = refs[:6], refs[6:12], refs[12:]
    small_scratch, out_sem = refs[:-1], refs[-1]

    i, j = place()
    z, y = j // 2, lax.rem(j, 2)
    mine_first = 2 * (1 - lax.rem(i, 2))
    low_half = i < 2

    def turn(u):
        return lax.rem(mine_first + u, 4)

    ez_all, dqkv_ref, do_ref, out_part = dgate_s, dup_s, hidden_s, turned
    home = Home((tok, tab, idr, cot), (tok_all, tab_all, idr_all, cot_all), home_in, False)
    group = GroupGather((tok_all, tab_all, idr_all, cot_all), gather_in)
    spread = Exchange(attention_pieces(packed, w_out, attn_all), spread_a)
    spread_ffn = Exchange(ffn_pieces(w_gate, w_up, w_down, ffn_all), spread_f)
    attn_w = SeqGather(attn_all, ((0, 1280),), chain_a)
    ffn_w = SeqGather(ffn_all, FFN_CHUNKS, chain_f)
    branch = GroupSum(part, buffers, sum_sems[0])
    second = GroupGather((a2_all,), gather_a2)
    da_sum = GroupSum(part, buffers, sum_sems[1])
    out_sum = GroupSum(out_part, out_buffers, sum_sems[2])
    da1_sum = GroupSum(part, buffers, sum_sems[3])
    third = GroupGather((ez_all,), gather_ez)
    leave = Home((out_own, in_own), (output, input_grad), home_out, True)
    ffn_fold = SeqSum(ffn_g, GRAD_CHUNKS, fold_f)
    attn_fold = SeqSum(attn_all, ATTENTION_CHUNKS, fold_a)
    ffn_back = Exchange(return_ffn(fold_f[0].at[z], r_gate, r_up, r_down), back_f)
    attn_back = Exchange(return_attention(fold_a[0].at[z], r_qkv, r_out), back_a)

    meet(dp_peers() + seq_peers(), home=True)
    spread.start()
    for a in (0, 1, 2):
        for s in (0, 1):
            home.start(a, s)
    spread_ffn.start()
    spread.wait()
    attn_w.start(0)
    for a in (0, 1, 2):
        for s in (0, 1):
            home.wait(a, s)
            group.push(a, s)
    for s in (0, 1):
        tok_own[s] = tok_all[owned(i, s)]
    for n in (0, 1, 2):
        attn_w.forward(0, n)
    for s in (0, 1):
        home.start(3, s)
    spread_ffn.wait()
    ffn_w.start(0)
    ffn_w.start(1)
    for a in (0, 1, 2):
        for s in (0, 1):
            group.relay(a, s)
    for a in (0, 1, 2):
        group.finish(a)
        home.finish(a)
    for b in range(8):
        rows_ref[:, 128 * b : 128 * b + 128] = idr_all[b]

    @pl.loop(0, 8)
    def _(b):
        hidden = tok_all[b].astype(jnp.float32)
        tok_all[b] = (hidden * norm_rows(hidden) * gain_one[...]).astype(jnp.bfloat16)

    a1_all = tok_all
    attn_w.finish(0)
    head_weights(attn_all, wh_ref, wm_ref, low_half)

    @pl.loop(0, 4)
    def _(t):
        rows = pl.ds(pl.multiple_of(t * 256, 256), 256)
        proj = dot(two(a1_all, t), wh_ref[...])
        cos_t, sin_t = angle_tables(two(tab_all, t))
        for pair in (0, 1):
            cols = slice(128 * pair, 128 * pair + 128)
            for base, out in ((0, q_ref), (256, k_ref)):
                x = proj[:, base + 128 * pair : base + 128 * pair + 128]
                out[rows, cols] = (x * cos_t + swap_halves(x) * sin_t).astype(jnp.bfloat16)
        v_ref[rows, :] = proj[:, 512:768].astype(jnp.bfloat16)

    @pl.loop(0, 4)
    def _(u):
        t = turn(u)
        start = pl.multiple_of(t * 256, 256)
        rows = pl.ds(start, 256)
        columns = two(tab_all, t)
        seg_q, var_q = columns[:, 64:65], columns[:, 65:66]
        code_k, var_k = rows_ref[0:1, :], rows_ref[1:2, :]
        row = start + lax.broadcasted_iota(jnp.int32, (256, 1024), 0)
        col = lax.broadcasted_iota(jnp.int32, (256, 1024), 1)
        allowed = ((seg_q == code_k) & (jnp.abs(row - col) <= WINDOW)) | (row == col)
        masked = jnp.where(allowed, 0.0, NEGATIVE)
        same = jnp.where(var_q == var_k, 1.0, 0.0)
        stats = jnp.zeros((256, 128), jnp.float32)
        lane = lax.broadcasted_iota(jnp.int32, (256, 128), 1)
        for h in range(4):
            cols = slice(64 * h, 64 * h + 64)
            scores = dot(q_ref[rows, cols] * 0.125, k_ref[:, cols], NT)
            scores = scores + bias[h] * same + masked
            top = jnp.max(scores, axis=1, keepdims=True)
            weight = jnp.exp(scores - top)
            total = jnp.sum(weight, axis=1, keepdims=True)
            mixed = dot(weight.astype(jnp.bfloat16), v_ref[:, cols])
            o_ref[rows, cols] = (mixed / total).astype(jnp.bfloat16)
            stats = jnp.where(lane == h, top + jnp.log(total), stats)
        lse_ref[:, rows] = stats.T[:8]
        part[pl.ds(2 * t, 2)] = dot(o_ref[rows, :], wm_ref[...], out=jnp.bfloat16).reshape(2, 128, 1024)
        for s in (0, 1):

            @pl.when(u == s)
            def _():
                branch.start(s)

            @pl.when(u == s + 2)
            def _():
                branch.cross(s)

        @pl.when(u == 0)
        def _():
            for s in (0, 1):
                home.wait(3, s)
                group.push(3, s)

        @pl.when(u == 3)
        def _():
            for s in (0, 1):
                group.relay(3, s)

        for n in (0, 1, 2):

            @pl.when(u == n + 1)
            def _():
                ffn_w.forward(0, n)

    for s in (0, 1):
        block = owned(i, s)
        mid = tok_own[s].astype(jnp.float32) + branch.total(s)
        mid_ref[s] = mid
        a2_all[block] = (mid * norm_rows(mid) * gain_two[...]).astype(jnp.bfloat16)
        second.push(0, s)
    branch.finish()
    ffn_w.forward(1, 0)
    for s in (0, 1):
        second.relay(0, s)
    group.finish(3)
    home.finish(3)
    second.finish(0)
    ffn_w.finish(0)

    @pl.loop(0, 4)
    def _(t):
        for d in range(4):
            turned[2 * d : 2 * d + 2, :, pl.ds(pl.multiple_of(256 * t, 256), 256)] = (
                two(a2_all, t, slice(256 * d, 256 * d + 256)).T.reshape(2, 128, 256)
            )

    def unit(f):
        cols = pl.ds(pl.multiple_of(256 * f, 256), 256)
        wg, wu = wide(ffn_all, 2 * f, slice(0, 1024)), wide(ffn_all, 2 * f, slice(1024, 2048))
        down = pl.ds(pl.multiple_of(2048 + 256 * f, 256), 256)
        wd = jnp.concatenate([ffn_all[b, down, :] for b in range(8)], axis=1)

        @pl.loop(0, 4)
        def _(t):
            a, g = two(a2_all, t), two(cot_all, t)
            gate, up, dh = dot(a, wg), dot(a, wu), dot(g, wd, NT)
            sig = 1.0 / (1.0 + jnp.exp(-gate))
            gate_sig = gate * sig
            into = (pl.ds(2 * t, 2), slice(None), cols)
            hidden_s[into] = (gate_sig * up).astype(jnp.bfloat16).reshape(2, 128, 256)
            dgate = dh * up * (sig + gate_sig * (1.0 - sig))
            dgate_s[into] = dgate.astype(jnp.bfloat16).reshape(2, 128, 256)
            dup_s[into] = (dh * gate_sig).astype(jnp.bfloat16).reshape(2, 128, 256)

        @pl.loop(0, 4)
        def _(d):
            rows = pl.ds(pl.multiple_of(d * 256, 256), 256)
            rows_up = pl.ds(pl.multiple_of(1024 + d * 256, 256), 256)
            a_t = two(turned, d)
            dgate, dup = dgate_s[:, :, cols].reshape(1024, 256), dup_s[:, :, cols].reshape(1024, 256)
            store_wide(ffn_g, 2 * f, rows, dot(a_t, dgate, out=jnp.bfloat16))
            store_wide(ffn_g, 2 * f, rows_up, dot(a_t, dup, out=jnp.bfloat16))

        h_t = hidden_s[:, :, cols].reshape(1024, 256).T
        for d in range(4):
            g = cot_all[:, :, 256 * d : 256 * d + 256].reshape(1024, 256)
            store_wide(ffn_g, 2 * d, down, dot(h_t, g, out=jnp.bfloat16))

    @pl.loop(0, 4)
    def _(step):
        f = z
        for n in (0, 1, 2):
            f = jnp.where(step == n + 1, pick(ARRIVAL, z, n), f)
        ffn_w.arrived(1, f)
        for n in (1, 2):

            @pl.when(step == n - 1)
            def _():
                ffn_w.forward(1, n)

        unit(f)

        @pl.when(step > 0)
        def _():
            ffn_fold.start(0, f)

    ffn_fold.start_rest(1)
    ffn_fold.start(0, z)
    ffn_fold.start(1, z)
    ffn_w.drain(1)

    def product(left, t, first_row):
        total = None
        for p in range(4):
            piece = dot(
                two(left, t, slice(256 * p, 256 * p + 256)),
                wide(ffn_all, 2 * p, slice(first_row, first_row + 1024)),
                NT,
            )
            total = piece if total is None else total + piece
        return total

    @pl.loop(0, 4)
    def _(u):
        t = turn(u)
        value = product(dgate_s, t, 0) + product(dup_s, t, 1024)
        part[pl.ds(2 * t, 2)] = value.astype(jnp.bfloat16).reshape(2, 128, 1024)
        for s in (0, 1):

            @pl.when(u == s)
            def _():
                da_sum.start(s)

            @pl.when(u == s + 2)
            def _():
                da_sum.cross(s)

    @pl.loop(0, 4)
    def _(u):
        t = turn(u)
        hidden = two(hidden_s, t)
        for d in range(4):
            w = wide(ffn_all, 2 * d, slice(2048, 3072))
            out_part[pl.ds(2 * t, 2), :, 256 * d : 256 * d + 256] = dot(
                hidden, w, out=jnp.bfloat16
            ).reshape(2, 128, 256)
        for s in (0, 1):

            @pl.when(u == s)
            def _():
                out_sum.start(s)

    gain_rows = jnp.zeros((1, 1024), jnp.float32)
    for s in (0, 1):
        mid = mid_ref[s]
        inv = norm_rows(mid)
        da2 = da_sum.total(s)
        gain_rows = gain_rows + jnp.sum(da2 * (mid * inv), axis=0, keepdims=True)
        e2 = cot_all[owned(i, s)].astype(jnp.float32) + back_rows(da2 * gain_two[...], mid, inv)
        e2_ref[s] = e2
        ez_all[owned(i, s)] = e2.astype(jnp.bfloat16)
        third.push(0, s)
    for b in range(8):
        small[8 + b : 9 + b, :] = gain_rows[:, 128 * b : 128 * b + 128]
    da_sum.finish()
    ffn_fold.cross(0, 0)
    for s in (0, 1):
        out_sum.cross(s)
    for s in (0, 1):
        third.relay(0, s)
    third.finish(0)
    ffn_fold.cross(0, 1)

    @pl.loop(0, 4)
    def _(t):
        do_ref[pl.ds(2 * t, 2), :, 0:256] = dot(two(ez_all, t), wm_ref[...], NT, jnp.bfloat16).reshape(
            2, 128, 256
        )

    for d in range(4):
        ez = ez_all[:, :, 256 * d : 256 * d + 256].reshape(1024, 256)
        store_wide(attn_all, 2 * d, slice(1024, 1280), dot(o_ref[...], ez, TN, jnp.bfloat16))
    attn_fold.start_rest(1)
    attn_fold.start(1, z)
    for s in (0, 1):
        out_own[s] = (mid_ref[s] + out_sum.total(s)).astype(jnp.bfloat16)
        leave.start(0, s)

    def unturn(acc, base, t, rows):
        cos_t, sin_t = angle_tables(two(tab_all, t))
        for pair in (0, 1):
            g = acc[rows, 128 * pair : 128 * pair + 128]
            dqkv_ref[pl.ds(2 * t, 2), :, base + 128 * pair : base + 128 * pair + 128] = (
                (g * cos_t - swap_halves(g) * sin_t).astype(jnp.bfloat16).reshape(2, 128, 128)
            )

    dk_acc[...] = jnp.zeros_like(dk_acc)
    dv_acc[...] = jnp.zeros_like(dv_acc)
    dbias[...] = jnp.zeros_like(dbias)

    @pl.loop(0, 4)
    def _(t):
        start = pl.multiple_of(t * 256, 256)
        rows = pl.ds(start, 256)
        columns = tab_all[...].reshape(1024, 128)
        var_k, code_k = columns[:, 65:66], columns[:, 66:67]
        pair = idr_all[pl.ds(2 * t, 2)]
        label = jnp.concatenate([pair[0], pair[1]], axis=1)
        seg_q, var_q = label[2:3, :], label[1:2, :]
        row = lax.broadcasted_iota(jnp.int32, (1024, 256), 0)
        col = start + lax.broadcasted_iota(jnp.int32, (1024, 256), 1)
        allowed = ((seg_q == code_k) & (jnp.abs(row - col) <= WINDOW)) | (row == col)
        masked = jnp.where(allowed, 0.0, NEGATIVE)
        same = jnp.where(var_q == var_k, 1.0, 0.0)
        for h in range(4):
            cols = slice(64 * h, 64 * h + 64)
            q_h, k_h, v_h = q_ref[rows, cols] * 0.125, k_ref[:, cols], v_ref[:, cols]
            do_h = two(do_ref, t, cols)
            scores = dot(k_h, q_h, NT) + bias[h] * same + masked
            prob = jnp.exp(scores - lse_ref[h : h + 1, rows])
            dv_acc[:, cols] += dot(prob.astype(jnp.bfloat16), do_h)
            dprob = dot(v_h, do_h, NT)
            mean = jnp.sum(prob * dprob, axis=0, keepdims=True)
            dscore = (prob * (dprob - mean)).astype(jnp.bfloat16)
            dbias[h : h + 1, :] += jnp.sum(dscore.astype(jnp.float32) * same, axis=0, keepdims=True)
            dk_acc[:, cols] += dot(dscore, q_h)
            dq_acc[:, cols] = dot(dscore, k_h, TN) * 0.125

        unturn(dq_acc, 0, t, slice(None))

        @pl.when(t == 0)
        def _():
            ffn_fold.cross(1, 0)

        @pl.when(t == 1)
        def _():
            ffn_fold.cross(0, 2)

        @pl.when(t == 2)
        def _():
            ffn_fold.cross(1, 1)

        @pl.when(t == 3)
        def _():
            attn_fold.cross(1, 0)

    @pl.loop(0, 4)
    def _(t):
        rows = pl.ds(pl.multiple_of(t * 256, 256), 256)
        unturn(dk_acc, 256, t, rows)
        dqkv_ref[pl.ds(2 * t, 2), :, 512:768] = (
            dv_acc[rows, :].astype(jnp.bfloat16).reshape(2, 128, 256)
        )

    for d in range(4):
        block = slice(256 * d, 256 * d + 256)
        grads = dot(
            a1_all[:, :, block].reshape(1024, 256), dqkv_ref[:, :, 0:768].reshape(1024, 768), TN
        )
        for b in range(8):
            attn_all[b, block, :] = jnp.concatenate(
                [slot_columns(grads, 2 * b + e, low_half) for e in (0, 1)], axis=1
            ).astype(jnp.bfloat16)
    attn_fold.start_rest(0)
    attn_fold.start(0, z)

    @pl.loop(0, 4)
    def _(u):
        t = turn(u)
        part[pl.ds(2 * t, 2)] = dot(
            two(dqkv_ref, t, slice(0, 768)), wh_ref[...], NT, jnp.bfloat16
        ).reshape(2, 128, 1024)
        for s in (0, 1):

            @pl.when(u == s)
            def _():
                da1_sum.start(s)

            @pl.when(u == s + 2)
            def _():
                da1_sum.cross(s)

    ffn_fold.cross(1, 2)
    attn_fold.cross(1, 1)
    attn_fold.cross(0, 0)
    attn_fold.cross(1, 2)
    for chunk in (0, 1):
        ffn_fold.finish(chunk)
    ffn_back.start()
    gain_rows = jnp.zeros((1, 1024), jnp.float32)
    for s in (0, 1):
        hidden = tok_own[s].astype(jnp.float32)
        inv = norm_rows(hidden)
        da1 = da1_sum.total(s)
        gain_rows = gain_rows + jnp.sum(da1 * (hidden * inv), axis=0, keepdims=True)
        grad = e2_ref[s] + back_rows(da1 * gain_one[...], hidden, inv)
        in_own[s] = grad.astype(jnp.bfloat16)
    for b in range(8):
        small[b : b + 1, :] = gain_rows[:, 128 * b : 128 * b + 128]
    lane = lax.broadcasted_iota(jnp.int32, (8, 128), 1)
    line = lax.broadcasted_iota(jnp.int32, (8, 128), 0)
    bias_row = jnp.zeros((8, 128), jnp.float32)
    for h in range(4):
        value = jnp.sum(dbias[h : h + 1, :], axis=1, keepdims=True)
        bias_row = jnp.where((line == 0) & (lane == 4 * h + i), value, bias_row)
    small[16:24, :] = bias_row
    small_sum = SmallSum(small, small_scratch)
    small_sum.start(0)
    attn_fold.cross(0, 1)
    attn_fold.cross(0, 2)
    small_sum.start(1)
    for s in (0, 1):
        leave.start(1, s)
    for chunk in (1, 0):
        attn_fold.finish(chunk)
    attn_back.start()
    small_sum.start(2)
    ffn_back.wait()
    copies = []
    for start, source, target in ((0, r_gate, g_gate), (512, r_up, g_up)):
        for half in (0, 1):
            cols = slice(256 * half, 256 * half + 256)
            rows = slice(start + 256 * half, start + 256 * half + 256)
            dv_acc[rows, :] = source[:, cols].astype(jnp.float32)
            copies.append((dv_acc.at[rows], target.at[:, cols]))
    dk_acc[:, 0:128] = r_down[...].astype(jnp.float32)
    copies.append((dk_acc.at[:, 0:128], g_down))
    copies = [
        pltpu.make_async_copy(src, dst, out_sem.at[index]) for index, (src, dst) in enumerate(copies)
    ]
    for copy in copies:
        copy.start()
    small_out[...] = small_sum.total(2)
    out_sum.finish()
    da1_sum.finish()
    for a in (0, 1):
        for s in (0, 1):
            leave.wait(a, s)
        leave.finish(a)
    for chunk in (0, 1):
        ffn_fold.drain(chunk)
        attn_fold.drain(chunk)
    attn_back.wait()
    g_qkv[...] = r_qkv[...].astype(jnp.float32)
    g_out[...] = r_out[...].astype(jnp.float32)
    for copy in copies:
        copy.wait()


def layer(arrays):
    def vmem(dtype, *shape):
        return pltpu.VMEM(shape, dtype)

    low, full = jnp.bfloat16, jnp.float32
    blocks = vmem(low, 8, 128, 1024)
    own = vmem(low, 2, 128, 1024)
    heads = vmem(low, 1024, 256)
    grads = vmem(full, 1024, 256)
    return pl.pallas_call(
        layer_kernel,
        out_shape=[
            bf16(2, 128, 1024),
            bf16(2, 128, 1024),
            f32(256, 512),
            f32(256, 512),
            f32(1024, 128),
            f32(4, 256, 128),
            f32(256, 128),
            f32(24, 128),
        ],
        in_specs=[HB, HB, VM, VM, VM, VM, HB, HB, HB, VM, VM, SM],
        out_specs=[HB] * 5 + [VM] * 3,
        scratch_shapes=[
            blocks,
            blocks,
            vmem(full, 8, 128, 128),
            vmem(full, 8, 8, 128),
            own,
            vmem(low, 8, 1280, 128),
            vmem(low, 1024, 768),
            vmem(low, 256, 1024),
            heads,
            heads,
            heads,
            heads,
            vmem(full, 8, 1024),
            vmem(full, 8, 1024),
            blocks,
            vmem(full, 2, 128, 1024),
            blocks,
            blocks,
            vmem(low, 8, 3072, 128),
            vmem(low, 8, 3072, 128),
            blocks,
            blocks,
            blocks,
            vmem(full, 2, 128, 1024),
            vmem(full, 256, 256),
            grads,
            grads,
            own,
            own,
            vmem(full, 8, 256),
            vmem(full, 24, 128),
            vmem(low, 256, 512),
            vmem(low, 256, 512),
            vmem(low, 1024, 128),
            vmem(low, 4, 256, 128),
            vmem(low, 256, 128),
        ]
        + Home.sems(4)
        + Home.sems(2)
        + GroupGather.sems(4)
        + GroupGather.sems(1)
        + GroupGather.sems(1)
        + GroupSum.buffers()
        + GroupSum.buffers()
        + GroupSum.sems() * 4
        + Exchange.sems(2)
        + Exchange.sems(4)
        + Exchange.sems(2)
        + Exchange.sems(4)
        + SeqGather.sems(1)
        + SeqGather.sems(2)
        + SeqSum.scratch(3072, 2)
        + SeqSum.scratch(1280, 2)
        + SmallSum.scratch((24, 128))
        + [DMA((5,))],
        compiler_params=pltpu.CompilerParams(
            collective_id=1, has_side_effects=True, vmem_limit_bytes=67_043_328
        ),
        name="layer",
    )(*arrays)


def on_group(
    tokens, segment_ids, variate_ids, time_ids, pad_mask, cotangent,
    w_qkv, w_out, w_gate, w_up, w_down, gain_attn, gain_ffn, variate_bias,
):
    i = lax.axis_index("dp")
    gain_one = gain_attn.astype(jnp.float32)[None]
    gain_two = gain_ffn.astype(jnp.float32)[None]
    packed = jnp.pad(w_qkv, ((0, 0), (0, 128))).reshape(256, 2, 4, 64)
    packed = packed.transpose(2, 0, 1, 3).reshape(4, 256, 128)
    frequency = jnp.exp(-jnp.log(10000.0) * jnp.arange(32, dtype=jnp.float32) / 32)
    angles = time_ids.astype(jnp.float32)[..., None] * frequency
    code_ids = jnp.where(pad_mask == 1, segment_ids, -1)
    labels = jnp.stack([segment_ids, variate_ids, code_ids], axis=-1).astype(jnp.float32)
    tables = jnp.concatenate(
        [jnp.cos(angles), jnp.sin(angles), labels, jnp.zeros((2, 128, 61), jnp.float32)], axis=-1
    )
    label_rows = jnp.stack([code_ids, variate_ids, segment_ids] + [segment_ids] * 5, axis=1)
    bias = jnp.where(
        jnp.arange(4)[None, :] == i, variate_bias.astype(jnp.float32).reshape(4, 4), 0.0
    ).sum(axis=1)
    output, input_grad, g_gate, g_up, g_down, g_qkv, g_out, small = layer(
        [
            tokens, cotangent, tables, label_rows.astype(jnp.float32), packed, w_out, w_gate, w_up, w_down,
            gain_one, gain_two, bias,
        ]
    )
    g_qkv = g_qkv.reshape(4, 256, 2, 64).transpose(1, 2, 0, 3).reshape(256, 512)[:, :384]
    small = small.reshape(3, 1024)
    return (
        output, input_grad, g_qkv, g_out, g_gate, g_up, g_down, small[0], small[1], small[2, :16],
    )


def solution(mesh):
    in_specs = (
        P("dp", "seq", None),
        P("dp", "seq"),
        P("dp", "seq"),
        P("dp", "seq"),
        P("dp", "seq"),
        P("dp", "seq", None),
        P("dp", "seq"),
        P("dp", "seq"),
        P("dp", "seq"),
        P("dp", "seq"),
        P("dp", "seq"),
        P(),
        P(),
        P(),
    )
    out_specs = (
        P("dp", "seq", None),
        P("dp", "seq", None),
        P("dp", "seq"),
        P("dp", "seq"),
        P("dp", "seq"),
        P("dp", "seq"),
        P("dp", "seq"),
        P(),
        P(),
        P(),
    )
    grouped = mesh.shape["dp"] == 4 and mesh.shape["seq"] == 8
    return jax.shard_map(
        on_group if grouped else on_device, mesh=mesh, in_specs=in_specs, out_specs=out_specs, check_vma=False
    )
```

```python
import functools

import jax
import jax.numpy as jnp
from jax import lax
from jax.experimental import pallas as pl
from jax.experimental.pallas import tpu as pltpu
from jax.sharding import PartitionSpec as P

HEADS = 16
HEAD_DIM = 64
WINDOW = 512


EPSILON = 1e-06
NEGATIVE = -1e30


def passed_along(block, axis, distance):
    devices = range(lax.axis_size(axis))
    route = [(i - distance, i) for i in devices if i - distance in devices]
    return lax.ppermute(block, axis, route)


def norm_scale(hidden):
    return lax.rsqrt(jnp.mean(hidden * hidden, axis=-1, keepdims=True) + EPSILON)


def norm_back(grad_in, hidden, inv_rms):
    return inv_rms * grad_in - hidden * inv_rms * inv_rms * inv_rms * jnp.mean(
        grad_in * hidden, axis=-1, keepdims=True
    )


def rope_tables(time_row, half_dim):
    frequency = jnp.exp(-jnp.log(10000.0) * jnp.arange(half_dim, dtype=jnp.float32) / half_dim)
    angles = time_row.astype(jnp.float32)[:, None] * frequency[None, :]
    return (jnp.cos(angles)[:, None, :], jnp.sin(angles)[:, None, :])


def rotate(values_in, cos_table, sine_table):
    half_dim = cos_table.shape[-1]
    first_half = values_in[..., :half_dim]
    second_half = values_in[..., half_dim:]
    return jnp.concatenate(
        [
            first_half * cos_table - second_half * sine_table,
            second_half * cos_table + first_half * sine_table,
        ],
        axis=-1,
    )


def rotate_back(grad_in, cos_table, sine_table):
    half_dim = cos_table.shape[-1]
    first_half = grad_in[..., :half_dim]
    second_half = grad_in[..., half_dim:]
    return jnp.concatenate(
        [
            first_half * cos_table + second_half * sine_table,
            second_half * cos_table - first_half * sine_table,
        ],
        axis=-1,
    )


def masked_scores(query_rot, keys_all, labels_own, labels_keys, var_bias, hop_count):
    row_count = query_rot.shape[0]
    key_count = keys_all.shape[0]
    offsets = (
        jnp.arange(key_count)[None, :] - hop_count * row_count - jnp.arange(row_count)[:, None]
    )
    allowed = (
        (jnp.abs(offsets) <= WINDOW)
        & (labels_own[0][:, None] == labels_keys[0][None, :])
        & ((labels_keys[2][None, :] == 1) | (offsets == 0))
    )
    same_var = (labels_own[1][:, None] == labels_keys[1][None, :]).astype(jnp.float32)
    scores = jnp.einsum(
        "qhd,khd->hqk", query_rot, keys_all, preferred_element_type=jnp.float32
    ) * HEAD_DIM ** (-0.5)
    scores = scores + var_bias[:, None, None] * same_var[None]
    return (jnp.where(allowed[None], scores, NEGATIVE), same_var)


def fetch_weights(shards):
    row_blocks = (
        lax.all_gather(shards[0], "dp", axis=0, tiled=True),
        lax.all_gather(shards[1], "dp", axis=0, tiled=True),
        lax.all_gather(shards[2], "dp", axis=0, tiled=True),
        lax.all_gather(shards[3], "dp", axis=0, tiled=True),
        lax.all_gather(shards[4], "dp", axis=0, tiled=True),
    )
    return (
        lax.all_gather(row_blocks[0], "seq", axis=1, tiled=True),
        lax.all_gather(row_blocks[1], "seq", axis=1, tiled=True),
        lax.all_gather(row_blocks[2], "seq", axis=1, tiled=True),
        lax.all_gather(row_blocks[3], "seq", axis=1, tiled=True),
        lax.all_gather(row_blocks[4], "seq", axis=1, tiled=True),
    )


def fetch_keep(shards):
    row_blocks = (
        lax.all_gather(shards[0], "dp", axis=0, tiled=True),
        lax.all_gather(shards[1], "dp", axis=0, tiled=True),
        lax.all_gather(shards[2], "dp", axis=0, tiled=True),
        lax.all_gather(shards[3], "dp", axis=0, tiled=True),
        lax.all_gather(shards[4], "dp", axis=0, tiled=True),
    )
    return (
        lax.all_gather(row_blocks[0], "seq", axis=1, tiled=True),
        lax.all_gather(row_blocks[1], "seq", axis=1, tiled=True),
        lax.all_gather(row_blocks[2], "seq", axis=1, tiled=True),
        lax.all_gather(row_blocks[3], "seq", axis=1, tiled=True),
        lax.all_gather(row_blocks[4], "seq", axis=1, tiled=True),
    )


def reduce_last(grads_full):
    col_sums = (
        lax.psum_scatter(grads_full[0], "seq", scatter_dimension=1, tiled=True),
        lax.psum_scatter(grads_full[1], "seq", scatter_dimension=1, tiled=True),
        lax.psum_scatter(grads_full[2], "seq", scatter_dimension=1, tiled=True),
        lax.psum_scatter(grads_full[3], "seq", scatter_dimension=1, tiled=True),
        lax.psum_scatter(grads_full[4], "seq", scatter_dimension=1, tiled=True),
    )
    return (
        lax.psum_scatter(
            col_sums[0].astype(jnp.bfloat16), "dp", scatter_dimension=0, tiled=True
        ).astype(jnp.float32),
        lax.psum_scatter(
            col_sums[1].astype(jnp.bfloat16), "dp", scatter_dimension=0, tiled=True
        ).astype(jnp.float32),
        lax.psum_scatter(
            col_sums[2].astype(jnp.bfloat16), "dp", scatter_dimension=0, tiled=True
        ).astype(jnp.float32),
        lax.psum_scatter(
            col_sums[3].astype(jnp.bfloat16), "dp", scatter_dimension=0, tiled=True
        ).astype(jnp.float32),
        lax.psum_scatter(
            col_sums[4].astype(jnp.bfloat16), "dp", scatter_dimension=0, tiled=True
        ).astype(jnp.float32),
    )


def weight_grads(pieces):
    (
        normed_one,
        grad_qkv,
        attended,
        grad_branch,
        normed_two,
        grad_gate,
        grad_up,
        hidden,
        grad_ffn,
    ) = pieces
    grad_w_qkv = jnp.einsum("td,tf->df", normed_one, grad_qkv, preferred_element_type=jnp.float32)
    grad_w_out = jnp.einsum("ti,to->io", attended, grad_branch, preferred_element_type=jnp.float32)
    grad_w_gate = jnp.einsum("td,tf->df", normed_two, grad_gate, preferred_element_type=jnp.float32)
    grad_w_up = jnp.einsum("td,tf->df", normed_two, grad_up, preferred_element_type=jnp.float32)
    grad_w_down = jnp.einsum("tf,td->fd", hidden, grad_ffn, preferred_element_type=jnp.float32)
    return (grad_w_qkv, grad_w_out, grad_w_gate, grad_w_up, grad_w_down)


def on_device(
    tokens,
    segment_ids,
    variate_ids,
    time_ids,
    pad_mask,
    cotangent,
    w_qkv,
    w_out,
    w_gate,
    w_up,
    w_down,
    gain_attn,
    gain_ffn,
    variate_bias,
):
    micro_count, row_count, model_width = tokens.shape
    hop_count = -(-WINDOW // row_count)
    key_count = (2 * hop_count + 1) * row_count
    shards = (w_qkv, w_out, w_gate, w_up, w_down)
    var_bias = variate_bias.astype(jnp.float32)
    gain_one = gain_attn.astype(jnp.float32)
    gain_two = gain_ffn.astype(jnp.float32)
    bias_total = jnp.zeros(var_bias.shape, jnp.float32)
    gain_one_total = jnp.zeros(gain_one.shape, jnp.float32)
    gain_two_total = jnp.zeros(gain_two.shape, jnp.float32)
    grad_totals = None
    saved = []
    outputs = []
    input_grads = []
    held_weights = fetch_weights(shards)
    for micro_step in range(micro_count):
        if micro_step == 0:
            weights = held_weights
        else:
            weights = fetch_keep(shards)
        resid_in = tokens[micro_step].astype(jnp.float32)
        inv_one = norm_scale(resid_in)
        normed_one = (resid_in * inv_one * gain_one).astype(jnp.bfloat16)
        qkv_proj = jnp.dot(normed_one, weights[0], preferred_element_type=jnp.float32)
        cos_table, sine_table = rope_tables(time_ids[micro_step], HEAD_DIM // 2)
        query_rot = rotate(
            qkv_proj[:, :model_width].reshape(row_count, HEADS, HEAD_DIM), cos_table, sine_table
        ).astype(jnp.bfloat16)
        key_rot = rotate(
            qkv_proj[:, model_width : 2 * model_width].reshape(row_count, HEADS, HEAD_DIM),
            cos_table,
            sine_table,
        ).astype(jnp.bfloat16)
        value_own = qkv_proj[:, 2 * model_width :].astype(jnp.bfloat16)
        kv_own = jnp.stack([key_rot.reshape(row_count, model_width), value_own])
        labels_own = jnp.stack(
            [segment_ids[micro_step], variate_ids[micro_step], pad_mask[micro_step]]
        )
        kv_slots = []
        label_slots = []
        for slot_index in range(2 * hop_count + 1):
            offset = slot_index - hop_count
            if offset == 0:
                kv_slots.append(kv_own)
                label_slots.append(labels_own)
            else:
                kv_slots.append(passed_along(kv_own, "seq", -offset))
                label_slots.append(passed_along(labels_own, "seq", -offset))
        kv_all = jnp.concatenate(kv_slots, axis=1)
        labels_keys = jnp.concatenate(label_slots, axis=1)
        keys_all = kv_all[0].reshape(key_count, HEADS, HEAD_DIM)
        values_all = kv_all[1].reshape(key_count, HEADS, HEAD_DIM)
        scores, same_var = masked_scores(
            query_rot, keys_all, labels_own, labels_keys, var_bias, hop_count
        )
        maxima = jnp.max(scores, axis=-1, keepdims=True)
        exp_shift = jnp.exp(scores - maxima)
        denom_sum = jnp.sum(exp_shift, axis=-1, keepdims=True)
        log_norm = maxima + jnp.log(denom_sum)
        prob_low = (exp_shift / denom_sum).astype(jnp.bfloat16)
        attended = jnp.einsum(
            "hqk,khd->qhd", prob_low, values_all, preferred_element_type=jnp.float32
        )
        attended = attended.reshape(row_count, model_width).astype(jnp.bfloat16)
        resid_mid = resid_in + jnp.dot(attended, weights[1], preferred_element_type=jnp.float32)
        inv_two = norm_scale(resid_mid)
        normed_two = (resid_mid * inv_two * gain_two).astype(jnp.bfloat16)
        gate_proj = jnp.dot(normed_two, weights[2], preferred_element_type=jnp.float32)
        up_proj = jnp.dot(normed_two, weights[3], preferred_element_type=jnp.float32)
        gate_sig = jax.nn.sigmoid(gate_proj)
        hidden = (gate_proj * gate_sig * up_proj).astype(jnp.bfloat16)
        ffn_out = jnp.dot(hidden, weights[4], preferred_element_type=jnp.float32)
        outputs.append((resid_mid + ffn_out).astype(jnp.bfloat16))
        grad_out = cotangent[micro_step].astype(jnp.float32)
        grad_ffn = grad_out.astype(jnp.bfloat16)
        grad_hidden = jnp.einsum(
            "td,fd->tf", grad_ffn, weights[4], preferred_element_type=jnp.float32
        )
        grad_gate = (
            grad_hidden * up_proj * gate_sig * (1.0 + gate_proj * (1.0 - gate_sig))
        ).astype(jnp.bfloat16)
        grad_up = (grad_hidden * gate_proj * gate_sig).astype(jnp.bfloat16)
        grad_normed_two = jnp.einsum(
            "tf,df->td", grad_gate, weights[2], preferred_element_type=jnp.float32
        )
        grad_normed_two = grad_normed_two + jnp.einsum(
            "tf,df->td", grad_up, weights[3], preferred_element_type=jnp.float32
        )
        gain_two_total = gain_two_total + jnp.sum(grad_normed_two * resid_mid * inv_two, axis=0)
        grad_mid = grad_out + norm_back(grad_normed_two * gain_two, resid_mid, inv_two)
        grad_branch = grad_mid.astype(jnp.bfloat16)
        grad_attended = jnp.einsum(
            "to,io->ti", grad_branch, weights[1], preferred_element_type=jnp.float32
        )
        grad_attended = grad_attended.astype(jnp.bfloat16).reshape(row_count, HEADS, HEAD_DIM)
        scores, same_var = masked_scores(
            query_rot, keys_all, labels_own, labels_keys, var_bias, hop_count
        )
        prob_full = jnp.exp(scores - log_norm)
        prob_low = prob_full.astype(jnp.bfloat16)
        grad_values = jnp.einsum(
            "hqk,qhd->khd", prob_low, grad_attended, preferred_element_type=jnp.float32
        )
        grad_prob = jnp.einsum(
            "qhd,khd->hqk", grad_attended, values_all, preferred_element_type=jnp.float32
        )
        grad_scores = prob_full * (
            grad_prob - jnp.sum(prob_full * grad_prob, axis=-1, keepdims=True)
        )
        grad_scores = grad_scores.astype(jnp.bfloat16)
        bias_total = bias_total + jnp.sum(
            grad_scores.astype(jnp.float32) * same_var[None], axis=(1, 2)
        )
        grad_query = jnp.einsum(
            "hqk,khd->qhd", grad_scores, keys_all, preferred_element_type=jnp.float32
        ) * HEAD_DIM ** (-0.5)
        grad_keys = jnp.einsum(
            "hqk,qhd->khd", grad_scores, query_rot, preferred_element_type=jnp.float32
        ) * HEAD_DIM ** (-0.5)
        grad_kv = jnp.stack(
            [grad_keys.reshape(key_count, model_width), grad_values.reshape(key_count, model_width)]
        )
        grad_kv_own = grad_kv[:, hop_count * row_count : (hop_count + 1) * row_count]
        for slot_index in range(2 * hop_count + 1):
            offset = slot_index - hop_count
            if offset != 0:
                slot_grad = grad_kv[:, slot_index * row_count : (slot_index + 1) * row_count]
                grad_kv_own = grad_kv_own + passed_along(
                    slot_grad.astype(jnp.bfloat16), "seq", offset
                ).astype(slot_grad.dtype)
        grad_q_plain = rotate_back(grad_query, cos_table, sine_table).reshape(
            row_count, model_width
        )
        grad_k_plain = rotate_back(
            grad_kv_own[0].reshape(row_count, HEADS, HEAD_DIM), cos_table, sine_table
        ).reshape(row_count, model_width)
        grad_qkv = jnp.concatenate([grad_q_plain, grad_k_plain, grad_kv_own[1]], axis=1).astype(
            jnp.bfloat16
        )
        grad_normed_one = jnp.einsum(
            "tf,df->td", grad_qkv, weights[0], preferred_element_type=jnp.float32
        )
        gain_one_total = gain_one_total + jnp.sum(grad_normed_one * resid_in * inv_one, axis=0)
        grad_input = grad_mid + norm_back(grad_normed_one * gain_one, resid_in, inv_one)
        input_grads.append(grad_input.astype(jnp.bfloat16))
        pieces = (
            normed_one,
            grad_qkv,
            attended,
            grad_branch,
            normed_two,
            grad_gate,
            grad_up,
            hidden,
            grad_ffn,
        )
        saved.append(pieces)
    joined = tuple(
        (
            jnp.concatenate([entry[index] for entry in saved], axis=0)
            for index in range(len(saved[0]))
        )
    )
    grad_totals = reduce_last(weight_grads(joined))
    bias_sum, gain_one_sum, gain_two_sum = lax.psum(
        (bias_total, gain_one_total, gain_two_total), ("dp", "seq")
    )
    return (
        jnp.stack(outputs),
        jnp.stack(input_grads),
        grad_totals[0],
        grad_totals[1],
        grad_totals[2],
        grad_totals[3],
        grad_totals[4],
        gain_one_sum,
        gain_two_sum,
        bias_sum,
    )


MESH = pl.DeviceIdType.MESH
VM = pl.BlockSpec(memory_space=pltpu.VMEM)
HB = pl.BlockSpec(memory_space=pl.ANY)
SM = pl.BlockSpec(memory_space=pltpu.SMEM)
DMA = pltpu.SemaphoreType.DMA
NT = (((1,), (1,)), ((), ()))
TN = (((0,), (0,)), ((), ()))
EVERY = slice(None)


def bf16(*shape):
    return jax.ShapeDtypeStruct(shape, jnp.bfloat16)


def f32(*shape):
    return jax.ShapeDtypeStruct(shape, jnp.float32)


def dot(a, b, dims=None, out=jnp.float32):
    dims = (((1,), (0,)), ((), ())) if dims is None else dims
    return lax.dot_general(a, b, dims, preferred_element_type=jnp.float32).astype(out)


def at(i, j):
    return {"dp": 2 * lax.rem(j, 2) + lax.rem(i, 2), "seq": 2 * (j // 2) + i // 2}


def place():
    dp, seq = lax.axis_index("dp"), lax.axis_index("seq")
    return 2 * lax.rem(seq, 2) + lax.rem(dp, 2), 2 * (seq // 2) + dp // 2


def row_block(i, j):
    return 2 * lax.rem(j, 2) + lax.rem(i, 2)


def column_block(i, j):
    return 2 * (j // 2) + i // 2


def ring(i):
    return i + 1 - 2 * lax.rem(i, 2), lax.rem(i + 2, 4)


def owned(i, s):
    return 4 * lax.rem(i, 2) + 2 * s + i // 2


def keeper(i, j):
    return 2 * (i // 2) + j // 4


def taker(i, j, s):
    return 4 * lax.rem(i, 2) + 2 * s + lax.rem(j, 2)


def send(src, dst, send_sem, recv_sem, peer):
    return pltpu.make_async_remote_copy(
        src_ref=src,
        dst_ref=dst,
        send_sem=send_sem,
        recv_sem=recv_sem,
        device_id=peer,
        device_id_type=MESH,
    )


def landed(ref, sem):
    pltpu.make_async_copy(ref, ref, sem).wait()


def meet(peers, home=False):
    i, j = place()
    barrier = pltpu.get_barrier_semaphore()
    for peer in peers:
        pl.semaphore_signal(barrier, inc=1, device_id=peer, device_id_type=MESH)
    if home:
        target, stays = keeper(i, j), keeper(i, j) == i
        for s in (0, 1):

            @pl.when(jnp.logical_not(stays & (taker(i, j, s) == j)))
            def _():
                pl.semaphore_signal(
                    barrier, inc=1, device_id=at(target, taker(i, j, s)), device_id_type=MESH
                )

        pl.semaphore_wait(barrier, len(peers) + jnp.where(stays, 1, 2))
    else:
        pl.semaphore_wait(barrier, len(peers))


def dp_peers():
    i, j = place()
    return [at(lax.rem(i + step, 4), j) for step in (1, 2, 3)]


def seq_peers():
    i, j = place()
    z, y = j // 2, lax.rem(j, 2)
    return [at(i, 2 * lax.rem(z + step, 4) + y) for step in (1, 2, 3)] + [at(i, 2 * z + 1 - y)]


class Home:
    def __init__(self, ins, outs, sems, slotted):
        self.ins, self.outs, self.slotted = ins, outs, slotted
        self.send_sem, self.recv_sem = sems

    @staticmethod
    def sems(count):
        return [DMA((count, 2)), DMA((count, 2))]

    def target(self, a, s):
        i, _ = place()
        return self.outs[a].at[s if self.slotted else owned(i, s)]

    def start(self, a, s):
        i, j = place()
        slot = lax.rem(j // 2, 2)
        src, dst = self.ins[a].at[s], self.outs[a].at[slot if self.slotted else column_block(i, j)]
        here = (keeper(i, j) == i) & (taker(i, j, s) == j)

        @pl.when(jnp.logical_not(here))
        def _():
            peer = at(keeper(i, j), taker(i, j, s))
            send(src, dst, self.send_sem.at[a, s], self.recv_sem.at[a, slot], peer).start()

        @pl.when(here)
        def _():
            pltpu.make_async_copy(src, dst, self.recv_sem.at[a, slot]).start()

    def wait(self, a, s):
        landed(self.target(a, s), self.recv_sem.at[a, s])

    def finish(self, a):
        i, j = place()
        for s in (0, 1):

            @pl.when(jnp.logical_not((keeper(i, j) == i) & (taker(i, j, s) == j)))
            def _():
                landed(self.ins[a].at[s], self.send_sem.at[a, s])


class GroupGather:
    def __init__(self, outs, sems):
        self.outs = outs
        self.s_core, self.r_core, self.s_x, self.r_x, self.s_on, self.r_on = sems

    @staticmethod
    def sems(count):
        return [DMA((count, 2))] * 6

    def push(self, a, s):
        i, j = place()
        core, across = ring(i)
        block = self.outs[a].at[owned(i, s)]
        send(block, block, self.s_x.at[a, s], self.r_x.at[a, s], at(across, j)).start()
        send(block, block, self.s_core.at[a, s], self.r_core.at[a, s], at(core, j)).start()

    def relay(self, a, s):
        i, j = place()
        core, across = ring(i)
        block = self.outs[a].at[owned(across, s)]
        landed(block, self.r_x.at[a, s])
        send(block, block, self.s_on.at[a, s], self.r_on.at[a, s], at(core, j)).start()

    def near(self, a):
        core, _ = ring(place()[0])
        for s in (0, 1):
            landed(self.outs[a].at[owned(core, s)], self.r_core.at[a, s])

    def beyond(self, a):
        core, _ = ring(place()[0])
        for s in (0, 1):
            landed(self.outs[a].at[owned(lax.rem(core + 2, 4), s)], self.r_on.at[a, s])

    def finish(self, a):
        self.near(a)
        self.beyond(a)
        self.sent(a)

    def sent(self, a):
        for s in (0, 1):
            for sem in (self.s_x, self.s_core, self.s_on):
                landed(self.outs[a].at[s], sem.at[a, s])


class GroupSum:
    def __init__(self, parts, buffers, sems):
        self.parts = parts
        self.near, self.far = buffers
        self.s_core, self.r_core, self.s_x, self.r_x = sems

    @staticmethod
    def buffers():
        block = (128, 1024)
        return [pltpu.VMEM((2, 2) + block, jnp.bfloat16), pltpu.VMEM((2,) + block, jnp.bfloat16)]

    @staticmethod
    def sems():
        return [DMA((2, 2)), DMA((2, 2)), DMA((2,)), DMA((2,))]

    def start(self, s):
        i, j = place()
        core, _ = ring(i)
        for side, owner in ((0, lax.rem(core + 2, 4)), (1, core)):
            send(
                self.parts.at[owned(owner, s)],
                self.near.at[side, s],
                self.s_core.at[side, s],
                self.r_core.at[side, s],
                at(core, j),
            ).start()

    def cross(self, s):
        i, j = place()
        _, across = ring(i)
        landed(self.near.at[0, s], self.r_core.at[0, s])
        both = self.parts[owned(across, s)].astype(jnp.float32)
        both = both + self.near[0, s].astype(jnp.float32)
        self.near[0, s] = both.astype(jnp.bfloat16)
        send(
            self.near.at[0, s], self.far.at[s], self.s_x.at[s], self.r_x.at[s], at(across, j)
        ).start()

    def total(self, s):
        i, _ = place()
        landed(self.near.at[1, s], self.r_core.at[1, s])
        both = self.parts[owned(i, s)].astype(jnp.float32) + self.near[1, s].astype(jnp.float32)
        landed(self.far.at[s], self.r_x.at[s])
        return both + self.far[s].astype(jnp.float32)

    def finish(self):
        for s in (0, 1):
            landed(self.near.at[0, s], self.s_x.at[s])
            for side in (0, 1):
                landed(self.near.at[side, s], self.s_core.at[side, s])


def when(condition):
    return (lambda body: body()) if condition is None else pl.when(condition)


class Exchange:
    def __init__(self, pieces, sems):
        self.pieces = pieces
        self.send_sem, self.recv_sem, self.own_sem = sems

    @staticmethod
    def sems(count):
        return [DMA((3, count)), DMA((3, count)), DMA((count,))]

    def start(self):
        i, j = place()
        for step in (2, 3, 1):
            other = lax.rem(i + step, 4)
            for index, (src, dst, sends, _) in enumerate(self.pieces(i, other)):

                @when(sends)
                def _():
                    send(
                        src,
                        dst,
                        self.send_sem.at[step - 1, index],
                        self.recv_sem.at[step - 1, index],
                        at(other, j),
                    ).start()

        for index, (src, dst, sends, _) in enumerate(self.pieces(i, i)):

            @when(sends)
            def _():
                pltpu.make_async_copy(src, dst, self.own_sem.at[index]).start()

    def wait(self):
        i, _ = place()
        for step in (2, 3, 1):
            there, source = lax.rem(i + step, 4), lax.rem(i + 4 - step, 4)
            for index, (src, _, sends, _) in enumerate(self.pieces(i, there)):

                @when(sends)
                def _():
                    landed(src, self.send_sem.at[step - 1, index])

            for index, (src, _, _, gets) in enumerate(self.pieces(i, source)):

                @when(gets)
                def _():
                    landed(src, self.recv_sem.at[step - 1, index])

        for index, (src, _, sends, _) in enumerate(self.pieces(i, i)):

            @when(sends)
            def _():
                landed(src, self.own_sem.at[index])


ARRIVAL = ((1, 2, 3), (2, 0, 3), (1, 3, 0), (2, 1, 0))
LEAVING = ((1, 2, 3), (0, 2, 3), (3, 1, 0), (2, 1, 0))


def pick(table, z, n):
    row = [entry[n] for entry in table]
    return jnp.where(z == 0, row[0], jnp.where(z == 1, row[1], jnp.where(z == 2, row[2], row[3])))


def inner(z):
    return (z == 1) | (z == 2)


class SeqGather:
    def __init__(self, blocks, sems):
        self.blocks = blocks
        self.s_z, self.r_z, self.s_on, self.s_y, self.r_y = sems

    @staticmethod
    def sems(count):
        return [DMA((count, 2)), DMA((count, 4)), DMA((count, 4)), DMA((count, 4)), DMA((count, 4))]

    def relays(self, source):
        z = place()[1] // 2
        return inner(z) & ((source // 2 != z // 2) | inner(source))

    def start_z(self, chunk):
        i, j = place()
        z, x = j // 2, lax.rem(j, 2)
        own = self.blocks[chunk](z, x)
        targets = [pick(((2, 1), (2, 0), (1, 3), (1, 2)), z, n) for n in (0, 1)]
        for n, target in enumerate(targets):
            peer = at(i, 2 * target + x)
            send(own, own, self.s_z.at[chunk, n], self.r_z.at[chunk, z], peer).start()

    def start_y(self, chunk):
        i, j = place()
        z, x = j // 2, lax.rem(j, 2)
        own = self.blocks[chunk](z, x)
        peer = at(i, 2 * z + 1 - x)
        send(own, own, self.s_y.at[chunk, z], self.r_y.at[chunk, z], peer).start()

    def relayed(self, chunk):
        _, j = place()
        z, x = j // 2, lax.rem(j, 2)
        own = self.blocks[chunk](z, x)
        for n in (0, 1):
            landed(own, self.s_z.at[chunk, n])
        for n in (0, 1, 2):
            source = pick(ARRIVAL, z, n)

            @pl.when(self.relays(source))
            def _():
                landed(own, self.s_on.at[chunk, source])

    def forward(self, chunk, n):
        i, j = place()
        z, x = j // 2, lax.rem(j, 2)
        source = pick(ARRIVAL, z, n)
        block = self.blocks[chunk](source, x)
        landed(block, self.r_z.at[chunk, source])

        @pl.when(self.relays(source))
        def _():
            peer = at(i, 2 * jnp.where(z == 1, 0, 3) + x)
            send(
                block, block, self.s_on.at[chunk, source], self.r_z.at[chunk, source], peer
            ).start()

        peer = at(i, 2 * z + 1 - x)
        send(block, block, self.s_y.at[chunk, source], self.r_y.at[chunk, source], peer).start()

    def arrived(self, chunk, source):
        x = lax.rem(place()[1], 2)
        landed(self.blocks[chunk](source, 1 - x), self.r_y.at[chunk, source])

    def drain(self, chunk):
        _, j = place()
        z, x = j // 2, lax.rem(j, 2)
        own = self.blocks[chunk](z, x)
        landed(own, self.s_y.at[chunk, z])
        for n in (0, 1, 2):
            landed(own, self.s_y.at[chunk, pick(ARRIVAL, z, n)])

    def finish(self, chunk):
        z = place()[1] // 2
        self.arrived(chunk, z)
        for n in (0, 1, 2):
            self.arrived(chunk, pick(ARRIVAL, z, n))
        self.drain(chunk)


class SeqSum:
    def __init__(self, parts, near, far, sems):
        self.parts, self.near, self.far = parts, near, far
        self.s_y, self.r_y, self.s_z, self.r_z = sems

    @staticmethod
    def sems(count):
        return [DMA((count, 4)) for _ in range(4)]

    def start(self, chunk, row):
        i, j = place()
        z, x = j // 2, lax.rem(j, 2)
        send(
            self.parts[chunk](row, 1 - x),
            self.near[chunk](row),
            self.s_y.at[chunk, row],
            self.r_y.at[chunk, row],
            at(i, 2 * z + 1 - x),
        ).start()

    def start_rest(self, chunk):
        z = place()[1] // 2
        for n in (0, 1, 2):
            self.start(chunk, pick(LEAVING, z, n))

    def add(self, target, terms):
        if len(target.shape) == 3:
            for e in range(target.shape[0]):
                self.add(target.at[e], [term.at[e] for term in terms])
            return
        rows = target.shape[0]
        step = min(256, rows)

        @pl.loop(0, rows // step)
        def _(t):
            part = pl.ds(pl.multiple_of(t * step, step), step)
            total = target[part, :].astype(jnp.float32)
            for term in terms:
                total = total + term[part, :].astype(jnp.float32)
            target[part, :] = total.astype(jnp.bfloat16)

    def cross(self, chunk, n):
        i, j = place()
        z, x = j // 2, lax.rem(j, 2)
        row = pick(LEAVING, z, n)
        held = 2 + lax.rem(row, 2)
        near, own, far = self.near[chunk](row), self.parts[chunk](row, x), self.far[chunk](held)
        landed(near, self.r_y.at[chunk, row])
        if n == 0:
            self.add(near, (own,))
        else:

            @pl.when(inner(z))
            def _():
                landed(far, self.r_z.at[chunk, held])
                self.add(near, (own, far))

            @pl.when(jnp.logical_not(inner(z)))
            def _():
                self.add(near, (own,))

        target = jnp.where(inner(z), row, jnp.where(z == 0, 1, 2))
        spot = jnp.where(target == row, z // 2, held)
        send(
            near,
            self.far[chunk](spot),
            self.s_z.at[chunk, row],
            self.r_z.at[chunk, spot],
            at(i, 2 * target + x),
        ).start()

    def finish(self, chunk):
        _, j = place()
        z, x = j // 2, lax.rem(j, 2)
        near, far = self.near[chunk](z), [self.far[chunk](spot) for spot in (0, 1)]
        landed(near, self.r_y.at[chunk, z])
        for spot in (0, 1):
            landed(far[spot], self.r_z.at[chunk, spot])
        self.add(near, (self.parts[chunk](z, x), *far))

    def drain(self, chunk):
        _, j = place()
        z, x = j // 2, lax.rem(j, 2)
        for row in range(4):
            landed(self.near[chunk](row), self.s_y.at[chunk, row])
        for n in (0, 1, 2):
            row = pick(LEAVING, z, n)
            landed(self.near[chunk](row), self.s_z.at[chunk, row])


class SmallSum:
    def __init__(self, value, scratch):
        self.value = value
        self.stages, self.sems = scratch[:3], scratch[3:]

    @staticmethod
    def scratch(shape):
        return [pltpu.VMEM((count,) + shape, jnp.float32) for count in (4, 4, 2)] + [
            DMA((count,)) for count in (3, 3, 3, 3, 1, 1)
        ]

    def round(self, stage):
        i, j = place()
        z, y = j // 2, lax.rem(j, 2)
        return ((i, dp_peers()), (z, seq_peers()[:3]), (y, seq_peers()[3:]))[stage]

    def start(self, stage):
        spot, peers = self.round(stage)
        held = self.stages[stage]
        held[spot] = self.value[...] if stage == 0 else self.total(stage - 1)
        for step, peer in enumerate(peers):
            send(
                held.at[spot],
                held.at[spot],
                self.sems[2 * stage].at[step],
                self.sems[2 * stage + 1].at[step],
                peer,
            ).start()

    def total(self, stage):
        held = self.stages[stage]
        for step in range(held.shape[0] - 1):
            landed(held.at[0], self.sems[2 * stage + 1].at[step])
            landed(held.at[0], self.sems[2 * stage].at[step])
        total = held[0]
        for index in range(1, held.shape[0]):
            total = total + held[index]
        return total


def swap_halves(x):
    lane = lax.broadcasted_iota(jnp.int32, x.shape, 1)
    width = x.shape[1]
    return jnp.where(lane % 64 < 32, pltpu.roll(x, width - 32, 1), pltpu.roll(x, 32, 1))


def angle_tables(table):
    lane = lax.broadcasted_iota(jnp.int32, table.shape, 1)
    by_32, by_64, by_96 = (pltpu.roll(table, shift, 1) for shift in (32, 64, 96))
    first, second, third = lane < 32, lane < 64, lane < 96
    cos_t = jnp.where(first, table, jnp.where(second, by_32, jnp.where(third, by_64, by_96)))
    sin_t = jnp.where(first, -by_96, jnp.where(second, table, jnp.where(third, -by_32, by_64)))
    return cos_t, sin_t


def first_slice(i, b, second=0):
    return jnp.minimum((6 * b - i + 3) // 4 + second, 11)


def local_slice(i, b, second=0):
    return jnp.minimum(lax.rem(i + 2 * lax.rem(b, 2), 4) + 4 * second, 5)


def has_second(i, b):
    return lax.rem(i + 2 * lax.rem(b, 2), 4) < 2


def spot(index, size):
    return pl.ds(pl.multiple_of(size * index, size), size)


def attention_pieces(turned_qkv, w_out, heads, outs):
    def pieces(me, other):
        _, j = place()
        b, rows = column_block(me, j), row_block(me, j)
        found = [(w_out.at[spot(other, 64)], outs.at[b, spot(rows, 64)], None, None)]
        for second in (0, 1):
            found.append(
                (
                    turned_qkv.at[spot(local_slice(other, b, second), 64)],
                    heads.at[spot(first_slice(other, b, second), 64), spot(rows, 256)],
                    has_second(other, b) if second else None,
                    has_second(me, column_block(other, j)) if second else None,
                )
            )
        return found

    return pieces


def return_attention(heads, outs, g_qkv, g_out):
    def pieces(me, other):
        _, j = place()
        b = column_block(other, j)
        side, half = other // 2, lax.rem(other, 2)
        found = [(outs.at[side, spot(half, 64)], g_out.at[spot(me, 64)], None, None)]
        for second in (0, 1):
            held = jnp.minimum(first_slice(me, b, second) - 3 * (j // 2), 2)
            found.append(
                (
                    heads.at[spot(held, 64), spot(half, 256)],
                    g_qkv.at[spot(local_slice(me, b, second), 64)],
                    has_second(me, b) if second else None,
                    has_second(other, column_block(me, j)) if second else None,
                )
            )
        return found

    return pieces


def ffn_pieces(w_gate, w_up, w_down, dst):
    def pieces(me, other):
        _, j = place()
        b, rows = column_block(me, j), row_block(me, j)
        return [
            (w_gate.at[:, spot(other, 128)], dst.at[b, spot(rows, 256)], None, None),
            (w_up.at[:, spot(other, 128)], dst.at[b, spot(4 + rows, 256)], None, None),
        ] + [
            (
                w_down.at[spot(4 * half + other, 128)],
                dst.at[b, spot(16 + 2 * rows + half, 128)],
                None,
                None,
            )
            for half in (0, 1)
        ]

    return pieces


def return_ffn(src, g_gate, g_up, g_down):
    def pieces(me, other):
        side, part = other // 2, lax.rem(other, 2)
        return [
            (src.at[0, side, spot(part, 256)], g_gate.at[:, spot(me, 128)], None, None),
            (src.at[1, side, spot(part, 256)], g_up.at[:, spot(me, 128)], None, None),
        ] + [
            (
                src.at[2, side, spot(2 * part + half, 128)],
                g_down.at[spot(4 * half + me, 128)],
                None,
                None,
            )
            for half in (0, 1)
        ]

    return pieces


def position_table(labels):
    lane = lax.broadcasted_iota(jnp.int32, (128, 128), 1)
    frequency = jnp.exp(-jnp.log(10000.0) * (lane % 32).astype(jnp.float32) / 32)
    angle = labels[:, 3:4] * frequency
    rest = jnp.where(lane == 64, labels[:, 2:3], jnp.where(lane == 65, labels[:, 1:2], labels[:, 0:1]))
    return jnp.where(lane < 32, jnp.cos(angle), jnp.where(lane < 64, jnp.sin(angle), rest))


def norm_rows(hidden):
    return lax.rsqrt(jnp.mean(hidden * hidden, axis=1, keepdims=True) + EPSILON)


def back_rows(grad_in, hidden, inv_rms):
    mean = jnp.mean(grad_in * hidden, axis=1, keepdims=True)
    return inv_rms * grad_in - hidden * (inv_rms * inv_rms * inv_rms * mean)


FFN_CHUNKS = (2048, 0, 1024)
GRAD_CHUNKS = (0, 1024, 2048)


def wide(ref, first, rows):
    return jnp.concatenate([ref[first, rows, :], ref[first + 1, rows, :]], axis=1)


def store_wide(ref, first, rows, value):
    ref[first, rows, :] = value[:, :128]
    ref[first + 1, rows, :] = value[:, 128:]


def two(ref, t, cols=slice(None)):
    value = ref[pl.ds(2 * t, 2), :, cols]
    return value.reshape(256, value.shape[2])


def layer_kernel(*refs):
    (
        tok, cot, segments, variates, times, pads, w_qkv, w_out, w_gate, w_up, w_down,
        gain_attn, gain_ffn, bias_all,
    ), refs = refs[:14], refs[14:]
    (output, input_grad, r_gate, r_up, r_down, r_qkv, r_out, small_out), refs = refs[:8], refs[8:]
    (
        tok_all, cot_all, tab_all, idr_all, tok_own, heads_w, out_w, heads_g, out_g, wm_ref, q_ref,
        k_ref, v_ref, o_ref, lse_ref, rows_ref, part, mid_ref, a2_all, turned, ffn_all, ffn_g,
        hidden_s, dgate_s, dup_s, e2_ref, dq_acc, dk_acc, dv_acc, out_own, in_own, dbias, small,
        near_f, far_f, near_q, far_q, near_o, far_o, idr, turned_qkv,
    ), refs = refs[:41], refs[41:]
    home_in, refs = refs[:2], refs[2:]
    home_out, refs = refs[:2], refs[2:]
    gather_in, refs = refs[:6], refs[6:]
    gather_a2, refs = refs[:6], refs[6:]
    gather_ez, refs = refs[:6], refs[6:]
    buffers, refs = refs[:2], refs[2:]
    out_buffers, refs = refs[:2], refs[2:]
    sum_sems, refs = [refs[4 * n : 4 * n + 4] for n in range(4)], refs[16:]
    spread_a, spread_f, back_a, back_f = [refs[3 * n : 3 * n + 3] for n in range(4)]
    refs = refs[12:]
    chain_a, chain_f, refs = refs[:5], refs[5:10], refs[10:]
    fold_f, fold_a, refs = refs[:4], refs[4:8], refs[8:]
    small_scratch = refs

    i, j = place()
    z, y = j // 2, lax.rem(j, 2)
    mine_first = 2 * (1 - lax.rem(i, 2))

    def turn(u):
        return lax.rem(mine_first + u, 4)

    ez_all, dqkv_ref, out_part = dgate_s, dup_s, turned
    home = Home((tok, idr, cot), (tok_all, idr_all, cot_all), home_in, False)
    group = GroupGather((tok_all, idr_all, cot_all), gather_in)
    spread = Exchange(attention_pieces(turned_qkv, w_out, heads_w, out_w), spread_a)
    spread_ffn = Exchange(ffn_pieces(w_gate, w_up, w_down, ffn_all), spread_f)

    def heads_block(ref):
        return lambda row, side: ref.at[spot(row, 192), spot(side, 512)]

    def outs_block(ref):
        return lambda row, side: ref.at[spot(row, 2), spot(side, 128)]

    def ffn_block(ref, start):
        return lambda row, side: ref.at[spot(row, 2), spot(start // 512 + side, 512)]

    attn_w = SeqGather((heads_block(heads_w), outs_block(out_w)), chain_a)
    ffn_w = SeqGather([ffn_block(ffn_all, start) for start in FFN_CHUNKS], chain_f)
    branch = GroupSum(part, buffers, sum_sems[0])
    second = GroupGather((a2_all,), gather_a2)
    da_sum = GroupSum(part, buffers, sum_sems[1])
    out_sum = GroupSum(out_part, out_buffers, sum_sems[2])
    da1_sum = GroupSum(part, buffers, sum_sems[3])
    third = GroupGather((ez_all,), gather_ez)
    leave = Home((out_own, in_own), (output, input_grad), home_out, True)
    ffn_fold = SeqSum(
        [ffn_block(ffn_g, start) for start in GRAD_CHUNKS],
        [lambda row, chunk=chunk: near_f.at[row, chunk] for chunk in (0, 1, 2)],
        [lambda held, chunk=chunk: far_f.at[held, chunk] for chunk in (0, 1, 2)],
        fold_f,
    )
    attn_fold = SeqSum(
        (heads_block(heads_g), outs_block(out_g)),
        (lambda row: near_q.at[row], lambda row: near_o.at[row]),
        (lambda held: far_q.at[held], lambda held: far_o.at[held]),
        fold_a,
    )
    ffn_back = Exchange(return_ffn(near_f.at[z], r_gate, r_up, r_down), back_f)
    attn_back = Exchange(return_attention(near_q.at[z], near_o.at[z], r_qkv, r_out), back_a)

    turned_qkv[...] = w_qkv[...].T
    for s in (0, 1):
        label = [ref[s : s + 1, :] for ref in (segments, variates, times, pads)]
        lines = (jnp.where(label[3] == 1, label[0], -1), label[1], label[0], label[2])
        for line, value in enumerate(lines):
            idr[s, line : line + 1, :] = value.astype(jnp.float32)
        idr[s, 4:8, :] = jnp.zeros((4, 128), jnp.float32)
    gain_one, gain_two = gain_attn[...].astype(jnp.float32), gain_ffn[...].astype(jnp.float32)
    sixteen = lax.broadcasted_iota(jnp.int32, (1, 16), 1)
    bias = [
        jnp.sum(
            jnp.where(sixteen == 4 * h + i, bias_all[...].astype(jnp.float32), 0.0),
            axis=1,
            keepdims=True,
        )
        for h in range(4)
    ]
    meet(dp_peers() + seq_peers(), home=True)
    spread.start()
    for a in (0, 1):
        for s in (0, 1):
            home.start(a, s)
    spread.wait()
    for chunk in (0, 1):
        attn_w.start_z(chunk)
    for chunk in (0, 1):
        attn_w.start_y(chunk)
    for a in (0, 1):
        for s in (0, 1):
            home.wait(a, s)
            group.push(a, s)
    spread_ffn.start()
    for s in (0, 1):
        tok_own[s] = tok_all[owned(i, s)]
    for n in (0, 1, 2):
        for chunk in (0, 1):
            attn_w.forward(chunk, n)
    for a in (0, 1):
        for s in (0, 1):
            group.relay(a, s)
    for chunk in (0, 1):
        attn_w.relayed(chunk)
    spread_ffn.wait()
    ffn_w.start_z(0)
    for s in (0, 1):
        home.start(2, s)
    for a in (0, 1):
        group.finish(a)
        home.finish(a)
    for b in range(8):
        rows_ref[:, 128 * b : 128 * b + 128] = idr_all[b]

    @pl.loop(0, 8)
    def _(b):
        hidden = tok_all[b].astype(jnp.float32)
        tok_all[b] = (hidden * norm_rows(hidden) * gain_one).astype(jnp.bfloat16)
        tab_all[b] = position_table(idr_all[b].T)

    a1_all = tok_all
    for chunk in (0, 1):
        attn_w.finish(chunk)
    for chunk in (0, 1, 2):
        ffn_w.start_y(chunk)
    for b in range(8):
        wm_ref[:, 128 * b : 128 * b + 128] = out_w[b]

    @pl.loop(0, 4)
    def _(t):
        rows = pl.ds(pl.multiple_of(t * 256, 256), 256)
        proj = dot(two(a1_all, t), heads_w[...], NT)
        cos_t, sin_t = angle_tables(two(tab_all, t))
        for pair in (0, 1):
            cols = slice(128 * pair, 128 * pair + 128)
            for base, out in ((0, q_ref), (256, k_ref)):
                x = proj[:, base + 128 * pair : base + 128 * pair + 128]
                out[rows, cols] = (x * cos_t + swap_halves(x) * sin_t).astype(jnp.bfloat16)
        v_ref[rows, :] = proj[:, 512:768].astype(jnp.bfloat16)

    @pl.loop(0, 4)
    def _(u):
        t = turn(u)
        start = pl.multiple_of(t * 256, 256)
        rows = pl.ds(start, 256)
        columns = two(tab_all, t)
        seg_q, var_q = columns[:, 64:65], columns[:, 65:66]
        code_k, var_k = rows_ref[0:1, :], rows_ref[1:2, :]
        row = start + lax.broadcasted_iota(jnp.int32, (256, 1024), 0)
        col = lax.broadcasted_iota(jnp.int32, (256, 1024), 1)
        allowed = ((seg_q == code_k) & (jnp.abs(row - col) <= WINDOW)) | (row == col)
        masked = jnp.where(allowed, 0.0, NEGATIVE)
        same = jnp.where(var_q == var_k, 1.0, 0.0)
        stats = jnp.zeros((256, 128), jnp.float32)
        lane = lax.broadcasted_iota(jnp.int32, (256, 128), 1)
        for h in range(4):
            cols = slice(64 * h, 64 * h + 64)
            scores = dot(q_ref[rows, cols] * 0.125, k_ref[:, cols], NT)
            scores = scores + bias[h] * same + masked
            top = jnp.max(scores, axis=1, keepdims=True)
            weight = jnp.exp(scores - top)
            total = jnp.sum(weight, axis=1, keepdims=True)
            mixed = dot(weight.astype(jnp.bfloat16), v_ref[:, cols])
            o_ref[rows, cols] = (mixed / total).astype(jnp.bfloat16)
            stats = jnp.where(lane == h, top + jnp.log(total), stats)
        lse_ref[:, rows] = stats.T[:8]
        part[pl.ds(2 * t, 2)] = dot(o_ref[rows, :], wm_ref[...], out=jnp.bfloat16).reshape(2, 128, 1024)
        for s in (0, 1):

            @pl.when(u == s)
            def _():
                branch.start(s)

            @pl.when(u == s + 2)
            def _():
                branch.cross(s)

        @pl.when(u == 0)
        def _():
            for n in (0, 1, 2):
                ffn_w.forward(0, n)
            ffn_w.start_z(1)

        @pl.when(u == 1)
        def _():
            for s in (0, 1):
                home.wait(2, s)
                group.push(2, s)

        @pl.when(u == 3)
        def _():
            for s in (0, 1):
                group.relay(2, s)
            for n in (0, 1, 2):
                ffn_w.forward(1, n)
            ffn_w.start_z(2)

    for s in (0, 1):
        block = owned(i, s)
        mid = tok_own[s].astype(jnp.float32) + branch.total(s)
        mid_ref[s] = mid
        a2_all[block] = (mid * norm_rows(mid) * gain_two).astype(jnp.bfloat16)
        second.push(0, s)
    branch.finish()
    for s in (0, 1):
        second.relay(0, s)
    group.finish(2)
    home.finish(2)
    second.finish(0)
    ffn_w.finish(0)
    for n in (0, 1):
        ffn_w.forward(2, n)

    @pl.loop(0, 4)
    def _(t):
        for d in range(4):
            turned[2 * d : 2 * d + 2, :, pl.ds(pl.multiple_of(256 * t, 256), 256)] = (
                two(a2_all, t, slice(256 * d, 256 * d + 256)).T.reshape(2, 128, 256)
            )

    def unit(f):
        cols = pl.ds(pl.multiple_of(256 * f, 256), 256)
        wg, wu = wide(ffn_all, 2 * f, slice(0, 1024)), wide(ffn_all, 2 * f, slice(1024, 2048))
        down = pl.ds(pl.multiple_of(2048 + 256 * f, 256), 256)
        wd = jnp.concatenate([ffn_all[b, down, :] for b in range(8)], axis=1)

        @pl.loop(0, 4)
        def _(t):
            a, g = two(a2_all, t), two(cot_all, t)
            gate, up, dh = dot(a, wg), dot(a, wu), dot(g, wd, NT)
            sig = 1.0 / (1.0 + jnp.exp(-gate))
            gate_sig = gate * sig
            into = (pl.ds(2 * t, 2), slice(None), cols)
            hidden_s[into] = (gate_sig * up).astype(jnp.bfloat16).reshape(2, 128, 256)
            dgate = dh * up * (sig + gate_sig * (1.0 - sig))
            dgate_s[into] = dgate.astype(jnp.bfloat16).reshape(2, 128, 256)
            dup_s[into] = (dh * gate_sig).astype(jnp.bfloat16).reshape(2, 128, 256)

        @pl.loop(0, 4)
        def _(d):
            rows = pl.ds(pl.multiple_of(d * 256, 256), 256)
            rows_up = pl.ds(pl.multiple_of(1024 + d * 256, 256), 256)
            a_t = two(turned, d)
            dgate, dup = dgate_s[:, :, cols].reshape(1024, 256), dup_s[:, :, cols].reshape(1024, 256)
            store_wide(ffn_g, 2 * f, rows, dot(a_t, dgate, out=jnp.bfloat16))
            store_wide(ffn_g, 2 * f, rows_up, dot(a_t, dup, out=jnp.bfloat16))

        h_t = hidden_s[:, :, cols].reshape(1024, 256).T
        for d in range(4):
            g = cot_all[:, :, 256 * d : 256 * d + 256].reshape(1024, 256)
            store_wide(ffn_g, 2 * d, down, dot(h_t, g, out=jnp.bfloat16))

    @pl.loop(0, 4)
    def _(step):
        f = z
        for n in (0, 1, 2):
            f = jnp.where(step == n + 1, pick(ARRIVAL, z, n), f)
        @pl.when(step == 1)
        def _():
            ffn_w.forward(2, 2)

        ffn_w.arrived(1, f)
        ffn_w.arrived(2, f)
        unit(f)

        @pl.when(step > 0)
        def _():
            ffn_fold.start(0, f)
            ffn_fold.start(1, f)

    for chunk in (0, 1, 2):
        ffn_w.relayed(chunk)
    for chunk in (1, 2):
        ffn_w.drain(chunk)

    def at_end(chunk, n):
        @pl.when(jnp.logical_not(inner(z)))
        def _():
            ffn_fold.cross(chunk, n)

    def at_inner(chunk, n):
        @pl.when(inner(z))
        def _():
            ffn_fold.cross(chunk, n)

    def product(left, t, first_row):
        total = None
        for p in range(4):
            piece = dot(
                two(left, t, slice(256 * p, 256 * p + 256)),
                wide(ffn_all, 2 * p, slice(first_row, first_row + 1024)),
                NT,
            )
            total = piece if total is None else total + piece
        return total

    @pl.loop(0, 4)
    def _(u):
        t = turn(u)
        value = product(dgate_s, t, 0) + product(dup_s, t, 1024)
        part[pl.ds(2 * t, 2)] = value.astype(jnp.bfloat16).reshape(2, 128, 1024)
        for s in (0, 1):

            @pl.when(u == s)
            def _():
                da_sum.start(s)

            @pl.when(u == s + 2)
            def _():
                da_sum.cross(s)

    @pl.loop(0, 4)
    def _(u):
        t = turn(u)
        hidden = two(hidden_s, t)
        for d in range(4):
            w = wide(ffn_all, 2 * d, slice(2048, 3072))
            out_part[pl.ds(2 * t, 2), :, 256 * d : 256 * d + 256] = dot(
                hidden, w, out=jnp.bfloat16
            ).reshape(2, 128, 256)
        for s in (0, 1):

            @pl.when(u == s)
            def _():
                out_sum.start(s)

    at_end(0, 0), at_end(1, 0)
    gain_rows = jnp.zeros((1, 1024), jnp.float32)
    for s in (0, 1):
        mid = mid_ref[s]
        inv = norm_rows(mid)
        da2 = da_sum.total(s)
        gain_rows = gain_rows + jnp.sum(da2 * (mid * inv), axis=0, keepdims=True)
        e2 = cot_all[owned(i, s)].astype(jnp.float32) + back_rows(da2 * gain_two, mid, inv)
        e2_ref[s] = e2
        ez_all[owned(i, s)] = e2.astype(jnp.bfloat16)
        third.push(0, s)
    for b in range(8):
        small[8 + b : 9 + b, :] = gain_rows[:, 128 * b : 128 * b + 128]
    da_sum.finish()
    ffn_fold.start_rest(2)
    at_inner(0, 0), at_inner(1, 0)
    at_end(0, 1), at_end(1, 1)
    for s in (0, 1):
        out_sum.cross(s)
    third.near(0)

    def unturn(acc, base, blocks, rows):
        for block, part_rows in zip(blocks, rows):
            cos_t, sin_t = angle_tables(tab_all[block])
            for pair in (0, 1):
                g = acc[part_rows, 128 * pair : 128 * pair + 128]
                dqkv_ref[block, :, base + 128 * pair : base + 128 * pair + 128] = (
                    g * cos_t - swap_halves(g) * sin_t
                ).astype(jnp.bfloat16)

    dk_acc[...] = jnp.zeros_like(dk_acc)
    dv_acc[...] = jnp.zeros_like(dv_acc)
    dbias[...] = jnp.zeros_like(dbias)

    @pl.loop(0, 4)
    def _(u):
        @pl.when(u == 2)
        def _():
            third.relay(0, 0)
            third.relay(0, 1)
            third.beyond(0)
            for d in range(4):
                ez = ez_all[:, :, 256 * d : 256 * d + 256].reshape(1024, 256)
                store_wide(out_g, 2 * d, slice(None), dot(o_ref[...], ez, TN, jnp.bfloat16))
            attn_fold.start_rest(1)

        b = 2 * lax.rem(u, 2) + jnp.where(u < 2, i // 2, 1 - i // 2)
        upper = b + 4
        rows = pl.ds(pl.multiple_of(128 * b, 128), 128)
        rows_up = pl.ds(pl.multiple_of(128 * upper, 128), 128)

        def both(ref, cols):
            return jnp.concatenate([ref[rows, cols], ref[rows_up, cols]], axis=0)

        do = dot(jnp.concatenate([ez_all[b], ez_all[upper]], axis=0), wm_ref[...], NT, jnp.bfloat16)
        columns = tab_all[...].reshape(1024, 128)
        var_k, code_k = columns[:, 65:66], columns[:, 66:67]
        label = jnp.concatenate([idr_all[b], idr_all[upper]], axis=1)
        log_sum = jnp.concatenate([lse_ref[:, rows], lse_ref[:, rows_up]], axis=1)
        seg_q, var_q = label[2:3, :], label[1:2, :]
        row = lax.broadcasted_iota(jnp.int32, (1024, 256), 0)
        lane = lax.broadcasted_iota(jnp.int32, (1024, 256), 1)
        col = 128 * b + jnp.where(lane < 128, lane, lane + 384)
        allowed = ((seg_q == code_k) & (jnp.abs(row - col) <= WINDOW)) | (row == col)
        masked = jnp.where(allowed, 0.0, NEGATIVE)
        same = jnp.where(var_q == var_k, 1.0, 0.0)
        for h in range(4):
            cols = slice(64 * h, 64 * h + 64)
            q_h, k_h, v_h = both(q_ref, cols) * 0.125, k_ref[:, cols], v_ref[:, cols]
            do_h = do[:, cols]
            scores = dot(k_h, q_h, NT) + bias[h] * same + masked
            prob = jnp.exp(scores - log_sum[h : h + 1, :])
            dv_acc[:, cols] += dot(prob.astype(jnp.bfloat16), do_h)
            dprob = dot(v_h, do_h, NT)
            mean = jnp.sum(prob * dprob, axis=0, keepdims=True)
            dscore = (prob * (dprob - mean)).astype(jnp.bfloat16)
            dbias[h : h + 1, :] += jnp.sum(dscore.astype(jnp.float32) * same, axis=0, keepdims=True)
            dk_acc[:, cols] += dot(dscore, q_h)
            dq_acc[:, cols] = dot(dscore, k_h, TN) * 0.125

        unturn(dq_acc, 0, (b, upper), (slice(0, 128), slice(128, 256)))

        @pl.when(u == 0)
        def _():
            at_end(0, 2), at_end(1, 2)

        @pl.when(u == 1)
        def _():
            at_inner(0, 1), at_inner(1, 1)
            ffn_fold.cross(2, 0)

        @pl.when(u == 2)
        def _():
            at_inner(0, 2), at_inner(1, 2)
            at_end(2, 1), at_end(2, 2)
            ffn_fold.start(0, z)

        @pl.when(u == 3)
        def _():
            at_inner(2, 1)

    @pl.loop(0, 4)
    def _(t):
        rows = pl.ds(pl.multiple_of(t * 256, 256), 256)
        unturn(
            dk_acc,
            256,
            (2 * t, 2 * t + 1),
            [pl.ds(pl.multiple_of(t * 256 + 128 * e, 128), 128) for e in (0, 1)],
        )
        dqkv_ref[pl.ds(2 * t, 2), :, 512:768] = (
            dv_acc[rows, :].astype(jnp.bfloat16).reshape(2, 128, 256)
        )

    for d in range(3):
        block = slice(256 * d, 256 * d + 256)
        heads_g[block, :] = dot(
            dqkv_ref[:, :, block].reshape(1024, 256), a1_all[...].reshape(1024, 1024), TN, jnp.bfloat16
        )
    at_inner(2, 2)
    attn_fold.start_rest(0)
    for s in (0, 1):
        out_own[s] = (mid_ref[s] + out_sum.total(s)).astype(jnp.bfloat16)
        leave.start(0, s)

    @pl.loop(0, 4)
    def _(u):
        t = turn(u)
        part[pl.ds(2 * t, 2)] = dot(
            two(dqkv_ref, t, slice(0, 768)), heads_w[...], out=jnp.bfloat16
        ).reshape(2, 128, 1024)
        for s in (0, 1):

            @pl.when(u == s)
            def _():
                da1_sum.start(s)

            @pl.when(u == s + 2)
            def _():
                da1_sum.cross(s)

    third.sent(0)
    for chunk in (1, 2):
        ffn_fold.start(chunk, z)
    for chunk in (1, 0):
        attn_fold.start(chunk, z)
    for chunk in (1, 0):
        attn_fold.cross(chunk, 0)

    @pl.when(jnp.logical_not(inner(z)))
    def _():
        for n in (1, 2):
            for chunk in (1, 0):
                attn_fold.cross(chunk, n)

    gain_rows = jnp.zeros((1, 1024), jnp.float32)
    for s in (0, 1):
        hidden = tok_own[s].astype(jnp.float32)
        inv = norm_rows(hidden)
        da1 = da1_sum.total(s)
        gain_rows = gain_rows + jnp.sum(da1 * (hidden * inv), axis=0, keepdims=True)
        grad = e2_ref[s] + back_rows(da1 * gain_one, hidden, inv)
        in_own[s] = grad.astype(jnp.bfloat16)
        leave.start(1, s)
    for b in range(8):
        small[b : b + 1, :] = gain_rows[:, 128 * b : 128 * b + 128]
    lane = lax.broadcasted_iota(jnp.int32, (8, 128), 1)
    line = lax.broadcasted_iota(jnp.int32, (8, 128), 0)
    bias_row = jnp.zeros((8, 128), jnp.float32)
    for h in range(4):
        value = jnp.sum(dbias[h : h + 1, :], axis=1, keepdims=True)
        bias_row = jnp.where((line == 0) & (lane == 4 * h + i), value, bias_row)
    small[16:24, :] = bias_row
    small_sum = SmallSum(small, small_scratch)
    small_sum.start(0)

    @pl.when(inner(z))
    def _():
        for n in (1, 2):
            for chunk in (1, 0):
                attn_fold.cross(chunk, n)

    for chunk in (0, 1, 2):
        ffn_fold.finish(chunk)
    ffn_back.start()
    small_sum.start(1)
    for chunk in (1, 0):
        attn_fold.finish(chunk)
    attn_back.start()
    small_sum.start(2)
    ffn_back.wait()
    small_out[...] = small_sum.total(2)
    out_sum.finish()
    da1_sum.finish()
    for a in (0, 1):
        for s in (0, 1):
            leave.wait(a, s)
        leave.finish(a)
    for chunk in (0, 1, 2):
        ffn_fold.drain(chunk)
    for chunk in (0, 1):
        attn_fold.drain(chunk)
    attn_back.wait()


def layer(arrays):
    def vmem(dtype, *shape):
        return pltpu.VMEM(shape, dtype)

    low, full = jnp.bfloat16, jnp.float32
    blocks = vmem(low, 8, 128, 1024)
    own = vmem(low, 2, 128, 1024)
    heads = vmem(low, 1024, 256)
    grads = vmem(full, 1024, 256)
    return pl.pallas_call(
        layer_kernel,
        out_shape=[
            bf16(2, 128, 1024),
            bf16(2, 128, 1024),
            bf16(256, 512),
            bf16(256, 512),
            bf16(1024, 128),
            bf16(384, 256),
            bf16(256, 128),
            f32(24, 128),
        ],
        in_specs=[HB, HB] + [VM] * 6 + [HB] * 3 + [VM] * 3,
        out_specs=[HB] * 7 + [VM],
        scratch_shapes=[
            blocks,
            blocks,
            vmem(full, 8, 128, 128),
            vmem(full, 8, 8, 128),
            own,
            vmem(low, 768, 1024),
            vmem(low, 8, 256, 128),
            vmem(low, 768, 1024),
            vmem(low, 8, 256, 128),
            vmem(low, 256, 1024),
            heads,
            heads,
            heads,
            heads,
            vmem(full, 8, 1024),
            vmem(full, 8, 1024),
            blocks,
            vmem(full, 2, 128, 1024),
            blocks,
            blocks,
            vmem(low, 8, 3072, 128),
            vmem(low, 8, 3072, 128),
            blocks,
            blocks,
            blocks,
            vmem(full, 2, 128, 1024),
            vmem(full, 256, 256),
            grads,
            grads,
            own,
            own,
            vmem(full, 8, 256),
            vmem(full, 24, 128),
            vmem(low, 4, 3, 2, 512, 128),
            vmem(low, 4, 3, 2, 512, 128),
            vmem(low, 4, 192, 512),
            vmem(low, 4, 192, 512),
            vmem(low, 4, 2, 128, 128),
            vmem(low, 4, 2, 128, 128),
            vmem(full, 2, 8, 128),
            vmem(low, 384, 256),
        ]
        + Home.sems(3)
        + Home.sems(2)
        + GroupGather.sems(3)
        + GroupGather.sems(1)
        + GroupGather.sems(1)
        + GroupSum.buffers()
        + GroupSum.buffers()
        + GroupSum.sems() * 4
        + Exchange.sems(3)
        + Exchange.sems(4)
        + Exchange.sems(3)
        + Exchange.sems(4)
        + SeqGather.sems(2)
        + SeqGather.sems(3)
        + SeqSum.sems(3)
        + SeqSum.sems(2)
        + SmallSum.scratch((24, 128)),
        compiler_params=pltpu.CompilerParams(
            collective_id=1, has_side_effects=True, vmem_limit_bytes=67_043_328
        ),
        name="layer",
    )(*arrays)


def finish_kernel(*refs):
    (out_in, grad_in, gate, up, down, qkv, out, small), refs = refs[:8], refs[8:]
    output, input_grad, g_qkv, g_out, g_gate, g_up, g_down, one, two_, bias = refs
    output[...] = out_in[...]
    input_grad[...] = grad_in[...]
    g_qkv[...] = qkv[...].astype(jnp.float32).T
    for target, source in ((g_out, out), (g_gate, gate), (g_up, up), (g_down, down)):
        target[...] = source[...].astype(jnp.float32)
    one[...] = small[0:8, :]
    two_[...] = small[8:16, :]
    bias[...] = small[16:17, 0:16]


def finish(arrays):
    return pl.pallas_call(
        finish_kernel,
        out_shape=[
            bf16(2, 128, 1024),
            bf16(2, 128, 1024),
            f32(256, 384),
            f32(256, 128),
            f32(256, 512),
            f32(256, 512),
            f32(1024, 128),
            f32(8, 128),
            f32(8, 128),
            f32(1, 16),
        ],
        in_specs=[VM] * 8,
        out_specs=[VM] * 10,
        name="finish",
    )(*arrays)


def on_group(
    tokens, segment_ids, variate_ids, time_ids, pad_mask, cotangent,
    w_qkv, w_out, w_gate, w_up, w_down, gain_attn, gain_ffn, variate_bias,
):
    results = layer(
        [
            tokens, cotangent, segment_ids, variate_ids, time_ids, pad_mask, w_qkv, w_out, w_gate, w_up,
            w_down, gain_attn[None], gain_ffn[None], variate_bias[None],
        ]
    )
    *large, one, two_, bias_grad = finish(results)
    return (*large, one.reshape(1024), two_.reshape(1024), bias_grad.reshape(16))


def solution(mesh):
    in_specs = (
        P("dp", "seq", None),
        P("dp", "seq"),
        P("dp", "seq"),
        P("dp", "seq"),
        P("dp", "seq"),
        P("dp", "seq", None),
        P("dp", "seq"),
        P("dp", "seq"),
        P("dp", "seq"),
        P("dp", "seq"),
        P("dp", "seq"),
        P(),
        P(),
        P(),
    )
    out_specs = (
        P("dp", "seq", None),
        P("dp", "seq", None),
        P("dp", "seq"),
        P("dp", "seq"),
        P("dp", "seq"),
        P("dp", "seq"),
        P("dp", "seq"),
        P(),
        P(),
        P(),
    )
    grouped = mesh.shape["dp"] == 4 and mesh.shape["seq"] == 8
    return jax.shard_map(
        on_group if grouped else on_device, mesh=mesh, in_specs=in_specs, out_specs=out_specs, check_vma=False
    )
```

```python
import functools

import jax
import jax.numpy as jnp
from jax import lax
from jax.experimental import pallas as pl
from jax.experimental.pallas import tpu as pltpu
from jax.sharding import PartitionSpec as P

HEADS = 16
HEAD_DIM = 64
WINDOW = 512


EPSILON = 1e-06
NEGATIVE = -1e30


def passed_along(block, axis, distance):
    devices = range(lax.axis_size(axis))
    route = [(i - distance, i) for i in devices if i - distance in devices]
    return lax.ppermute(block, axis, route)


def norm_scale(hidden):
    return lax.rsqrt(jnp.mean(hidden * hidden, axis=-1, keepdims=True) + EPSILON)


def norm_back(grad_in, hidden, inv_rms):
    return inv_rms * grad_in - hidden * inv_rms * inv_rms * inv_rms * jnp.mean(
        grad_in * hidden, axis=-1, keepdims=True
    )


def rope_tables(time_row, half_dim):
    frequency = jnp.exp(-jnp.log(10000.0) * jnp.arange(half_dim, dtype=jnp.float32) / half_dim)
    angles = time_row.astype(jnp.float32)[:, None] * frequency[None, :]
    return (jnp.cos(angles)[:, None, :], jnp.sin(angles)[:, None, :])


def rotate(values_in, cos_table, sine_table):
    half_dim = cos_table.shape[-1]
    first_half = values_in[..., :half_dim]
    second_half = values_in[..., half_dim:]
    return jnp.concatenate(
        [
            first_half * cos_table - second_half * sine_table,
            second_half * cos_table + first_half * sine_table,
        ],
        axis=-1,
    )


def rotate_back(grad_in, cos_table, sine_table):
    half_dim = cos_table.shape[-1]
    first_half = grad_in[..., :half_dim]
    second_half = grad_in[..., half_dim:]
    return jnp.concatenate(
        [
            first_half * cos_table + second_half * sine_table,
            second_half * cos_table - first_half * sine_table,
        ],
        axis=-1,
    )


def masked_scores(query_rot, keys_all, labels_own, labels_keys, var_bias, hop_count):
    row_count = query_rot.shape[0]
    key_count = keys_all.shape[0]
    offsets = (
        jnp.arange(key_count)[None, :] - hop_count * row_count - jnp.arange(row_count)[:, None]
    )
    allowed = (
        (jnp.abs(offsets) <= WINDOW)
        & (labels_own[0][:, None] == labels_keys[0][None, :])
        & ((labels_keys[2][None, :] == 1) | (offsets == 0))
    )
    same_var = (labels_own[1][:, None] == labels_keys[1][None, :]).astype(jnp.float32)
    scores = jnp.einsum(
        "qhd,khd->hqk", query_rot, keys_all, preferred_element_type=jnp.float32
    ) * HEAD_DIM ** (-0.5)
    scores = scores + var_bias[:, None, None] * same_var[None]
    return (jnp.where(allowed[None], scores, NEGATIVE), same_var)


def fetch_weights(shards):
    row_blocks = (
        lax.all_gather(shards[0], "dp", axis=0, tiled=True),
        lax.all_gather(shards[1], "dp", axis=0, tiled=True),
        lax.all_gather(shards[2], "dp", axis=0, tiled=True),
        lax.all_gather(shards[3], "dp", axis=0, tiled=True),
        lax.all_gather(shards[4], "dp", axis=0, tiled=True),
    )
    return (
        lax.all_gather(row_blocks[0], "seq", axis=1, tiled=True),
        lax.all_gather(row_blocks[1], "seq", axis=1, tiled=True),
        lax.all_gather(row_blocks[2], "seq", axis=1, tiled=True),
        lax.all_gather(row_blocks[3], "seq", axis=1, tiled=True),
        lax.all_gather(row_blocks[4], "seq", axis=1, tiled=True),
    )


def fetch_keep(shards):
    row_blocks = (
        lax.all_gather(shards[0], "dp", axis=0, tiled=True),
        lax.all_gather(shards[1], "dp", axis=0, tiled=True),
        lax.all_gather(shards[2], "dp", axis=0, tiled=True),
        lax.all_gather(shards[3], "dp", axis=0, tiled=True),
        lax.all_gather(shards[4], "dp", axis=0, tiled=True),
    )
    return (
        lax.all_gather(row_blocks[0], "seq", axis=1, tiled=True),
        lax.all_gather(row_blocks[1], "seq", axis=1, tiled=True),
        lax.all_gather(row_blocks[2], "seq", axis=1, tiled=True),
        lax.all_gather(row_blocks[3], "seq", axis=1, tiled=True),
        lax.all_gather(row_blocks[4], "seq", axis=1, tiled=True),
    )


def reduce_last(grads_full):
    col_sums = (
        lax.psum_scatter(grads_full[0], "seq", scatter_dimension=1, tiled=True),
        lax.psum_scatter(grads_full[1], "seq", scatter_dimension=1, tiled=True),
        lax.psum_scatter(grads_full[2], "seq", scatter_dimension=1, tiled=True),
        lax.psum_scatter(grads_full[3], "seq", scatter_dimension=1, tiled=True),
        lax.psum_scatter(grads_full[4], "seq", scatter_dimension=1, tiled=True),
    )
    return (
        lax.psum_scatter(
            col_sums[0].astype(jnp.bfloat16), "dp", scatter_dimension=0, tiled=True
        ).astype(jnp.float32),
        lax.psum_scatter(
            col_sums[1].astype(jnp.bfloat16), "dp", scatter_dimension=0, tiled=True
        ).astype(jnp.float32),
        lax.psum_scatter(
            col_sums[2].astype(jnp.bfloat16), "dp", scatter_dimension=0, tiled=True
        ).astype(jnp.float32),
        lax.psum_scatter(
            col_sums[3].astype(jnp.bfloat16), "dp", scatter_dimension=0, tiled=True
        ).astype(jnp.float32),
        lax.psum_scatter(
            col_sums[4].astype(jnp.bfloat16), "dp", scatter_dimension=0, tiled=True
        ).astype(jnp.float32),
    )


def weight_grads(pieces):
    (
        normed_one,
        grad_qkv,
        attended,
        grad_branch,
        normed_two,
        grad_gate,
        grad_up,
        hidden,
        grad_ffn,
    ) = pieces
    grad_w_qkv = jnp.einsum("td,tf->df", normed_one, grad_qkv, preferred_element_type=jnp.float32)
    grad_w_out = jnp.einsum("ti,to->io", attended, grad_branch, preferred_element_type=jnp.float32)
    grad_w_gate = jnp.einsum("td,tf->df", normed_two, grad_gate, preferred_element_type=jnp.float32)
    grad_w_up = jnp.einsum("td,tf->df", normed_two, grad_up, preferred_element_type=jnp.float32)
    grad_w_down = jnp.einsum("tf,td->fd", hidden, grad_ffn, preferred_element_type=jnp.float32)
    return (grad_w_qkv, grad_w_out, grad_w_gate, grad_w_up, grad_w_down)


def on_device(
    tokens,
    segment_ids,
    variate_ids,
    time_ids,
    pad_mask,
    cotangent,
    w_qkv,
    w_out,
    w_gate,
    w_up,
    w_down,
    gain_attn,
    gain_ffn,
    variate_bias,
):
    micro_count, row_count, model_width = tokens.shape
    hop_count = -(-WINDOW // row_count)
    key_count = (2 * hop_count + 1) * row_count
    shards = (w_qkv, w_out, w_gate, w_up, w_down)
    var_bias = variate_bias.astype(jnp.float32)
    gain_one = gain_attn.astype(jnp.float32)
    gain_two = gain_ffn.astype(jnp.float32)
    bias_total = jnp.zeros(var_bias.shape, jnp.float32)
    gain_one_total = jnp.zeros(gain_one.shape, jnp.float32)
    gain_two_total = jnp.zeros(gain_two.shape, jnp.float32)
    grad_totals = None
    saved = []
    outputs = []
    input_grads = []
    held_weights = fetch_weights(shards)
    for micro_step in range(micro_count):
        if micro_step == 0:
            weights = held_weights
        else:
            weights = fetch_keep(shards)
        resid_in = tokens[micro_step].astype(jnp.float32)
        inv_one = norm_scale(resid_in)
        normed_one = (resid_in * inv_one * gain_one).astype(jnp.bfloat16)
        qkv_proj = jnp.dot(normed_one, weights[0], preferred_element_type=jnp.float32)
        cos_table, sine_table = rope_tables(time_ids[micro_step], HEAD_DIM // 2)
        query_rot = rotate(
            qkv_proj[:, :model_width].reshape(row_count, HEADS, HEAD_DIM), cos_table, sine_table
        ).astype(jnp.bfloat16)
        key_rot = rotate(
            qkv_proj[:, model_width : 2 * model_width].reshape(row_count, HEADS, HEAD_DIM),
            cos_table,
            sine_table,
        ).astype(jnp.bfloat16)
        value_own = qkv_proj[:, 2 * model_width :].astype(jnp.bfloat16)
        kv_own = jnp.stack([key_rot.reshape(row_count, model_width), value_own])
        labels_own = jnp.stack(
            [segment_ids[micro_step], variate_ids[micro_step], pad_mask[micro_step]]
        )
        kv_slots = []
        label_slots = []
        for slot_index in range(2 * hop_count + 1):
            offset = slot_index - hop_count
            if offset == 0:
                kv_slots.append(kv_own)
                label_slots.append(labels_own)
            else:
                kv_slots.append(passed_along(kv_own, "seq", -offset))
                label_slots.append(passed_along(labels_own, "seq", -offset))
        kv_all = jnp.concatenate(kv_slots, axis=1)
        labels_keys = jnp.concatenate(label_slots, axis=1)
        keys_all = kv_all[0].reshape(key_count, HEADS, HEAD_DIM)
        values_all = kv_all[1].reshape(key_count, HEADS, HEAD_DIM)
        scores, same_var = masked_scores(
            query_rot, keys_all, labels_own, labels_keys, var_bias, hop_count
        )
        maxima = jnp.max(scores, axis=-1, keepdims=True)
        exp_shift = jnp.exp(scores - maxima)
        denom_sum = jnp.sum(exp_shift, axis=-1, keepdims=True)
        log_norm = maxima + jnp.log(denom_sum)
        prob_low = (exp_shift / denom_sum).astype(jnp.bfloat16)
        attended = jnp.einsum(
            "hqk,khd->qhd", prob_low, values_all, preferred_element_type=jnp.float32
        )
        attended = attended.reshape(row_count, model_width).astype(jnp.bfloat16)
        resid_mid = resid_in + jnp.dot(attended, weights[1], preferred_element_type=jnp.float32)
        inv_two = norm_scale(resid_mid)
        normed_two = (resid_mid * inv_two * gain_two).astype(jnp.bfloat16)
        gate_proj = jnp.dot(normed_two, weights[2], preferred_element_type=jnp.float32)
        up_proj = jnp.dot(normed_two, weights[3], preferred_element_type=jnp.float32)
        gate_sig = jax.nn.sigmoid(gate_proj)
        hidden = (gate_proj * gate_sig * up_proj).astype(jnp.bfloat16)
        ffn_out = jnp.dot(hidden, weights[4], preferred_element_type=jnp.float32)
        outputs.append((resid_mid + ffn_out).astype(jnp.bfloat16))
        grad_out = cotangent[micro_step].astype(jnp.float32)
        grad_ffn = grad_out.astype(jnp.bfloat16)
        grad_hidden = jnp.einsum(
            "td,fd->tf", grad_ffn, weights[4], preferred_element_type=jnp.float32
        )
        grad_gate = (
            grad_hidden * up_proj * gate_sig * (1.0 + gate_proj * (1.0 - gate_sig))
        ).astype(jnp.bfloat16)
        grad_up = (grad_hidden * gate_proj * gate_sig).astype(jnp.bfloat16)
        grad_normed_two = jnp.einsum(
            "tf,df->td", grad_gate, weights[2], preferred_element_type=jnp.float32
        )
        grad_normed_two = grad_normed_two + jnp.einsum(
            "tf,df->td", grad_up, weights[3], preferred_element_type=jnp.float32
        )
        gain_two_total = gain_two_total + jnp.sum(grad_normed_two * resid_mid * inv_two, axis=0)
        grad_mid = grad_out + norm_back(grad_normed_two * gain_two, resid_mid, inv_two)
        grad_branch = grad_mid.astype(jnp.bfloat16)
        grad_attended = jnp.einsum(
            "to,io->ti", grad_branch, weights[1], preferred_element_type=jnp.float32
        )
        grad_attended = grad_attended.astype(jnp.bfloat16).reshape(row_count, HEADS, HEAD_DIM)
        scores, same_var = masked_scores(
            query_rot, keys_all, labels_own, labels_keys, var_bias, hop_count
        )
        prob_full = jnp.exp(scores - log_norm)
        prob_low = prob_full.astype(jnp.bfloat16)
        grad_values = jnp.einsum(
            "hqk,qhd->khd", prob_low, grad_attended, preferred_element_type=jnp.float32
        )
        grad_prob = jnp.einsum(
            "qhd,khd->hqk", grad_attended, values_all, preferred_element_type=jnp.float32
        )
        grad_scores = prob_full * (
            grad_prob - jnp.sum(prob_full * grad_prob, axis=-1, keepdims=True)
        )
        grad_scores = grad_scores.astype(jnp.bfloat16)
        bias_total = bias_total + jnp.sum(
            grad_scores.astype(jnp.float32) * same_var[None], axis=(1, 2)
        )
        grad_query = jnp.einsum(
            "hqk,khd->qhd", grad_scores, keys_all, preferred_element_type=jnp.float32
        ) * HEAD_DIM ** (-0.5)
        grad_keys = jnp.einsum(
            "hqk,qhd->khd", grad_scores, query_rot, preferred_element_type=jnp.float32
        ) * HEAD_DIM ** (-0.5)
        grad_kv = jnp.stack(
            [grad_keys.reshape(key_count, model_width), grad_values.reshape(key_count, model_width)]
        )
        grad_kv_own = grad_kv[:, hop_count * row_count : (hop_count + 1) * row_count]
        for slot_index in range(2 * hop_count + 1):
            offset = slot_index - hop_count
            if offset != 0:
                slot_grad = grad_kv[:, slot_index * row_count : (slot_index + 1) * row_count]
                grad_kv_own = grad_kv_own + passed_along(
                    slot_grad.astype(jnp.bfloat16), "seq", offset
                ).astype(slot_grad.dtype)
        grad_q_plain = rotate_back(grad_query, cos_table, sine_table).reshape(
            row_count, model_width
        )
        grad_k_plain = rotate_back(
            grad_kv_own[0].reshape(row_count, HEADS, HEAD_DIM), cos_table, sine_table
        ).reshape(row_count, model_width)
        grad_qkv = jnp.concatenate([grad_q_plain, grad_k_plain, grad_kv_own[1]], axis=1).astype(
            jnp.bfloat16
        )
        grad_normed_one = jnp.einsum(
            "tf,df->td", grad_qkv, weights[0], preferred_element_type=jnp.float32
        )
        gain_one_total = gain_one_total + jnp.sum(grad_normed_one * resid_in * inv_one, axis=0)
        grad_input = grad_mid + norm_back(grad_normed_one * gain_one, resid_in, inv_one)
        input_grads.append(grad_input.astype(jnp.bfloat16))
        pieces = (
            normed_one,
            grad_qkv,
            attended,
            grad_branch,
            normed_two,
            grad_gate,
            grad_up,
            hidden,
            grad_ffn,
        )
        saved.append(pieces)
    joined = tuple(
        (
            jnp.concatenate([entry[index] for entry in saved], axis=0)
            for index in range(len(saved[0]))
        )
    )
    grad_totals = reduce_last(weight_grads(joined))
    bias_sum, gain_one_sum, gain_two_sum = lax.psum(
        (bias_total, gain_one_total, gain_two_total), ("dp", "seq")
    )
    return (
        jnp.stack(outputs),
        jnp.stack(input_grads),
        grad_totals[0],
        grad_totals[1],
        grad_totals[2],
        grad_totals[3],
        grad_totals[4],
        gain_one_sum,
        gain_two_sum,
        bias_sum,
    )


MESH = pl.DeviceIdType.MESH
VM = pl.BlockSpec(memory_space=pltpu.VMEM)
HB = pl.BlockSpec(memory_space=pl.ANY)
SM = pl.BlockSpec(memory_space=pltpu.SMEM)
DMA = pltpu.SemaphoreType.DMA
NT = (((1,), (1,)), ((), ()))
TN = (((0,), (0,)), ((), ()))
EVERY = slice(None)


def bf16(*shape):
    return jax.ShapeDtypeStruct(shape, jnp.bfloat16)


def f32(*shape):
    return jax.ShapeDtypeStruct(shape, jnp.float32)


def dot(a, b, dims=None, out=jnp.float32):
    dims = (((1,), (0,)), ((), ())) if dims is None else dims
    return lax.dot_general(a, b, dims, preferred_element_type=jnp.float32).astype(out)


def at(i, j):
    return {"dp": 2 * lax.rem(j, 2) + lax.rem(i, 2), "seq": 2 * (j // 2) + i // 2}


def place():
    dp, seq = lax.axis_index("dp"), lax.axis_index("seq")
    return 2 * lax.rem(seq, 2) + lax.rem(dp, 2), 2 * (seq // 2) + dp // 2


def row_block(i, j):
    return 2 * lax.rem(j, 2) + lax.rem(i, 2)


def column_block(i, j):
    return 2 * (j // 2) + i // 2


def ring(i):
    return i + 1 - 2 * lax.rem(i, 2), lax.rem(i + 2, 4)


def owned(i, s):
    return 4 * lax.rem(i, 2) + 2 * s + i // 2


def keeper(i, j):
    return 2 * (i // 2) + j // 4


def taker(i, j, s):
    return 4 * lax.rem(i, 2) + 2 * s + lax.rem(j, 2)


def send(src, dst, send_sem, recv_sem, peer):
    return pltpu.make_async_remote_copy(
        src_ref=src,
        dst_ref=dst,
        send_sem=send_sem,
        recv_sem=recv_sem,
        device_id=peer,
        device_id_type=MESH,
    )


def landed(ref, sem):
    pltpu.make_async_copy(ref, ref, sem).wait()


def meet(peers, home=False):
    i, j = place()
    barrier = pltpu.get_barrier_semaphore()
    for peer in peers:
        pl.semaphore_signal(barrier, inc=1, device_id=peer, device_id_type=MESH)
    if home:
        target, stays = keeper(i, j), keeper(i, j) == i
        for s in (0, 1):

            @pl.when(jnp.logical_not(stays & (taker(i, j, s) == j)))
            def _():
                pl.semaphore_signal(
                    barrier, inc=1, device_id=at(target, taker(i, j, s)), device_id_type=MESH
                )

        pl.semaphore_wait(barrier, len(peers) + jnp.where(stays, 1, 2))
    else:
        pl.semaphore_wait(barrier, len(peers))


def dp_peers():
    i, j = place()
    return [at(lax.rem(i + step, 4), j) for step in (1, 2, 3)]


def seq_peers():
    i, j = place()
    z, y = j // 2, lax.rem(j, 2)
    return [at(i, 2 * lax.rem(z + step, 4) + y) for step in (1, 2, 3)] + [at(i, 2 * z + 1 - y)]


class Home:
    def __init__(self, ins, outs, sems, slotted):
        self.ins, self.outs, self.slotted = ins, outs, slotted
        self.send_sem, self.recv_sem = sems

    @staticmethod
    def sems(count):
        return [DMA((count, 2)), DMA((count, 2))]

    def target(self, a, s):
        i, _ = place()
        return self.outs[a].at[s if self.slotted else owned(i, s)]

    def start(self, a, s):
        i, j = place()
        slot = lax.rem(j // 2, 2)
        src, dst = self.ins[a].at[s], self.outs[a].at[slot if self.slotted else column_block(i, j)]
        here = (keeper(i, j) == i) & (taker(i, j, s) == j)

        @pl.when(jnp.logical_not(here))
        def _():
            peer = at(keeper(i, j), taker(i, j, s))
            send(src, dst, self.send_sem.at[a, s], self.recv_sem.at[a, slot], peer).start()

        @pl.when(here)
        def _():
            pltpu.make_async_copy(src, dst, self.recv_sem.at[a, slot]).start()

    def wait(self, a, s):
        landed(self.target(a, s), self.recv_sem.at[a, s])

    def finish(self, a):
        i, j = place()
        for s in (0, 1):

            @pl.when(jnp.logical_not((keeper(i, j) == i) & (taker(i, j, s) == j)))
            def _():
                landed(self.ins[a].at[s], self.send_sem.at[a, s])


class GroupGather:
    def __init__(self, outs, sems):
        self.outs = outs
        self.s_core, self.r_core, self.s_x, self.r_x, self.s_on, self.r_on = sems

    @staticmethod
    def sems(count):
        return [DMA((count, 2))] * 6

    def push(self, a, s):
        i, j = place()
        core, across = ring(i)
        block = self.outs[a].at[owned(i, s)]
        send(block, block, self.s_x.at[a, s], self.r_x.at[a, s], at(across, j)).start()
        send(block, block, self.s_core.at[a, s], self.r_core.at[a, s], at(core, j)).start()

    def relay(self, a, s):
        i, j = place()
        core, across = ring(i)
        block = self.outs[a].at[owned(across, s)]
        landed(block, self.r_x.at[a, s])
        send(block, block, self.s_on.at[a, s], self.r_on.at[a, s], at(core, j)).start()

    def near(self, a):
        core, _ = ring(place()[0])
        for s in (0, 1):
            landed(self.outs[a].at[owned(core, s)], self.r_core.at[a, s])

    def beyond(self, a):
        core, _ = ring(place()[0])
        for s in (0, 1):
            landed(self.outs[a].at[owned(lax.rem(core + 2, 4), s)], self.r_on.at[a, s])

    def finish(self, a):
        self.near(a)
        self.beyond(a)
        self.sent(a)

    def sent(self, a):
        for s in (0, 1):
            for sem in (self.s_x, self.s_core, self.s_on):
                landed(self.outs[a].at[s], sem.at[a, s])


class GroupSum:
    def __init__(self, parts, buffers, sems):
        self.parts = parts
        self.near, self.far = buffers
        self.s_core, self.r_core, self.s_x, self.r_x = sems

    @staticmethod
    def buffers():
        block = (128, 1024)
        return [pltpu.VMEM((2, 2) + block, jnp.bfloat16), pltpu.VMEM((2,) + block, jnp.bfloat16)]

    @staticmethod
    def sems():
        return [DMA((2, 2)), DMA((2, 2)), DMA((2,)), DMA((2,))]

    def start(self, s):
        i, j = place()
        core, _ = ring(i)
        for side, owner in ((0, lax.rem(core + 2, 4)), (1, core)):
            send(
                self.parts.at[owned(owner, s)],
                self.near.at[side, s],
                self.s_core.at[side, s],
                self.r_core.at[side, s],
                at(core, j),
            ).start()

    def cross(self, s):
        i, j = place()
        _, across = ring(i)
        landed(self.near.at[0, s], self.r_core.at[0, s])
        both = self.parts[owned(across, s)].astype(jnp.float32)
        both = both + self.near[0, s].astype(jnp.float32)
        self.near[0, s] = both.astype(jnp.bfloat16)
        send(
            self.near.at[0, s], self.far.at[s], self.s_x.at[s], self.r_x.at[s], at(across, j)
        ).start()

    def total(self, s):
        i, _ = place()
        landed(self.near.at[1, s], self.r_core.at[1, s])
        both = self.parts[owned(i, s)].astype(jnp.float32) + self.near[1, s].astype(jnp.float32)
        landed(self.far.at[s], self.r_x.at[s])
        return both + self.far[s].astype(jnp.float32)

    def finish(self):
        for s in (0, 1):
            landed(self.near.at[0, s], self.s_x.at[s])
            for side in (0, 1):
                landed(self.near.at[side, s], self.s_core.at[side, s])


def when(condition):
    return (lambda body: body()) if condition is None else pl.when(condition)


class Exchange:
    def __init__(self, pieces, sems):
        self.pieces = pieces
        self.send_sem, self.recv_sem, self.own_sem = sems

    @staticmethod
    def sems(count):
        return [DMA((3, count)), DMA((3, count)), DMA((count,))]

    def start(self):
        i, j = place()
        for step in (2, 3, 1):
            other = lax.rem(i + step, 4)
            for index, (src, dst, sends, _) in enumerate(self.pieces(i, other)):

                @when(sends)
                def _():
                    send(
                        src,
                        dst,
                        self.send_sem.at[step - 1, index],
                        self.recv_sem.at[step - 1, index],
                        at(other, j),
                    ).start()

        for index, (src, dst, sends, _) in enumerate(self.pieces(i, i)):

            @when(sends)
            def _():
                pltpu.make_async_copy(src, dst, self.own_sem.at[index]).start()

    def wait(self):
        i, _ = place()
        for step in (2, 3, 1):
            there, source = lax.rem(i + step, 4), lax.rem(i + 4 - step, 4)
            for index, (src, _, sends, _) in enumerate(self.pieces(i, there)):

                @when(sends)
                def _():
                    landed(src, self.send_sem.at[step - 1, index])

            for index, (src, _, _, gets) in enumerate(self.pieces(i, source)):

                @when(gets)
                def _():
                    landed(src, self.recv_sem.at[step - 1, index])

        for index, (src, _, sends, _) in enumerate(self.pieces(i, i)):

            @when(sends)
            def _():
                landed(src, self.own_sem.at[index])


ARRIVAL = ((1, 2, 3), (2, 0, 3), (1, 3, 0), (2, 1, 0))
LEAVING = ((1, 2, 3), (0, 2, 3), (3, 1, 0), (2, 1, 0))


def pick(table, z, n):
    row = [entry[n] for entry in table]
    return jnp.where(z == 0, row[0], jnp.where(z == 1, row[1], jnp.where(z == 2, row[2], row[3])))


def inner(z):
    return (z == 1) | (z == 2)


class SeqGather:
    def __init__(self, blocks, sems):
        self.blocks = blocks
        self.s_z, self.r_z, self.s_on, self.s_y, self.r_y = sems

    @staticmethod
    def sems(count):
        return [DMA((count, 2)), DMA((count, 4)), DMA((count, 4)), DMA((count, 4)), DMA((count, 4))]

    def relays(self, source):
        z = place()[1] // 2
        return inner(z) & ((source // 2 != z // 2) | inner(source))

    def start_z(self, chunk):
        i, j = place()
        z, x = j // 2, lax.rem(j, 2)
        own = self.blocks[chunk](z, x)
        targets = [pick(((2, 1), (2, 0), (1, 3), (1, 2)), z, n) for n in (0, 1)]
        for n, target in enumerate(targets):
            peer = at(i, 2 * target + x)
            send(own, own, self.s_z.at[chunk, n], self.r_z.at[chunk, z], peer).start()

    def start_y(self, chunk):
        i, j = place()
        z, x = j // 2, lax.rem(j, 2)
        own = self.blocks[chunk](z, x)
        peer = at(i, 2 * z + 1 - x)
        send(own, own, self.s_y.at[chunk, z], self.r_y.at[chunk, z], peer).start()

    def relayed(self, chunk):
        _, j = place()
        z, x = j // 2, lax.rem(j, 2)
        own = self.blocks[chunk](z, x)
        for n in (0, 1):
            landed(own, self.s_z.at[chunk, n])
        for n in (0, 1, 2):
            source = pick(ARRIVAL, z, n)

            @pl.when(self.relays(source))
            def _():
                landed(own, self.s_on.at[chunk, source])

    def forward(self, chunk, n):
        i, j = place()
        z, x = j // 2, lax.rem(j, 2)
        source = pick(ARRIVAL, z, n)
        block = self.blocks[chunk](source, x)
        landed(block, self.r_z.at[chunk, source])

        @pl.when(self.relays(source))
        def _():
            peer = at(i, 2 * jnp.where(z == 1, 0, 3) + x)
            send(
                block, block, self.s_on.at[chunk, source], self.r_z.at[chunk, source], peer
            ).start()

        peer = at(i, 2 * z + 1 - x)
        send(block, block, self.s_y.at[chunk, source], self.r_y.at[chunk, source], peer).start()

    def forward_at(self, inside, chunk, n):
        z = place()[1] // 2

        @pl.when(inner(z) if inside else jnp.logical_not(inner(z)))
        def _():
            self.forward(chunk, n)

    def arrived(self, chunk, source):
        x = lax.rem(place()[1], 2)
        landed(self.blocks[chunk](source, 1 - x), self.r_y.at[chunk, source])

    def drain(self, chunk):
        _, j = place()
        z, x = j // 2, lax.rem(j, 2)
        own = self.blocks[chunk](z, x)
        landed(own, self.s_y.at[chunk, z])
        for n in (0, 1, 2):
            landed(own, self.s_y.at[chunk, pick(ARRIVAL, z, n)])

    def finish(self, chunk):
        z = place()[1] // 2
        self.arrived(chunk, z)
        for n in (0, 1, 2):
            self.arrived(chunk, pick(ARRIVAL, z, n))
        self.drain(chunk)


class SeqSum:
    def __init__(self, parts, near, far, sems):
        self.parts, self.near, self.far = parts, near, far
        self.s_y, self.r_y, self.s_z, self.r_z = sems

    @staticmethod
    def sems(count):
        return [DMA((count, 4)) for _ in range(4)]

    def start(self, chunk, row):
        i, j = place()
        z, x = j // 2, lax.rem(j, 2)
        send(
            self.parts[chunk](row, 1 - x),
            self.near[chunk](row),
            self.s_y.at[chunk, row],
            self.r_y.at[chunk, row],
            at(i, 2 * z + 1 - x),
        ).start()

    def start_rest(self, chunk):
        z = place()[1] // 2
        for n in (0, 1, 2):
            self.start(chunk, pick(LEAVING, z, n))

    def add(self, target, terms):
        if len(target.shape) == 3:
            for e in range(target.shape[0]):
                self.add(target.at[e], [term.at[e] for term in terms])
            return
        rows = target.shape[0]
        step = min(256, rows)

        @pl.loop(0, rows // step)
        def _(t):
            part = pl.ds(pl.multiple_of(t * step, step), step)
            total = target[part, :].astype(jnp.float32)
            for term in terms:
                total = total + term[part, :].astype(jnp.float32)
            target[part, :] = total.astype(jnp.bfloat16)

    def cross(self, chunk, n):
        i, j = place()
        z, x = j // 2, lax.rem(j, 2)
        row = pick(LEAVING, z, n)
        held = 2 + lax.rem(row, 2)
        near, own, far = self.near[chunk](row), self.parts[chunk](row, x), self.far[chunk](held)
        landed(near, self.r_y.at[chunk, row])
        if n == 0:
            self.add(near, (own,))
        else:

            @pl.when(inner(z))
            def _():
                landed(far, self.r_z.at[chunk, held])
                self.add(near, (own, far))

            @pl.when(jnp.logical_not(inner(z)))
            def _():
                self.add(near, (own,))

        target = jnp.where(inner(z), row, jnp.where(z == 0, 1, 2))
        spot = jnp.where(target == row, z // 2, held)
        send(
            near,
            self.far[chunk](spot),
            self.s_z.at[chunk, row],
            self.r_z.at[chunk, spot],
            at(i, 2 * target + x),
        ).start()

    def finish(self, chunk):
        _, j = place()
        z, x = j // 2, lax.rem(j, 2)
        near, far = self.near[chunk](z), [self.far[chunk](spot) for spot in (0, 1)]
        landed(near, self.r_y.at[chunk, z])
        for spot in (0, 1):
            landed(far[spot], self.r_z.at[chunk, spot])
        self.add(near, (self.parts[chunk](z, x), *far))

    def drain(self, chunk):
        _, j = place()
        z, x = j // 2, lax.rem(j, 2)
        for row in range(4):
            landed(self.near[chunk](row), self.s_y.at[chunk, row])
        for n in (0, 1, 2):
            row = pick(LEAVING, z, n)
            landed(self.near[chunk](row), self.s_z.at[chunk, row])


class SmallSum:
    def __init__(self, value, scratch):
        self.value = value
        self.stages, self.sems = scratch[:3], scratch[3:]

    @staticmethod
    def scratch(shape):
        return [pltpu.VMEM((count,) + shape, jnp.float32) for count in (4, 4, 2)] + [
            DMA((count,)) for count in (3, 3, 3, 3, 1, 1)
        ]

    def round(self, stage):
        i, j = place()
        z, y = j // 2, lax.rem(j, 2)
        return ((i, dp_peers()), (z, seq_peers()[:3]), (y, seq_peers()[3:]))[stage]

    def start(self, stage):
        spot, peers = self.round(stage)
        held = self.stages[stage]
        held[spot] = self.value[...] if stage == 0 else self.total(stage - 1)
        for step, peer in enumerate(peers):
            send(
                held.at[spot],
                held.at[spot],
                self.sems[2 * stage].at[step],
                self.sems[2 * stage + 1].at[step],
                peer,
            ).start()

    def total(self, stage):
        held = self.stages[stage]
        for step in range(held.shape[0] - 1):
            landed(held.at[0], self.sems[2 * stage + 1].at[step])
            landed(held.at[0], self.sems[2 * stage].at[step])
        total = held[0]
        for index in range(1, held.shape[0]):
            total = total + held[index]
        return total


def swap_halves(x):
    lane = lax.broadcasted_iota(jnp.int32, x.shape, 1)
    width = x.shape[1]
    return jnp.where(lane % 64 < 32, pltpu.roll(x, width - 32, 1), pltpu.roll(x, 32, 1))


def angle_tables(table):
    lane = lax.broadcasted_iota(jnp.int32, table.shape, 1)
    by_32, by_64, by_96 = (pltpu.roll(table, shift, 1) for shift in (32, 64, 96))
    first, second, third = lane < 32, lane < 64, lane < 96
    cos_t = jnp.where(first, table, jnp.where(second, by_32, jnp.where(third, by_64, by_96)))
    sin_t = jnp.where(first, -by_96, jnp.where(second, table, jnp.where(third, -by_32, by_64)))
    return cos_t, sin_t


def first_slice(i, b, second=0):
    return jnp.minimum((6 * b - i + 3) // 4 + second, 11)


def local_slice(i, b, second=0):
    return jnp.minimum(lax.rem(i + 2 * lax.rem(b, 2), 4) + 4 * second, 5)


def has_second(i, b):
    return lax.rem(i + 2 * lax.rem(b, 2), 4) < 2


def spot(index, size):
    return pl.ds(pl.multiple_of(size * index, size), size)


def attention_pieces(turned_qkv, w_out, heads, outs):
    def pieces(me, other):
        _, j = place()
        b, rows = column_block(me, j), row_block(me, j)
        found = [(w_out.at[spot(other, 64)], outs.at[b, spot(rows, 64)], None, None)]
        for second in (0, 1):
            found.append(
                (
                    turned_qkv.at[spot(local_slice(other, b, second), 64)],
                    heads.at[spot(first_slice(other, b, second), 64), spot(rows, 256)],
                    has_second(other, b) if second else None,
                    has_second(me, column_block(other, j)) if second else None,
                )
            )
        return found

    return pieces


def return_attention(heads, outs, g_qkv, g_out):
    def pieces(me, other):
        _, j = place()
        b = column_block(other, j)
        side, half = other // 2, lax.rem(other, 2)
        found = [(outs.at[side, spot(half, 64)], g_out.at[spot(me, 64)], None, None)]
        for second in (0, 1):
            held = jnp.minimum(first_slice(me, b, second) - 3 * (j // 2), 2)
            found.append(
                (
                    heads.at[spot(held, 64), spot(half, 256)],
                    g_qkv.at[spot(local_slice(me, b, second), 64)],
                    has_second(me, b) if second else None,
                    has_second(other, column_block(me, j)) if second else None,
                )
            )
        return found

    return pieces


def ffn_pieces(w_gate, w_up, w_down, dst):
    def pieces(me, other):
        _, j = place()
        b, rows = column_block(me, j), row_block(me, j)
        return [
            (w_gate.at[:, spot(other, 128)], dst.at[b, spot(rows, 256)], None, None),
            (w_up.at[:, spot(other, 128)], dst.at[b, spot(4 + rows, 256)], None, None),
        ] + [
            (
                w_down.at[spot(4 * half + other, 128)],
                dst.at[b, spot(16 + 2 * rows + half, 128)],
                None,
                None,
            )
            for half in (0, 1)
        ]

    return pieces


def return_ffn(src, g_gate, g_up, g_down):
    def pieces(me, other):
        side, part = other // 2, lax.rem(other, 2)
        return [
            (src.at[0, side, spot(part, 256)], g_gate.at[:, spot(me, 128)], None, None),
            (src.at[1, side, spot(part, 256)], g_up.at[:, spot(me, 128)], None, None),
        ] + [
            (
                src.at[2, side, spot(2 * part + half, 128)],
                g_down.at[spot(4 * half + me, 128)],
                None,
                None,
            )
            for half in (0, 1)
        ]

    return pieces


def position_table(labels):
    lane = lax.broadcasted_iota(jnp.int32, (128, 128), 1)
    frequency = jnp.exp(-jnp.log(10000.0) * (lane % 32).astype(jnp.float32) / 32)
    angle = labels[:, 3:4] * frequency
    rest = jnp.where(lane == 64, labels[:, 2:3], jnp.where(lane == 65, labels[:, 1:2], labels[:, 0:1]))
    return jnp.where(lane < 32, jnp.cos(angle), jnp.where(lane < 64, jnp.sin(angle), rest))


def norm_rows(hidden):
    return lax.rsqrt(jnp.mean(hidden * hidden, axis=1, keepdims=True) + EPSILON)


def back_rows(grad_in, hidden, inv_rms):
    mean = jnp.mean(grad_in * hidden, axis=1, keepdims=True)
    return inv_rms * grad_in - hidden * (inv_rms * inv_rms * inv_rms * mean)


FFN_CHUNKS = (2048, 0, 1024)
GRAD_CHUNKS = (0, 1024, 2048)


def wide(ref, first, rows):
    return jnp.concatenate([ref[first, rows, :], ref[first + 1, rows, :]], axis=1)


def store_wide(ref, first, rows, value):
    ref[first, rows, :] = value[:, :128]
    ref[first + 1, rows, :] = value[:, 128:]


def two(ref, t, cols=slice(None)):
    value = ref[pl.ds(2 * t, 2), :, cols]
    return value.reshape(256, value.shape[2])


def layer_kernel(*refs):
    (
        tok, cot, segments, variates, times, pads, w_qkv, w_out, w_gate, w_up, w_down,
        gain_attn, gain_ffn, bias_all,
    ), refs = refs[:14], refs[14:]
    (output, input_grad, r_gate, r_up, r_down, r_qkv, r_out, small_out), refs = refs[:8], refs[8:]
    (
        tok_all, cot_all, tab_all, idr_all, tok_own, heads_w, out_w, heads_g, out_g, wm_ref, q_ref,
        k_ref, v_ref, o_ref, lse_ref, rows_ref, part, mid_ref, a2_all, turned, ffn_all, ffn_g,
        hidden_s, dgate_s, dup_s, e2_ref, dq_acc, dk_acc, dv_acc, out_own, in_own, dbias, small,
        near_f, far_f, near_q, far_q, near_o, far_o, idr, turned_qkv,
    ), refs = refs[:41], refs[41:]
    home_in, refs = refs[:2], refs[2:]
    home_out, refs = refs[:2], refs[2:]
    gather_in, refs = refs[:6], refs[6:]
    gather_a2, refs = refs[:6], refs[6:]
    gather_ez, refs = refs[:6], refs[6:]
    buffers, refs = refs[:2], refs[2:]
    out_buffers, refs = refs[:2], refs[2:]
    sum_sems, refs = [refs[4 * n : 4 * n + 4] for n in range(4)], refs[16:]
    spread_a, spread_f, back_a, back_f = [refs[3 * n : 3 * n + 3] for n in range(4)]
    refs = refs[12:]
    chain_a, chain_f, refs = refs[:5], refs[5:10], refs[10:]
    fold_f, fold_a, refs = refs[:4], refs[4:8], refs[8:]
    small_scratch = refs

    i, j = place()
    z, y = j // 2, lax.rem(j, 2)
    mine_first = 2 * (1 - lax.rem(i, 2))

    def turn(u):
        return lax.rem(mine_first + u, 4)

    ez_all, dqkv_ref, out_part = dgate_s, dup_s, turned
    home = Home((tok, idr, cot), (tok_all, idr_all, cot_all), home_in, False)
    group = GroupGather((tok_all, idr_all, cot_all), gather_in)
    spread = Exchange(attention_pieces(turned_qkv, w_out, heads_w, out_w), spread_a)
    spread_ffn = Exchange(ffn_pieces(w_gate, w_up, w_down, ffn_all), spread_f)

    def heads_block(ref):
        return lambda row, side: ref.at[spot(row, 192), spot(side, 512)]

    def outs_block(ref):
        return lambda row, side: ref.at[spot(row, 2), spot(side, 128)]

    def ffn_block(ref, start):
        return lambda row, side: ref.at[spot(row, 2), spot(start // 512 + side, 512)]

    attn_w = SeqGather((heads_block(heads_w), outs_block(out_w)), chain_a)
    ffn_w = SeqGather([ffn_block(ffn_all, start) for start in FFN_CHUNKS], chain_f)
    branch = GroupSum(part, buffers, sum_sems[0])
    second = GroupGather((a2_all,), gather_a2)
    da_sum = GroupSum(part, buffers, sum_sems[1])
    out_sum = GroupSum(out_part, out_buffers, sum_sems[2])
    da1_sum = GroupSum(part, buffers, sum_sems[3])
    third = GroupGather((ez_all,), gather_ez)
    leave = Home((out_own, in_own), (output, input_grad), home_out, True)
    ffn_fold = SeqSum(
        [ffn_block(ffn_g, start) for start in GRAD_CHUNKS],
        [lambda row, chunk=chunk: near_f.at[row, chunk] for chunk in (0, 1, 2)],
        [lambda held, chunk=chunk: far_f.at[held, chunk] for chunk in (0, 1, 2)],
        fold_f,
    )
    attn_fold = SeqSum(
        (heads_block(heads_g), outs_block(out_g)),
        (lambda row: near_q.at[row], lambda row: near_o.at[row]),
        (lambda held: far_q.at[held], lambda held: far_o.at[held]),
        fold_a,
    )
    ffn_back = Exchange(return_ffn(near_f.at[z], r_gate, r_up, r_down), back_f)
    attn_back = Exchange(return_attention(near_q.at[z], near_o.at[z], r_qkv, r_out), back_a)

    turned_qkv[...] = w_qkv[...].T
    for s in (0, 1):
        label = [ref[s : s + 1, :] for ref in (segments, variates, times, pads)]
        lines = (jnp.where(label[3] == 1, label[0], -1), label[1], label[0], label[2])
        for line, value in enumerate(lines):
            idr[s, line : line + 1, :] = value.astype(jnp.float32)
        idr[s, 4:8, :] = jnp.zeros((4, 128), jnp.float32)
    gain_one = gain_attn[...].astype(jnp.float32).reshape(1, 1024)
    gain_two = gain_ffn[...].astype(jnp.float32).reshape(1, 1024)
    sixteen = lax.broadcasted_iota(jnp.int32, (1, 16), 1)
    bias = [
        jnp.sum(
            jnp.where(sixteen == 4 * h + i, bias_all[...].astype(jnp.float32), 0.0),
            axis=1,
            keepdims=True,
        )
        for h in range(4)
    ]
    meet(dp_peers() + seq_peers(), home=True)
    spread.start()
    for a in (0, 1):
        for s in (0, 1):
            home.start(a, s)
    spread.wait()
    for chunk in (0, 1):
        attn_w.start_z(chunk)
    for chunk in (0, 1):
        attn_w.start_y(chunk)
    for a in (0, 1):
        for s in (0, 1):
            home.wait(a, s)
            group.push(a, s)
    spread_ffn.start()
    for s in (0, 1):
        tok_own[s] = tok_all[owned(i, s)]
    for n in (0, 1, 2):
        for chunk in (0, 1):
            attn_w.forward(chunk, n)
    for a in (0, 1):
        for s in (0, 1):
            group.relay(a, s)
    for chunk in (0, 1):
        attn_w.relayed(chunk)
    spread_ffn.wait()
    ffn_w.start_z(0)
    for s in (0, 1):
        home.start(2, s)
    for a in (0, 1):
        group.finish(a)
        home.finish(a)
    for b in range(8):
        rows_ref[:, 128 * b : 128 * b + 128] = idr_all[b]

    @pl.loop(0, 8)
    def _(b):
        hidden = tok_all[b].astype(jnp.float32)
        tok_all[b] = (hidden * norm_rows(hidden) * gain_one).astype(jnp.bfloat16)
        tab_all[b] = position_table(idr_all[b].T)

    a1_all = tok_all
    for chunk in (0, 1):
        attn_w.finish(chunk)
    for chunk in (0, 1, 2):
        ffn_w.start_y(chunk)
    for b in range(8):
        wm_ref[:, 128 * b : 128 * b + 128] = out_w[b]

    @pl.loop(0, 4)
    def _(t):
        rows = pl.ds(pl.multiple_of(t * 256, 256), 256)
        proj = dot(two(a1_all, t), heads_w[...], NT)
        cos_t, sin_t = angle_tables(two(tab_all, t))
        for pair in (0, 1):
            cols = slice(128 * pair, 128 * pair + 128)
            for base, out in ((0, q_ref), (256, k_ref)):
                x = proj[:, base + 128 * pair : base + 128 * pair + 128]
                out[rows, cols] = (x * cos_t + swap_halves(x) * sin_t).astype(jnp.bfloat16)
        v_ref[rows, :] = proj[:, 512:768].astype(jnp.bfloat16)

    @pl.loop(0, 4)
    def _(u):
        t = turn(u)
        start = pl.multiple_of(t * 256, 256)
        rows = pl.ds(start, 256)
        columns = two(tab_all, t)
        seg_q, var_q = columns[:, 64:65], columns[:, 65:66]
        code_k, var_k = rows_ref[0:1, :], rows_ref[1:2, :]
        row = start + lax.broadcasted_iota(jnp.int32, (256, 1024), 0)
        col = lax.broadcasted_iota(jnp.int32, (256, 1024), 1)
        allowed = ((seg_q == code_k) & (jnp.abs(row - col) <= WINDOW)) | (row == col)
        masked = jnp.where(allowed, 0.0, NEGATIVE)
        same = jnp.where(var_q == var_k, 1.0, 0.0)
        stats = jnp.zeros((256, 128), jnp.float32)
        lane = lax.broadcasted_iota(jnp.int32, (256, 128), 1)
        for h in range(4):
            cols = slice(64 * h, 64 * h + 64)
            scores = dot(q_ref[rows, cols] * 0.125, k_ref[:, cols], NT)
            scores = scores + bias[h] * same + masked
            top = jnp.max(scores, axis=1, keepdims=True)
            weight = jnp.exp(scores - top)
            total = jnp.sum(weight, axis=1, keepdims=True)
            mixed = dot(weight.astype(jnp.bfloat16), v_ref[:, cols])
            o_ref[rows, cols] = (mixed / total).astype(jnp.bfloat16)
            stats = jnp.where(lane == h, top + jnp.log(total), stats)
        lse_ref[:, rows] = stats.T[:8]
        part[pl.ds(2 * t, 2)] = dot(o_ref[rows, :], wm_ref[...], out=jnp.bfloat16).reshape(2, 128, 1024)
        for s in (0, 1):

            @pl.when(u == s)
            def _():
                branch.start(s)

            @pl.when(u == s + 2)
            def _():
                branch.cross(s)

        @pl.when(u == 0)
        def _():
            ffn_w.forward(0, 0)
            ffn_w.start_z(1)
            ffn_w.forward_at(True, 0, 1)
            ffn_w.forward_at(True, 0, 2)

        @pl.when(u == 1)
        def _():
            for s in (0, 1):
                home.wait(2, s)
                group.push(2, s)
            ffn_w.forward_at(False, 0, 1)

        @pl.when(u == 2)
        def _():
            ffn_w.forward_at(False, 0, 2)
            ffn_w.forward(1, 0)
            ffn_w.start_z(2)

        @pl.when(u == 3)
        def _():
            for s in (0, 1):
                group.relay(2, s)
            ffn_w.forward_at(True, 1, 1)

    for s in (0, 1):
        block = owned(i, s)
        mid = tok_own[s].astype(jnp.float32) + branch.total(s)
        mid_ref[s] = mid
        a2_all[block] = (mid * norm_rows(mid) * gain_two).astype(jnp.bfloat16)
        second.push(0, s)
    branch.finish()
    ffn_w.forward_at(True, 1, 2)
    ffn_w.forward_at(False, 1, 1)
    for s in (0, 1):
        second.relay(0, s)
    ffn_w.forward_at(False, 1, 2)
    group.finish(2)
    home.finish(2)
    second.finish(0)
    ffn_w.finish(0)
    for n in (0, 1):
        ffn_w.forward(2, n)

    @pl.loop(0, 4)
    def _(t):
        for d in range(4):
            turned[2 * d : 2 * d + 2, :, pl.ds(pl.multiple_of(256 * t, 256), 256)] = (
                two(a2_all, t, slice(256 * d, 256 * d + 256)).T.reshape(2, 128, 256)
            )

    def unit(f):
        cols = pl.ds(pl.multiple_of(256 * f, 256), 256)
        wg, wu = wide(ffn_all, 2 * f, slice(0, 1024)), wide(ffn_all, 2 * f, slice(1024, 2048))
        down = pl.ds(pl.multiple_of(2048 + 256 * f, 256), 256)
        wd = jnp.concatenate([ffn_all[b, down, :] for b in range(8)], axis=1)

        @pl.loop(0, 4)
        def _(t):
            a, g = two(a2_all, t), two(cot_all, t)
            gate, up, dh = dot(a, wg), dot(a, wu), dot(g, wd, NT)
            sig = 1.0 / (1.0 + jnp.exp(-gate))
            gate_sig = gate * sig
            into = (pl.ds(2 * t, 2), slice(None), cols)
            hidden_s[into] = (gate_sig * up).astype(jnp.bfloat16).reshape(2, 128, 256)
            dgate = dh * up * (sig + gate_sig * (1.0 - sig))
            dgate_s[into] = dgate.astype(jnp.bfloat16).reshape(2, 128, 256)
            dup_s[into] = (dh * gate_sig).astype(jnp.bfloat16).reshape(2, 128, 256)

        @pl.loop(0, 4)
        def _(d):
            rows = pl.ds(pl.multiple_of(d * 256, 256), 256)
            rows_up = pl.ds(pl.multiple_of(1024 + d * 256, 256), 256)
            a_t = two(turned, d)
            dgate, dup = dgate_s[:, :, cols].reshape(1024, 256), dup_s[:, :, cols].reshape(1024, 256)
            store_wide(ffn_g, 2 * f, rows, dot(a_t, dgate, out=jnp.bfloat16))
            store_wide(ffn_g, 2 * f, rows_up, dot(a_t, dup, out=jnp.bfloat16))

        h_t = hidden_s[:, :, cols].reshape(1024, 256).T
        for d in range(4):
            g = cot_all[:, :, 256 * d : 256 * d + 256].reshape(1024, 256)
            store_wide(ffn_g, 2 * d, down, dot(h_t, g, out=jnp.bfloat16))

    @pl.loop(0, 4)
    def _(step):
        f = z
        for n in (0, 1, 2):
            f = jnp.where(step == n + 1, pick(ARRIVAL, z, n), f)
        @pl.when(step == 1)
        def _():
            ffn_w.forward(2, 2)

        ffn_w.arrived(1, f)
        ffn_w.arrived(2, f)
        unit(f)

        @pl.when(step > 0)
        def _():
            ffn_fold.start(0, f)
            ffn_fold.start(1, f)

    for chunk in (0, 1, 2):
        ffn_w.relayed(chunk)
    for chunk in (1, 2):
        ffn_w.drain(chunk)

    def at_end(chunk, n):
        @pl.when(jnp.logical_not(inner(z)))
        def _():
            ffn_fold.cross(chunk, n)

    def at_inner(chunk, n):
        @pl.when(inner(z))
        def _():
            ffn_fold.cross(chunk, n)

    def product(left, t, first_row):
        total = None
        for p in range(4):
            piece = dot(
                two(left, t, slice(256 * p, 256 * p + 256)),
                wide(ffn_all, 2 * p, slice(first_row, first_row + 1024)),
                NT,
            )
            total = piece if total is None else total + piece
        return total

    @pl.loop(0, 4)
    def _(u):
        t = turn(u)
        value = product(dgate_s, t, 0) + product(dup_s, t, 1024)
        part[pl.ds(2 * t, 2)] = value.astype(jnp.bfloat16).reshape(2, 128, 1024)
        for s in (0, 1):

            @pl.when(u == s)
            def _():
                da_sum.start(s)

            @pl.when(u == s + 2)
            def _():
                da_sum.cross(s)

    @pl.loop(0, 4)
    def _(u):
        t = turn(u)
        hidden = two(hidden_s, t)
        for d in range(4):
            w = wide(ffn_all, 2 * d, slice(2048, 3072))
            out_part[pl.ds(2 * t, 2), :, 256 * d : 256 * d + 256] = dot(
                hidden, w, out=jnp.bfloat16
            ).reshape(2, 128, 256)
        for s in (0, 1):

            @pl.when(u == s)
            def _():
                out_sum.start(s)

    at_end(0, 0), at_end(1, 0)
    gain_rows = jnp.zeros((1, 1024), jnp.float32)
    for s in (0, 1):
        mid = mid_ref[s]
        inv = norm_rows(mid)
        da2 = da_sum.total(s)
        gain_rows = gain_rows + jnp.sum(da2 * (mid * inv), axis=0, keepdims=True)
        e2 = cot_all[owned(i, s)].astype(jnp.float32) + back_rows(da2 * gain_two, mid, inv)
        e2_ref[s] = e2
        ez_all[owned(i, s)] = e2.astype(jnp.bfloat16)
        third.push(0, s)
    for b in range(8):
        small[8 + b : 9 + b, :] = gain_rows[:, 128 * b : 128 * b + 128]
    da_sum.finish()
    ffn_fold.start_rest(2)
    at_inner(0, 0), at_inner(1, 0)
    at_end(0, 1), at_end(1, 1)
    for s in (0, 1):
        out_sum.cross(s)
    third.near(0)

    def unturn(acc, base, blocks, rows):
        for block, part_rows in zip(blocks, rows):
            cos_t, sin_t = angle_tables(tab_all[block])
            for pair in (0, 1):
                g = acc[part_rows, 128 * pair : 128 * pair + 128]
                dqkv_ref[block, :, base + 128 * pair : base + 128 * pair + 128] = (
                    g * cos_t - swap_halves(g) * sin_t
                ).astype(jnp.bfloat16)

    dk_acc[...] = jnp.zeros_like(dk_acc)
    dv_acc[...] = jnp.zeros_like(dv_acc)
    dbias[...] = jnp.zeros_like(dbias)

    @pl.loop(0, 4)
    def _(u):
        @pl.when(u == 2)
        def _():
            third.relay(0, 0)
            third.relay(0, 1)
            third.beyond(0)
            for d in range(4):
                ez = ez_all[:, :, 256 * d : 256 * d + 256].reshape(1024, 256)
                store_wide(out_g, 2 * d, slice(None), dot(o_ref[...], ez, TN, jnp.bfloat16))
            attn_fold.start_rest(1)

        b = 2 * lax.rem(u, 2) + jnp.where(u < 2, i // 2, 1 - i // 2)
        upper = b + 4
        rows = pl.ds(pl.multiple_of(128 * b, 128), 128)
        rows_up = pl.ds(pl.multiple_of(128 * upper, 128), 128)

        def both(ref, cols):
            return jnp.concatenate([ref[rows, cols], ref[rows_up, cols]], axis=0)

        do = dot(jnp.concatenate([ez_all[b], ez_all[upper]], axis=0), wm_ref[...], NT, jnp.bfloat16)
        columns = tab_all[...].reshape(1024, 128)
        var_k, code_k = columns[:, 65:66], columns[:, 66:67]
        label = jnp.concatenate([idr_all[b], idr_all[upper]], axis=1)
        log_sum = jnp.concatenate([lse_ref[:, rows], lse_ref[:, rows_up]], axis=1)
        seg_q, var_q = label[2:3, :], label[1:2, :]
        row = lax.broadcasted_iota(jnp.int32, (1024, 256), 0)
        lane = lax.broadcasted_iota(jnp.int32, (1024, 256), 1)
        col = 128 * b + jnp.where(lane < 128, lane, lane + 384)
        allowed = ((seg_q == code_k) & (jnp.abs(row - col) <= WINDOW)) | (row == col)
        masked = jnp.where(allowed, 0.0, NEGATIVE)
        same = jnp.where(var_q == var_k, 1.0, 0.0)
        for h in range(4):
            cols = slice(64 * h, 64 * h + 64)
            q_h, k_h, v_h = both(q_ref, cols) * 0.125, k_ref[:, cols], v_ref[:, cols]
            do_h = do[:, cols]
            scores = dot(k_h, q_h, NT) + bias[h] * same + masked
            prob = jnp.exp(scores - log_sum[h : h + 1, :])
            dv_acc[:, cols] += dot(prob.astype(jnp.bfloat16), do_h)
            dprob = dot(v_h, do_h, NT)
            mean = jnp.sum(prob * dprob, axis=0, keepdims=True)
            dscore = (prob * (dprob - mean)).astype(jnp.bfloat16)
            dbias[h : h + 1, :] += jnp.sum(dscore.astype(jnp.float32) * same, axis=0, keepdims=True)
            dk_acc[:, cols] += dot(dscore, q_h)
            dq_acc[:, cols] = dot(dscore, k_h, TN) * 0.125

        unturn(dq_acc, 0, (b, upper), (slice(0, 128), slice(128, 256)))

        @pl.when(u == 0)
        def _():
            at_end(0, 2), at_end(1, 2)

        @pl.when(u == 1)
        def _():
            at_inner(0, 1), at_inner(1, 1)
            ffn_fold.cross(2, 0)

        @pl.when(u == 2)
        def _():
            at_inner(0, 2), at_inner(1, 2)
            at_end(2, 1), at_end(2, 2)
            ffn_fold.start(0, z)

        @pl.when(u == 3)
        def _():
            at_inner(2, 1)

    @pl.loop(0, 4)
    def _(t):
        rows = pl.ds(pl.multiple_of(t * 256, 256), 256)
        unturn(
            dk_acc,
            256,
            (2 * t, 2 * t + 1),
            [pl.ds(pl.multiple_of(t * 256 + 128 * e, 128), 128) for e in (0, 1)],
        )
        dqkv_ref[pl.ds(2 * t, 2), :, 512:768] = (
            dv_acc[rows, :].astype(jnp.bfloat16).reshape(2, 128, 256)
        )

    for d in range(3):
        block = slice(256 * d, 256 * d + 256)
        heads_g[block, :] = dot(
            dqkv_ref[:, :, block].reshape(1024, 256), a1_all[...].reshape(1024, 1024), TN, jnp.bfloat16
        )
    at_inner(2, 2)
    attn_fold.start_rest(0)
    for s in (0, 1):
        out_own[s] = (mid_ref[s] + out_sum.total(s)).astype(jnp.bfloat16)
        leave.start(0, s)

    @pl.loop(0, 4)
    def _(u):
        t = turn(u)
        part[pl.ds(2 * t, 2)] = dot(
            two(dqkv_ref, t, slice(0, 768)), heads_w[...], out=jnp.bfloat16
        ).reshape(2, 128, 1024)
        for s in (0, 1):

            @pl.when(u == s)
            def _():
                da1_sum.start(s)

            @pl.when(u == s + 2)
            def _():
                da1_sum.cross(s)

    third.sent(0)
    for chunk in (1, 2):
        ffn_fold.start(chunk, z)
    for chunk in (1, 0):
        attn_fold.start(chunk, z)
    for chunk in (1, 0):
        attn_fold.cross(chunk, 0)

    @pl.when(jnp.logical_not(inner(z)))
    def _():
        for n in (1, 2):
            for chunk in (1, 0):
                attn_fold.cross(chunk, n)

    gain_rows = jnp.zeros((1, 1024), jnp.float32)
    for s in (0, 1):
        hidden = tok_own[s].astype(jnp.float32)
        inv = norm_rows(hidden)
        da1 = da1_sum.total(s)
        gain_rows = gain_rows + jnp.sum(da1 * (hidden * inv), axis=0, keepdims=True)
        grad = e2_ref[s] + back_rows(da1 * gain_one, hidden, inv)
        in_own[s] = grad.astype(jnp.bfloat16)
        leave.start(1, s)
    for b in range(8):
        small[b : b + 1, :] = gain_rows[:, 128 * b : 128 * b + 128]
    lane = lax.broadcasted_iota(jnp.int32, (8, 128), 1)
    line = lax.broadcasted_iota(jnp.int32, (8, 128), 0)
    bias_row = jnp.zeros((8, 128), jnp.float32)
    for h in range(4):
        value = jnp.sum(dbias[h : h + 1, :], axis=1, keepdims=True)
        bias_row = jnp.where((line == 0) & (lane == 4 * h + i), value, bias_row)
    small[16:24, :] = bias_row
    small_sum = SmallSum(small, small_scratch)
    small_sum.start(0)

    @pl.when(inner(z))
    def _():
        for n in (1, 2):
            for chunk in (1, 0):
                attn_fold.cross(chunk, n)

    for chunk in (0, 1, 2):
        ffn_fold.finish(chunk)
    ffn_back.start()
    small_sum.start(1)
    for chunk in (1, 0):
        attn_fold.finish(chunk)
    attn_back.start()
    small_sum.start(2)
    ffn_back.wait()
    small_out[...] = small_sum.total(2)
    out_sum.finish()
    da1_sum.finish()
    for a in (0, 1):
        for s in (0, 1):
            leave.wait(a, s)
        leave.finish(a)
    for chunk in (0, 1, 2):
        ffn_fold.drain(chunk)
    for chunk in (0, 1):
        attn_fold.drain(chunk)
    attn_back.wait()


def layer(arrays):
    def vmem(dtype, *shape):
        return pltpu.VMEM(shape, dtype)

    low, full = jnp.bfloat16, jnp.float32
    blocks = vmem(low, 8, 128, 1024)
    own = vmem(low, 2, 128, 1024)
    heads = vmem(low, 1024, 256)
    grads = vmem(full, 1024, 256)
    return pl.pallas_call(
        layer_kernel,
        out_shape=[
            bf16(2, 128, 1024),
            bf16(2, 128, 1024),
            bf16(256, 512),
            bf16(256, 512),
            bf16(1024, 128),
            bf16(384, 256),
            bf16(256, 128),
            f32(24, 128),
        ],
        in_specs=[HB, HB] + [VM] * 6 + [HB] * 3 + [VM] * 3,
        out_specs=[HB] * 7 + [VM],
        scratch_shapes=[
            blocks,
            blocks,
            vmem(full, 8, 128, 128),
            vmem(full, 8, 8, 128),
            own,
            vmem(low, 768, 1024),
            vmem(low, 8, 256, 128),
            vmem(low, 768, 1024),
            vmem(low, 8, 256, 128),
            vmem(low, 256, 1024),
            heads,
            heads,
            heads,
            heads,
            vmem(full, 8, 1024),
            vmem(full, 8, 1024),
            blocks,
            vmem(full, 2, 128, 1024),
            blocks,
            blocks,
            vmem(low, 8, 3072, 128),
            vmem(low, 8, 3072, 128),
            blocks,
            blocks,
            blocks,
            vmem(full, 2, 128, 1024),
            vmem(full, 256, 256),
            grads,
            grads,
            own,
            own,
            vmem(full, 8, 256),
            vmem(full, 24, 128),
            vmem(low, 4, 3, 2, 512, 128),
            vmem(low, 4, 3, 2, 512, 128),
            vmem(low, 4, 192, 512),
            vmem(low, 4, 192, 512),
            vmem(low, 4, 2, 128, 128),
            vmem(low, 4, 2, 128, 128),
            vmem(full, 2, 8, 128),
            vmem(low, 384, 256),
        ]
        + Home.sems(3)
        + Home.sems(2)
        + GroupGather.sems(3)
        + GroupGather.sems(1)
        + GroupGather.sems(1)
        + GroupSum.buffers()
        + GroupSum.buffers()
        + GroupSum.sems() * 4
        + Exchange.sems(3)
        + Exchange.sems(4)
        + Exchange.sems(3)
        + Exchange.sems(4)
        + SeqGather.sems(2)
        + SeqGather.sems(3)
        + SeqSum.sems(3)
        + SeqSum.sems(2)
        + SmallSum.scratch((24, 128)),
        compiler_params=pltpu.CompilerParams(
            collective_id=1, has_side_effects=True, vmem_limit_bytes=67_043_328
        ),
        name="layer",
    )(*arrays)


def finish_kernel(*refs):
    (out_in, grad_in, gate, up, down, qkv, out, small), refs = refs[:8], refs[8:]
    output, input_grad, g_qkv, g_out, g_gate, g_up, g_down, one, two_, bias = refs
    output[...] = out_in[...]
    input_grad[...] = grad_in[...]
    g_qkv[...] = qkv[...].astype(jnp.float32).T
    for target, source in ((g_out, out), (g_gate, gate), (g_up, up), (g_down, down)):
        target[...] = source[...].astype(jnp.float32)
    one[...] = small[0:8, :]
    two_[...] = small[8:16, :]
    bias[...] = small[16:17, 0:16]


def finish(arrays):
    return pl.pallas_call(
        finish_kernel,
        out_shape=[
            bf16(2, 128, 1024),
            bf16(2, 128, 1024),
            f32(256, 384),
            f32(256, 128),
            f32(256, 512),
            f32(256, 512),
            f32(1024, 128),
            f32(8, 128),
            f32(8, 128),
            f32(1, 16),
        ],
        in_specs=[VM] * 8,
        out_specs=[VM] * 10,
        name="finish",
    )(*arrays)


def on_group(
    tokens, segment_ids, variate_ids, time_ids, pad_mask, cotangent,
    w_qkv, w_out, w_gate, w_up, w_down, gain_attn, gain_ffn, variate_bias,
):
    results = layer(
        [
            tokens, cotangent, segment_ids, variate_ids, time_ids, pad_mask, w_qkv, w_out, w_gate, w_up,
            w_down, gain_attn, gain_ffn, variate_bias[None],
        ]
    )
    *large, one, two_, bias_grad = finish(results)
    return (*large, one.reshape(1024), two_.reshape(1024), bias_grad.reshape(16))


def solution(mesh):
    in_specs = (
        P("dp", "seq", None),
        P("dp", "seq"),
        P("dp", "seq"),
        P("dp", "seq"),
        P("dp", "seq"),
        P("dp", "seq", None),
        P("dp", "seq"),
        P("dp", "seq"),
        P("dp", "seq"),
        P("dp", "seq"),
        P("dp", "seq"),
        P(),
        P(),
        P(),
    )
    out_specs = (
        P("dp", "seq", None),
        P("dp", "seq", None),
        P("dp", "seq"),
        P("dp", "seq"),
        P("dp", "seq"),
        P("dp", "seq"),
        P("dp", "seq"),
        P(),
        P(),
        P(),
    )
    grouped = mesh.shape["dp"] == 4 and mesh.shape["seq"] == 8
    return jax.shard_map(
        on_group if grouped else on_device, mesh=mesh, in_specs=in_specs, out_specs=out_specs, check_vma=False
    )
```
